512 devices in a mesh: mode: 128 (over y, z, core), cores: 4 (over x).
Axes of the slice: x: 4, y: 4, z: 16, core: 2. Of those that a mesh axis runs over, the one named last changes fastest.
Arguments:
- train_cores: bfloat16 [4, 400, 512, 400], P('cores', None, 'mode'), may hold values from -0.06187184 to 0.06187184
- sketch_cores: bfloat16 [4, 100, 512, 100], P('cores', None, 'mode'), may hold values from -0.3125 to 0.3125
- left_interface: float32 [100, 400], replicated, may hold values from -6 to 6
- right_sketch: bfloat16 [400, 100], replicated, may hold values from -6 to 6
Outputs:
- frames: bfloat16 [4, 100, 512, 100], P('cores', None, 'mode')
- interfaces: float32 [4, 100, 400], P('cores')
The draws below stay inside these ranges and needn't reach their ends.
All inputs are finite; a program needn't handle non-finite values.
Results may differ from the reference program's by a relative error of at most 0.019.
Values may be sent and summed in bfloat16 or wider, within the bound.
No kernel may reach another device: no remote copies, remote signals or barrier semaphores. Data moves between devices by JAX's collectives and lax.ppermute only.
A program may use at most 64 MiB of HBM per device.

```python
import math
import jax
import jax.numpy as jnp
from jax import lax

RANK = 400
SKETCH = 100
MODE = 512
CHAIN = 4


def draw_train_cores(key, part):
    key_scale = jax.random.fold_in(key, 11)
    key_entry = jax.random.fold_in(key, 12)
    exponent = jax.random.uniform(key_scale, (CHAIN, 1, MODE, 1), jnp.float32)
    factor = jnp.exp(exponent * math.log(10.0)) / 4.6
    entries = jnp.clip(jax.random.normal(key_entry, (CHAIN, RANK, MODE, RANK), jnp.float32), -6.0, 6.0)
    return (entries * factor / math.sqrt(MODE * SKETCH)).astype(jnp.bfloat16)


def levels(key, dims, cuts, smallest, largest):
    gain, own = 1.0, jax.random.fold_in(key, 6)
    for position, parts in cuts:
        heights = jnp.exp(jax.random.uniform(jax.random.fold_in(own, position), (parts,), jnp.float32, smallest / len(cuts), largest / len(cuts)))
        gain = gain * jnp.repeat(heights, dims[position] // parts).reshape([-1 if axis == position else 1 for axis in range(len(dims))])
    return gain


def gaussian(stream_key, shape, deviation, limit, shards=(), kind=jnp.bfloat16):
    values = deviation * jax.random.normal(stream_key, shape, jnp.float32)
    if shards:
        values = values * levels(stream_key, shape, shards, -0.22, 0.18)
    return jnp.clip(values, -limit, limit).astype(kind)


def setup_inputs(seed: int = 0) -> dict:
    keys = jax.random.split(jax.random.key(seed), 5)
    return {
        "train_cores": draw_train_cores(jax.random.fold_in(keys[4], 71), 0),
        "sketch_cores": gaussian(keys[1], (CHAIN, SKETCH, MODE, SKETCH), RANK ** -0.5, 0.3125, ((0, 4), (2, 128))),
        "left_interface": gaussian(keys[2], (SKETCH, RANK), 1.0, 6.0, (), jnp.float32),
        "right_sketch": gaussian(keys[3], (RANK, SKETCH), 1.0, 6.0),
    }


def reference(train_cores, sketch_cores, left_interface, right_sketch):
    sketches = [right_sketch]
    for index in range(CHAIN - 1, 0, -1):
        flat_core = train_cores[index].reshape(RANK * MODE, RANK)
        partial_value = jnp.dot(flat_core.astype(jnp.float32), sketches[0].astype(jnp.float32), preferred_element_type=jnp.float32).astype(jnp.bfloat16)
        partial_value = partial_value.reshape(RANK, MODE * SKETCH)
        sketch_flat = sketch_cores[index].reshape(SKETCH, MODE * SKETCH)
        next_sketch = lax.dot_general(partial_value.astype(jnp.float32), sketch_flat.astype(jnp.float32), (((1,), (1,)), ((), ())), preferred_element_type=jnp.float32)
        sketches.insert(0, next_sketch.astype(jnp.bfloat16))
    frame_scale = math.sqrt(SKETCH * MODE)
    carry = left_interface
    frame_list = []
    carry_list = []
    for index in range(CHAIN):
        carry_low = carry.astype(jnp.bfloat16)
        built = jnp.dot(carry_low.astype(jnp.float32), train_cores[index].reshape(RANK, MODE * RANK).astype(jnp.float32), preferred_element_type=jnp.float32)
        built = built.astype(jnp.bfloat16).reshape(SKETCH * MODE, RANK)
        images = jnp.dot(built.astype(jnp.float32), sketches[index].astype(jnp.float32), preferred_element_type=jnp.float32)
        gram_matrix = lax.dot_general(images, images, (((0,), (0,)), ((), ())), precision=lax.Precision.HIGHEST)
        chol_lower = jnp.linalg.cholesky(gram_matrix)
        frame_rows = lax.linalg.triangular_solve(chol_lower, images.T, left_side=True, lower=True)
        frame_list.append((frame_rows.T * frame_scale).astype(jnp.bfloat16).reshape(SKETCH, MODE, SKETCH))
        carry = jnp.dot(frame_rows, built.astype(jnp.float32), precision=lax.Precision.HIGHEST)
        carry_list.append(carry)
    return (jnp.stack(frame_list), jnp.stack(carry_list))
```

```python
import math

import jax
import jax.numpy as jnp
from jax import lax
from jax.experimental import pallas as pl
from jax.experimental.pallas import tpu as pltpu
from jax.sharding import Mesh
from jax.sharding import PartitionSpec as P

AXES = ("y", "zh", "zl", "c", "x")
MODE = ("y", "zh", "zl", "c")
NEAR = ("y", "zl", "c")
RANK = 400
SKETCH = 100
ROWS = 128
LANES = 512
F32 = jnp.float32
BF16 = jnp.bfloat16
PARAMS = pltpu.CompilerParams(vmem_limit_bytes=24 * 1024 * 1024)


def dot(a, b, ca, cb, precision=None):
    return lax.dot_general(
        a, b, (((ca,), (cb,)), ((), ())), precision=precision, preferred_element_type=F32
    )


def inverse_factor(gram):
    size = gram.shape[0]
    count = -(-size // 8)
    padded = jnp.pad(gram, ((0, count * 8 - size), (0, 128 - size)))
    tiles = [padded[8 * t : 8 * t + 8] for t in range(count)]
    lane = lax.broadcasted_iota(jnp.int32, (8, 128), 1)
    sub = lax.broadcasted_iota(jnp.int32, (8, 128), 0)
    for j in range(size):
        own, line = divmod(j, 8)
        pivot = tiles[own][line : line + 1]
        scale = 1.0 / pivot[:, j : j + 1]
        unit = jnp.where(lane[:1] == j, 1.0, pivot)
        for t in range(own, count):
            tile = tiles[t]
            factor = tile[:, j : j + 1] * scale
            new = jnp.where(lane == j, 0.0, tile) - factor * unit
            tiles[t] = jnp.where(sub > line, new, tile) if t == own else new
    done = []
    for t in range(count):
        row = sub + 8 * t
        diagonal = jnp.sum(jnp.where(lane == row, tiles[t], 0.0), axis=1, keepdims=True)
        lower = jnp.where(lane < row, tiles[t], jnp.where(lane == row, 1.0, 0.0))
        done.append(lower * lax.rsqrt(diagonal))
    return jnp.concatenate(done, axis=0)[:size, :size]


def symmetric_gram(m_value, sketch_t):
    return 0.5 * (dot(m_value, sketch_t, 1, 1) + dot(sketch_t, m_value, 1, 1))


def sketch_term(core_ref, sketch_core_ref, sketch_t):
    total = None
    for i in range(core_ref.shape[0]):
        partial = dot(core_ref[i], sketch_t, 1, 1).astype(BF16)
        term = dot(sketch_core_ref[i], partial, 1, 1)
        total = term if total is None else total + term
    return total


def first_kernel(x_ref, core_ref, sketch_core_ref, right_ref, left_ref, out_ref, rest_ref):
    out_ref[...] = jnp.zeros((ROWS, LANES), BF16)
    rest_ref[...] = jnp.zeros((ROWS, LANES), BF16)

    @pl.when(x_ref[0] != 0)
    def _():
        out_ref[:SKETCH, :RANK] = sketch_term(
            core_ref, sketch_core_ref, right_ref[...]
        ).astype(BF16)

    @pl.when(x_ref[0] == 0)
    def _():
        square = None
        for i in range(core_ref.shape[0]):
            built = dot(left_ref[...], core_ref[i], 1, 0).astype(BF16)
            term = dot(built, built, 0, 0)
            square = term if square is None else square + term
        square = square.astype(BF16)
        out_ref[:, :RANK] = square[:128]
        rest_ref[:, :256] = square[128:256, 128:384]
        rest_ref[:, 256:384] = square[256:384, 256:384]
        rest_ref[:, 384:400] = square[128:256, 384:400]
        rest_ref[:, 400:416] = square[256:384, 384:400]
        rest_ref[:16, 416:432] = square[384:400, 384:400]


def sketch_kernel(core_ref, sketch_core_ref, sketch_ref, out_ref):
    out_ref[...] = jnp.zeros((ROWS, LANES), BF16)
    out_ref[:SKETCH, :RANK] = sketch_term(
        core_ref, sketch_core_ref, sketch_ref[:SKETCH, :RANK]
    ).astype(BF16)


def last_sketch_kernel(x_ref, core_ref, sketch_core_ref, sketch_ref, rest_ref, out_ref):
    @pl.when(x_ref[0] == 0)
    def _():
        out_ref[...] = rest_ref[...]

    @pl.when(x_ref[0] != 0)
    def _():
        sketch_kernel(core_ref, sketch_core_ref, sketch_ref, out_ref)


def gram_term(core_ref, carry_low, sketch_t):
    total = None
    for i in range(core_ref.shape[0]):
        built = dot(carry_low, core_ref[i], 1, 0).astype(BF16)
        images = dot(built, sketch_t, 1, 1).astype(BF16)
        term = dot(images, built, 0, 0)
        total = term if total is None else total + term
    return total


def project_kernel(m_ref, before_ref, core_ref, sketch_ref, out_ref, carry_ref):
    m_value = m_ref[:SKETCH, :RANK]
    inverse = inverse_factor(symmetric_gram(m_value, before_ref[:SKETCH, :RANK]))
    carry = dot(inverse, m_value.astype(F32), 1, 0, lax.Precision.HIGHEST).astype(BF16)
    carry_ref[...] = carry
    out_ref[...] = jnp.zeros((ROWS, LANES), BF16)
    out_ref[:SKETCH, :RANK] = gram_term(core_ref, carry, sketch_ref[:SKETCH, :RANK]).astype(BF16)


def first_project_kernel(upper_ref, rest_ref, before_ref, core_ref, sketch_ref, out_ref, carry_ref, m0_ref):
    s = before_ref[:SKETCH, :RANK]
    sa, sb, sc, sd = s[:, :128], s[:, 128:256], s[:, 256:384], s[:, 384:400]
    a = upper_ref[:, :RANK]
    b = rest_ref[:, :256]
    c = rest_ref[:, 256:384]
    b_end = rest_ref[:, 384:400]
    c_end = rest_ref[:, 400:416]
    d_end = rest_ref[:16, 416:432]
    over_a = dot(sa, a, 1, 0)
    m0_ref[:, :128] = over_a[:, :128] + dot(s[:, 128:], a[:, 128:], 1, 1)
    m0_ref[:, 128:256] = (
        over_a[:, 128:256] + dot(sb, b[:, :128], 1, 0) + dot(sc, b[:, 128:], 1, 1) + dot(sd, b_end, 1, 1)
    )
    m0_ref[:, 256:384] = over_a[:, 256:384] + dot(sb, b[:, 128:], 1, 0) + dot(sc, c, 1, 0) + dot(sd, c_end, 1, 1)
    m0_ref[:, 384:400] = over_a[:, 384:400] + dot(sb, b_end, 1, 0) + dot(sc, c_end, 1, 0) + dot(sd, d_end, 1, 0)
    m_value = m0_ref[...]
    high = m_value.astype(BF16)
    low = (m_value - high.astype(F32)).astype(BF16)
    inverse = inverse_factor(symmetric_gram(high, s) + symmetric_gram(low, s))
    carry = dot(inverse, m_value, 1, 0, lax.Precision.HIGHEST).astype(BF16)
    carry_ref[...] = carry
    out_ref[...] = jnp.zeros((ROWS, LANES), BF16)
    out_ref[:SKETCH, :RANK] = gram_term(core_ref, carry, sketch_ref[:SKETCH, :RANK]).astype(BF16)


def images_kernel(carry_ref, core_ref, sketch_ref, out_ref):
    for i in range(core_ref.shape[0]):
        built = dot(carry_ref[...], core_ref[i], 1, 0).astype(BF16)
        out_ref[i] = dot(built, sketch_ref[...], 1, 1)


def final_kernel(scale, m_ref, sketch_ref, images_ref, frames_ref, interface_ref):
    m_value = m_ref[...]
    high = m_value.astype(BF16)
    low = (m_value - high.astype(F32)).astype(BF16)
    sketch_t = sketch_ref[...]
    inverse = inverse_factor(symmetric_gram(high, sketch_t) + symmetric_gram(low, sketch_t))
    interface_ref[...] = dot(inverse, m_value, 1, 0, lax.Precision.HIGHEST)
    for i in range(images_ref.shape[0]):
        orth = dot(images_ref[i], inverse, 1, 1, lax.Precision.HIGHEST)
        frames_ref[i] = (orth * scale).astype(BF16)


def call(kernel, *operands, out, scalar=False):
    specs = [pl.BlockSpec(memory_space=pltpu.VMEM) for _ in operands]
    if scalar:
        specs[0] = pl.BlockSpec(memory_space=pltpu.SMEM)
    outs = [jax.ShapeDtypeStruct(shape, kind) for shape, kind in out]
    return pl.pallas_call(
        kernel,
        out_shape=outs,
        in_specs=specs,
        out_specs=[pl.BlockSpec(memory_space=pltpu.VMEM) for _ in outs],
        compiler_params=PARAMS,
    )(*operands)


PAYLOAD = ((ROWS, LANES), BF16)


def everywhere(shard, axes, groups, count):
    copies = jnp.broadcast_to(shard, (count, *shard.shape))
    return lax.all_to_all(copies, axes, 0, 0, axis_index_groups=groups, tiled=True)


def shard_sum(value):
    near = 16
    tiles = value.reshape(near, ROWS // near, LANES)
    arrived = lax.all_to_all(tiles, NEAR, 0, 0, tiled=True)
    return arrived.astype(F32).sum(axis=0).astype(BF16)


def added(pieces):
    return pieces.astype(F32).sum(axis=0).astype(BF16)


def paired(value, pairs, far):
    groups = [[x * far + z for x in pair for z in range(far)] for pair in pairs]
    pieces = everywhere(shard_sum(value), ("x", "zh"), groups, 2 * far)
    return pieces[:far], pieces[far:]


def whole(shard):
    return everywhere(shard, NEAR, None, 16)


def body(train_cores, sketch_cores, left_interface, right_sketch):
    far = lax.axis_size("zh")
    plane = lax.axis_index("x")
    plane_ref = plane.astype(jnp.int32).reshape(1)
    core = jnp.swapaxes(train_cores[0], 0, 1)
    sketch_core = jnp.swapaxes(sketch_cores[0], 0, 1)
    modes = core.shape[0]
    frame_scale = math.sqrt(SKETCH * modes * lax.axis_size(MODE))
    right_t = right_sketch.T
    left_low = left_interface.astype(BF16)

    def full(shard):
        return whole(shard).reshape(ROWS, LANES)

    term, rest = call(
        first_kernel, plane_ref, core, sketch_core, right_t, left_low, out=[PAYLOAD, PAYLOAD], scalar=True
    )
    first = full(added(paired(term, ((3, 2), (0, 1)), far)[0]))
    (term,) = call(sketch_kernel, core, sketch_core, first, out=[PAYLOAD])
    second = full(added(paired(term, ((2, 1), (3, 0)), far)[0]))
    (term,) = call(last_sketch_kernel, plane_ref, core, sketch_core, second, rest, out=[PAYLOAD], scalar=True)
    both = paired(term, ((1, 0), (3, 2)), far)
    arrived = whole(jnp.concatenate([added(both[0]), added(both[1])], axis=0))
    third = arrived[:, :8].reshape(ROWS, LANES)
    rest = arrived[:, 8:].reshape(ROWS, LANES)

    carry_kind = ((SKETCH, RANK), BF16)
    term, carry_1, m_0 = call(
        first_project_kernel, first, rest, third, core, second, out=[PAYLOAD, carry_kind, ((SKETCH, RANK), F32)]
    )
    m_1 = full(added(paired(term, ((1, 2), (0, 3)), far)[0]))
    term, carry_2 = call(project_kernel, m_1, second, core, first, out=[PAYLOAD, carry_kind])
    m_2 = full(added(paired(term, ((2, 3), (0, 1)), far)[0]))
    right_wide = jnp.pad(right_t, ((0, ROWS - SKETCH), (0, LANES - RANK)))
    term, carry_3 = call(project_kernel, m_2, first, core, right_wide, out=[PAYLOAD, carry_kind])
    m_3 = full(added(everywhere(shard_sum(term), "zh", None, far)))

    def cut(value):
        return value[:SKETCH, :RANK]

    def own(zero, one, two, three):
        low = jnp.where(plane == 0, zero, one)
        high = jnp.where(plane == 2, two, three)
        return jnp.where(plane < 2, low, high)

    sketch_t = own(cut(third), cut(second), cut(first), right_t)
    carry = own(left_low, carry_1, carry_2, carry_3)
    (images,) = call(images_kernel, carry, core, sketch_t, out=[((modes, SKETCH, SKETCH), F32)])
    m_own = own(m_0, cut(m_1).astype(F32), cut(m_2).astype(F32), cut(m_3).astype(F32))

    def finish(*refs):
        final_kernel(frame_scale, *refs)

    frames, interface = call(
        finish, m_own, sketch_t, images, out=[((modes, SKETCH, SKETCH), BF16), ((SKETCH, RANK), F32)]
    )
    return (jnp.swapaxes(frames, 0, 1)[None], interface[None])


def solution(mesh):
    split = Mesh(mesh.devices.reshape(4, 8, 2, 2, 4), AXES)
    placed = (P("x", None, MODE, None), P("x", None, MODE, None), P(), P())
    return jax.shard_map(
        body,
        mesh=split,
        in_specs=placed,
        out_specs=(P("x", None, MODE, None), P("x", None, None)),
        check_vma=False,
    )
```

```python
import math

import jax
import jax.numpy as jnp
from jax import lax
from jax.experimental import pallas as pl
from jax.experimental.pallas import tpu as pltpu
from jax.sharding import Mesh
from jax.sharding import PartitionSpec as P

AXES = ("y", "zh", "zl", "c", "x")
MODE = ("y", "zh", "zl", "c")
NEAR = ("y", "zl", "c")
RANK = 400
SKETCH = 100
ROWS = 128
LANES = 512
F32 = jnp.float32
BF16 = jnp.bfloat16
PARAMS = pltpu.CompilerParams(vmem_limit_bytes=24 * 1024 * 1024)


def dot(a, b, ca, cb, precision=None):
    return lax.dot_general(
        a, b, (((ca,), (cb,)), ((), ())), precision=precision, preferred_element_type=F32
    )


def inverse_factor(gram):
    size = gram.shape[0]
    count = -(-size // 8)
    padded = jnp.pad(gram, ((0, count * 8 - size), (0, 128 - size)))
    tiles = [padded[8 * t : 8 * t + 8] for t in range(count)]
    lane = lax.broadcasted_iota(jnp.int32, (8, 128), 1)
    sub = lax.broadcasted_iota(jnp.int32, (8, 128), 0)

    def column(tile, j):
        return jnp.broadcast_to(tile[:, j : j + 1], (8, 128))

    def line(tile, s):
        return jnp.broadcast_to(tile[s : s + 1], (8, 128))

    for own in range(count):
        base = 8 * own
        width = min(8, size - base)
        step = lane - base
        columns = {t: [column(tiles[t], base + c) for c in range(width)] for t in range(own, count)}
        head = columns[own]
        scales, leads = [], []
        tile = tiles[own]
        for s in range(width):
            scales.append(1.0 / line(head[s], s))
            leads.append([line(head[c], s) if c > s else None for c in range(width)])
            factor = jnp.where(sub > s, head[s] * scales[s], 0.0)
            pivot = jnp.where(step == s, 1.0, line(tile, s))
            tile = jnp.where((step == s) & (sub > s), 0.0, tile) - factor * pivot
            for c in range(s + 1, width):
                head[c] = head[c] - factor * leads[s][c]
        tiles[own] = tile
        reduced = jnp.where((step > sub) & (step < 8), 0.0, jnp.where(step == sub, 1.0, tile))
        pivots = [line(reduced, s) for s in range(width)]
        for t in range(own + 1, count):
            col = columns[t]
            new = jnp.where((step >= 0) & (step < 8), 0.0, tiles[t])
            for s in range(width):
                factor = col[s] * scales[s]
                new = new - factor * pivots[s]
                for c in range(s + 1, width):
                    col[c] = col[c] - factor * leads[s][c]
            tiles[t] = new
    done = []
    for t in range(count):
        row = sub + 8 * t
        diagonal = jnp.sum(jnp.where(lane == row, tiles[t], 0.0), axis=1, keepdims=True)
        lower = jnp.where(lane < row, tiles[t], jnp.where(lane == row, 1.0, 0.0))
        done.append(lower * lax.rsqrt(diagonal))
    return jnp.concatenate(done, axis=0)[:size, :size]


def symmetric_gram(m_value, sketch_t):
    return 0.5 * (dot(m_value, sketch_t, 1, 1) + dot(sketch_t, m_value, 1, 1))


def sketch_term(core_ref, sketch_core_ref, sketch, dim):
    total = None
    for i in range(core_ref.shape[0]):
        partial = dot(core_ref[i], sketch, 1, dim).astype(BF16)
        term = dot(sketch_core_ref[i], partial, 1, 1)
        total = term if total is None else total + term
    return total


def first_kernel(x_ref, core_ref, sketch_core_ref, right_ref, left_ref, out_ref, rest_ref):
    out_ref[...] = jnp.zeros((ROWS, LANES), BF16)
    rest_ref[...] = jnp.zeros((ROWS, LANES), BF16)

    @pl.when(x_ref[0] != 0)
    def _():
        out_ref[:SKETCH, :RANK] = sketch_term(
            core_ref, sketch_core_ref, right_ref[...], 0
        ).astype(BF16)

    @pl.when(x_ref[0] == 0)
    def _():
        square = None
        left_t = left_ref[...].astype(BF16)
        for i in range(core_ref.shape[0]):
            built = dot(left_t, core_ref[i], 0, 0).astype(BF16)
            term = dot(built, built, 0, 0)
            square = term if square is None else square + term
        square = square.astype(BF16)
        out_ref[:, :RANK] = square[:128]
        rest_ref[:, :256] = square[128:256, 128:384]
        rest_ref[:, 256:384] = square[256:384, 256:384]
        rest_ref[:, 384:400] = square[128:256, 384:400]
        rest_ref[:, 400:416] = square[256:384, 384:400]
        rest_ref[:16, 416:432] = square[384:400, 384:400]


def sketch_kernel(core_ref, sketch_core_ref, sketch_ref, out_ref):
    out_ref[...] = jnp.zeros((ROWS, LANES), BF16)
    out_ref[:SKETCH, :RANK] = sketch_term(
        core_ref, sketch_core_ref, sketch_ref[:SKETCH, :RANK], 1
    ).astype(BF16)


def last_sketch_kernel(x_ref, core_ref, sketch_core_ref, sketch_ref, rest_ref, out_ref):
    @pl.when(x_ref[0] == 0)
    def _():
        out_ref[...] = rest_ref[...]

    @pl.when(x_ref[0] != 0)
    def _():
        sketch_kernel(core_ref, sketch_core_ref, sketch_ref, out_ref)


def gram_term(core_ref, carry_low, sketch_t):
    total = None
    for i in range(core_ref.shape[0]):
        built = dot(carry_low, core_ref[i], 1, 0).astype(BF16)
        images = dot(built, sketch_t, 1, 1).astype(BF16)
        term = dot(images, built, 0, 0)
        total = term if total is None else total + term
    return total


def project_kernel(m_ref, before_ref, core_ref, sketch_ref, out_ref, carry_ref):
    m_value = m_ref[:SKETCH, :RANK]
    inverse = inverse_factor(symmetric_gram(m_value, before_ref[:SKETCH, :RANK]))
    carry = dot(inverse, m_value.astype(F32), 1, 0, lax.Precision.HIGHEST).astype(BF16)
    carry_ref[...] = carry
    out_ref[...] = jnp.zeros((ROWS, LANES), BF16)
    out_ref[:SKETCH, :RANK] = gram_term(core_ref, carry, sketch_ref[:SKETCH, :RANK]).astype(BF16)


def first_project_kernel(upper_ref, rest_ref, before_ref, core_ref, sketch_ref, out_ref, carry_ref, m0_ref):
    s = before_ref[:SKETCH, :RANK]
    sa, sb, sc, sd = s[:, :128], s[:, 128:256], s[:, 256:384], s[:, 384:400]
    a = upper_ref[:, :RANK]
    b = rest_ref[:, :256]
    c = rest_ref[:, 256:384]
    b_end = rest_ref[:, 384:400]
    c_end = rest_ref[:, 400:416]
    d_end = rest_ref[:16, 416:432]
    over_a = dot(sa, a, 1, 0)
    m0_ref[:, :128] = over_a[:, :128] + dot(s[:, 128:], a[:, 128:], 1, 1)
    m0_ref[:, 128:256] = (
        over_a[:, 128:256] + dot(sb, b[:, :128], 1, 0) + dot(sc, b[:, 128:], 1, 1) + dot(sd, b_end, 1, 1)
    )
    m0_ref[:, 256:384] = over_a[:, 256:384] + dot(sb, b[:, 128:], 1, 0) + dot(sc, c, 1, 0) + dot(sd, c_end, 1, 1)
    m0_ref[:, 384:400] = over_a[:, 384:400] + dot(sb, b_end, 1, 0) + dot(sc, c_end, 1, 0) + dot(sd, d_end, 1, 0)
    m_value = m0_ref[...]
    high = m_value.astype(BF16)
    low = (m_value - high.astype(F32)).astype(BF16)
    inverse = inverse_factor(symmetric_gram(high, s) + symmetric_gram(low, s))
    carry = dot(inverse, m_value, 1, 0, lax.Precision.HIGHEST).astype(BF16)
    carry_ref[...] = carry
    out_ref[...] = jnp.zeros((ROWS, LANES), BF16)
    out_ref[:SKETCH, :RANK] = gram_term(core_ref, carry, sketch_ref[:SKETCH, :RANK]).astype(BF16)


def last_project_kernel(
    x_ref, m_ref, before_ref, core_ref, right_ref, left_ref, carry_1_ref, carry_2_ref,
    third_ref, second_ref, first_ref, out_ref, images_ref,
):
    out_ref[...] = jnp.zeros((ROWS, LANES), BF16)

    @pl.when(x_ref[0] == 3)
    def _():
        m_value = m_ref[:SKETCH, :RANK]
        inverse = inverse_factor(symmetric_gram(m_value, before_ref[:SKETCH, :RANK]))
        carry = dot(inverse, m_value.astype(F32), 1, 0, lax.Precision.HIGHEST).astype(BF16)
        total = None
        for i in range(core_ref.shape[0]):
            built = dot(carry, core_ref[i], 1, 0).astype(BF16)
            images = dot(built, right_ref[...], 1, 0)
            images_ref[i] = images
            term = dot(images.astype(BF16), built, 0, 0)
            total = term if total is None else total + term
        out_ref[:SKETCH, :RANK] = total.astype(BF16)

    def images_of(carry, dim, sketch_t):
        for i in range(core_ref.shape[0]):
            built = dot(carry, core_ref[i], dim, 0).astype(BF16)
            images_ref[i] = dot(built, sketch_t, 1, 1)

    @pl.when(x_ref[0] == 2)
    def _():
        images_of(carry_2_ref[...], 1, first_ref[:SKETCH, :RANK])

    @pl.when(x_ref[0] == 1)
    def _():
        images_of(carry_1_ref[...], 1, second_ref[:SKETCH, :RANK])

    @pl.when(x_ref[0] == 0)
    def _():
        images_of(left_ref[...].astype(BF16), 0, third_ref[:SKETCH, :RANK])


def final_kernel(
    scale, x_ref, m_0_ref, m_1_ref, m_2_ref, m_3_ref, third_ref, second_ref, first_ref, right_ref,
    images_ref, frames_ref, interface_ref, m_ref, gram_ref,
):
    def split_gram(m_value, sketch_t):
        high = m_value.astype(BF16)
        low = (m_value - high.astype(F32)).astype(BF16)
        return symmetric_gram(high, sketch_t) + symmetric_gram(low, sketch_t)

    @pl.when(x_ref[0] == 0)
    def _():
        m_ref[...] = m_0_ref[...]
        gram_ref[...] = split_gram(m_0_ref[...], third_ref[:SKETCH, :RANK])

    @pl.when(x_ref[0] == 1)
    def _():
        m_ref[...] = m_1_ref[:SKETCH, :RANK].astype(F32)
        gram_ref[...] = symmetric_gram(m_1_ref[:SKETCH, :RANK], second_ref[:SKETCH, :RANK])

    @pl.when(x_ref[0] == 2)
    def _():
        m_ref[...] = m_2_ref[:SKETCH, :RANK].astype(F32)
        gram_ref[...] = symmetric_gram(m_2_ref[:SKETCH, :RANK], first_ref[:SKETCH, :RANK])

    @pl.when(x_ref[0] == 3)
    def _():
        m_value = m_3_ref[:SKETCH, :RANK]
        m_ref[...] = m_value.astype(F32)
        gram_ref[...] = 0.5 * (dot(m_value, right_ref[...], 1, 0) + dot(right_ref[...], m_value, 0, 1))

    inverse = inverse_factor(gram_ref[...])
    interface_ref[...] = dot(inverse, m_ref[...], 1, 0, lax.Precision.HIGHEST)
    for i in range(images_ref.shape[0]):
        orth = dot(images_ref[i], inverse, 1, 1, lax.Precision.HIGHEST)
        frames_ref[i] = (orth * scale).astype(BF16)


def call(kernel, *operands, out, scalar=False, scratch=()):
    specs = [pl.BlockSpec(memory_space=pltpu.VMEM) for _ in operands]
    if scalar:
        specs[0] = pl.BlockSpec(memory_space=pltpu.SMEM)
    outs = [jax.ShapeDtypeStruct(shape, kind) for shape, kind in out]
    return pl.pallas_call(
        kernel,
        out_shape=outs,
        in_specs=specs,
        out_specs=[pl.BlockSpec(memory_space=pltpu.VMEM) for _ in outs],
        scratch_shapes=[pltpu.VMEM(shape, F32) for shape in scratch],
        compiler_params=PARAMS,
    )(*operands)


PAYLOAD = ((ROWS, LANES), BF16)


def everywhere(shard, axes, groups, count):
    copies = jnp.broadcast_to(shard, (count, *shard.shape))
    return lax.all_to_all(copies, axes, 0, 0, axis_index_groups=groups, tiled=True)


def shard_sum(value):
    near = 16
    tiles = value.reshape(near, ROWS // near, LANES)
    arrived = lax.all_to_all(tiles, NEAR, 0, 0, tiled=True)
    return arrived.astype(F32).sum(axis=0).astype(BF16)


def added(pieces):
    return pieces.astype(F32).sum(axis=0).astype(BF16)


def paired(value, pairs, far):
    groups = [[x * far + z for x in pair for z in range(far)] for pair in pairs]
    pieces = everywhere(shard_sum(value), ("x", "zh"), groups, 2 * far)
    return pieces[:far], pieces[far:]


def whole(shard):
    return everywhere(shard, NEAR, None, 16)


def body(train_cores, sketch_cores, left_interface, right_sketch):
    far = lax.axis_size("zh")
    plane = lax.axis_index("x")
    plane_ref = plane.astype(jnp.int32).reshape(1)
    core = jnp.swapaxes(train_cores[0], 0, 1)
    sketch_core = jnp.swapaxes(sketch_cores[0], 0, 1)
    modes = core.shape[0]
    frame_scale = math.sqrt(SKETCH * modes * lax.axis_size(MODE))
    left_t = left_interface.T

    def full(shard):
        return whole(shard).reshape(ROWS, LANES)

    term, rest = call(
        first_kernel, plane_ref, core, sketch_core, right_sketch, left_t, out=[PAYLOAD, PAYLOAD], scalar=True
    )
    first = full(added(paired(term, ((3, 2), (0, 1)), far)[0]))
    (term,) = call(sketch_kernel, core, sketch_core, first, out=[PAYLOAD])
    second = full(added(paired(term, ((2, 1), (3, 0)), far)[0]))
    (term,) = call(last_sketch_kernel, plane_ref, core, sketch_core, second, rest, out=[PAYLOAD], scalar=True)
    both = paired(term, ((1, 0), (3, 2)), far)
    arrived = whole(jnp.concatenate([added(both[0]), added(both[1])], axis=0))
    third = arrived[:, :8].reshape(ROWS, LANES)
    rest = arrived[:, 8:].reshape(ROWS, LANES)

    carry_kind = ((SKETCH, RANK), BF16)
    term, carry_1, m_0 = call(
        first_project_kernel, first, rest, third, core, second, out=[PAYLOAD, carry_kind, ((SKETCH, RANK), F32)]
    )
    m_1 = full(added(paired(term, ((1, 2), (0, 3)), far)[0]))
    term, carry_2 = call(project_kernel, m_1, second, core, first, out=[PAYLOAD, carry_kind])
    m_2 = full(added(paired(term, ((2, 3), (0, 1)), far)[0]))
    term, images = call(
        last_project_kernel, plane_ref, m_2, first, core, right_sketch, left_t, carry_1, carry_2,
        third, second, first, out=[PAYLOAD, ((modes, SKETCH, SKETCH), F32)], scalar=True,
    )
    m_3 = full(added(everywhere(shard_sum(term), "zh", None, far)))

    def finish(*refs):
        final_kernel(frame_scale, *refs)

    frames, interface = call(
        finish, plane_ref, m_0, m_1, m_2, m_3, third, second, first, right_sketch, images,
        out=[((modes, SKETCH, SKETCH), BF16), ((SKETCH, RANK), F32)], scalar=True,
        scratch=((SKETCH, RANK), (SKETCH, SKETCH)),
    )
    return (jnp.swapaxes(frames, 0, 1)[None], interface[None])


def solution(mesh):
    split = Mesh(mesh.devices.reshape(4, 8, 2, 2, 4), AXES)
    placed = (P("x", None, MODE, None), P("x", None, MODE, None), P(), P())
    return jax.shard_map(
        body,
        mesh=split,
        in_specs=placed,
        out_specs=(P("x", None, MODE, None), P("x", None, None)),
        check_vma=False,
    )
```

```python
import math

import jax
import jax.numpy as jnp
from jax import lax
from jax.experimental import pallas as pl
from jax.experimental.pallas import tpu as pltpu
from jax.sharding import Mesh
from jax.sharding import PartitionSpec as P

AXES = ("y", "z", "c", "x")
MODE = ("y", "z", "c")
RANK = 400
SKETCH = 100
ROWS = 128
LANES = 512
F32 = jnp.float32
BF16 = jnp.bfloat16
PARAMS = pltpu.CompilerParams(vmem_limit_bytes=24 * 1024 * 1024)


def dot(a, b, ca, cb, precision=None):
    return lax.dot_general(
        a, b, (((ca,), (cb,)), ((), ())), precision=precision, preferred_element_type=F32
    )


def inverse_factor(gram):
    size = gram.shape[0]
    count = -(-size // 8)
    padded = jnp.pad(gram, ((0, count * 8 - size), (0, 128 - size)))
    tiles = [padded[8 * t : 8 * t + 8] for t in range(count)]
    lane = lax.broadcasted_iota(jnp.int32, (8, 128), 1)
    sub = lax.broadcasted_iota(jnp.int32, (8, 128), 0)

    def column(tile, j):
        return jnp.broadcast_to(tile[:, j : j + 1], (8, 128))

    def line(tile, s):
        return jnp.broadcast_to(tile[s : s + 1], (8, 128))

    for own in range(count):
        base = 8 * own
        width = min(8, size - base)
        step = lane - base
        columns = {t: [column(tiles[t], base + c) for c in range(width)] for t in range(own, count)}
        head = columns[own]
        scales, leads = [], []
        tile = tiles[own]
        for s in range(width):
            scales.append(1.0 / line(head[s], s))
            leads.append([line(head[c], s) if c > s else None for c in range(width)])
            factor = jnp.where(sub > s, head[s] * scales[s], 0.0)
            pivot = jnp.where(step == s, 1.0, line(tile, s))
            tile = jnp.where((step == s) & (sub > s), 0.0, tile) - factor * pivot
            for c in range(s + 1, width):
                head[c] = head[c] - factor * leads[s][c]
        tiles[own] = tile
        reduced = jnp.where((step > sub) & (step < 8), 0.0, jnp.where(step == sub, 1.0, tile))
        pivots = [line(reduced, s) for s in range(width)]
        for t in range(own + 1, count):
            col = columns[t]
            new = jnp.where((step >= 0) & (step < 8), 0.0, tiles[t])
            for s in range(width):
                factor = col[s] * scales[s]
                new = new - factor * pivots[s]
                for c in range(s + 1, width):
                    col[c] = col[c] - factor * leads[s][c]
            tiles[t] = new
    done = []
    for t in range(count):
        row = sub + 8 * t
        diagonal = jnp.sum(jnp.where(lane == row, tiles[t], 0.0), axis=1, keepdims=True)
        lower = jnp.where(lane < row, tiles[t], jnp.where(lane == row, 1.0, 0.0))
        done.append(lower * lax.rsqrt(diagonal))
    return jnp.concatenate(done, axis=0)[:size, :size]


def symmetric_gram(m_value, sketch_t):
    return 0.5 * (dot(m_value, sketch_t, 1, 1) + dot(sketch_t, m_value, 1, 1))


def sketch_term(core_ref, sketch_core_ref, sketch, dim):
    total = None
    for i in range(core_ref.shape[0]):
        partial = dot(core_ref[i], sketch, 1, dim).astype(BF16)
        term = dot(sketch_core_ref[i], partial, 1, 1)
        total = term if total is None else total + term
    return total


def first_kernel(x_ref, core_ref, sketch_core_ref, right_ref, left_ref, out_ref, rest_ref):
    out_ref[...] = jnp.zeros((ROWS, LANES), BF16)
    rest_ref[...] = jnp.zeros((ROWS, LANES), BF16)

    @pl.when(x_ref[0] != 0)
    def _():
        out_ref[:SKETCH, :RANK] = sketch_term(
            core_ref, sketch_core_ref, right_ref[...], 0
        ).astype(BF16)

    @pl.when(x_ref[0] == 0)
    def _():
        square = None
        left_t = left_ref[...].astype(BF16)
        for i in range(core_ref.shape[0]):
            built = dot(left_t, core_ref[i], 0, 0).astype(BF16)
            term = dot(built, built, 0, 0)
            square = term if square is None else square + term
        square = square.astype(BF16)
        out_ref[:, :RANK] = square[:128]
        rest_ref[:, :256] = square[128:256, 128:384]
        rest_ref[:, 256:384] = square[256:384, 256:384]
        rest_ref[:, 384:400] = square[128:256, 384:400]
        rest_ref[:, 400:416] = square[256:384, 384:400]
        rest_ref[:16, 416:432] = square[384:400, 384:400]


def sketch_kernel(core_ref, sketch_core_ref, sketch_ref, out_ref):
    out_ref[...] = jnp.zeros((ROWS, LANES), BF16)
    out_ref[:SKETCH, :RANK] = sketch_term(
        core_ref, sketch_core_ref, sketch_ref[:SKETCH, :RANK], 1
    ).astype(BF16)


def last_sketch_kernel(x_ref, core_ref, sketch_core_ref, sketch_ref, rest_ref, out_ref):
    @pl.when(x_ref[0] == 0)
    def _():
        out_ref[...] = rest_ref[...]

    @pl.when(x_ref[0] != 0)
    def _():
        sketch_kernel(core_ref, sketch_core_ref, sketch_ref, out_ref)


def gram_term(core_ref, carry_low, sketch_t):
    total = None
    for i in range(core_ref.shape[0]):
        built = dot(carry_low, core_ref[i], 1, 0).astype(BF16)
        images = dot(built, sketch_t, 1, 1).astype(BF16)
        term = dot(images, built, 0, 0)
        total = term if total is None else total + term
    return total


def project_kernel(m_ref, before_ref, core_ref, sketch_ref, out_ref, carry_ref):
    m_value = m_ref[:SKETCH, :RANK]
    inverse = inverse_factor(symmetric_gram(m_value, before_ref[:SKETCH, :RANK]))
    carry = dot(inverse, m_value.astype(F32), 1, 0, lax.Precision.HIGHEST).astype(BF16)
    carry_ref[...] = carry
    out_ref[...] = jnp.zeros((ROWS, LANES), BF16)
    out_ref[:SKETCH, :RANK] = gram_term(core_ref, carry, sketch_ref[:SKETCH, :RANK]).astype(BF16)


def first_project_kernel(upper_ref, rest_ref, before_ref, core_ref, sketch_ref, out_ref, carry_ref, m0_ref):
    s = before_ref[:SKETCH, :RANK]
    sa, sb, sc, sd = s[:, :128], s[:, 128:256], s[:, 256:384], s[:, 384:400]
    a = upper_ref[:, :RANK]
    b = rest_ref[:, :256]
    c = rest_ref[:, 256:384]
    b_end = rest_ref[:, 384:400]
    c_end = rest_ref[:, 400:416]
    d_end = rest_ref[:16, 416:432]
    over_a = dot(sa, a, 1, 0)
    m0_ref[:, :128] = over_a[:, :128] + dot(s[:, 128:], a[:, 128:], 1, 1)
    m0_ref[:, 128:256] = (
        over_a[:, 128:256] + dot(sb, b[:, :128], 1, 0) + dot(sc, b[:, 128:], 1, 1) + dot(sd, b_end, 1, 1)
    )
    m0_ref[:, 256:384] = over_a[:, 256:384] + dot(sb, b[:, 128:], 1, 0) + dot(sc, c, 1, 0) + dot(sd, c_end, 1, 1)
    m0_ref[:, 384:400] = over_a[:, 384:400] + dot(sb, b_end, 1, 0) + dot(sc, c_end, 1, 0) + dot(sd, d_end, 1, 0)
    m_value = m0_ref[...]
    high = m_value.astype(BF16)
    low = (m_value - high.astype(F32)).astype(BF16)
    inverse = inverse_factor(symmetric_gram(high, s) + symmetric_gram(low, s))
    carry = dot(inverse, m_value, 1, 0, lax.Precision.HIGHEST).astype(BF16)
    carry_ref[...] = carry
    out_ref[...] = jnp.zeros((ROWS, LANES), BF16)
    out_ref[:SKETCH, :RANK] = gram_term(core_ref, carry, sketch_ref[:SKETCH, :RANK]).astype(BF16)


def last_project_kernel(
    x_ref, m_ref, before_ref, core_ref, right_ref, left_ref, carry_1_ref, carry_2_ref,
    third_ref, second_ref, first_ref, out_ref, images_ref,
):
    out_ref[...] = jnp.zeros((ROWS, LANES), BF16)

    @pl.when(x_ref[0] == 3)
    def _():
        m_value = m_ref[:SKETCH, :RANK]
        inverse = inverse_factor(symmetric_gram(m_value, before_ref[:SKETCH, :RANK]))
        carry = dot(inverse, m_value.astype(F32), 1, 0, lax.Precision.HIGHEST).astype(BF16)
        total = None
        for i in range(core_ref.shape[0]):
            built = dot(carry, core_ref[i], 1, 0).astype(BF16)
            images = dot(built, right_ref[...], 1, 0)
            images_ref[i] = images
            term = dot(images.astype(BF16), built, 0, 0)
            total = term if total is None else total + term
        out_ref[:SKETCH, :RANK] = total.astype(BF16)

    def images_of(carry, dim, sketch_t):
        for i in range(core_ref.shape[0]):
            built = dot(carry, core_ref[i], dim, 0).astype(BF16)
            images_ref[i] = dot(built, sketch_t, 1, 1)

    @pl.when(x_ref[0] == 2)
    def _():
        images_of(carry_2_ref[...], 1, first_ref[:SKETCH, :RANK])

    @pl.when(x_ref[0] == 1)
    def _():
        images_of(carry_1_ref[...], 1, second_ref[:SKETCH, :RANK])

    @pl.when(x_ref[0] == 0)
    def _():
        images_of(left_ref[...].astype(BF16), 0, third_ref[:SKETCH, :RANK])


def final_kernel(
    scale, x_ref, m_0_ref, m_1_ref, m_2_ref, m_3_ref, third_ref, second_ref, first_ref, right_ref,
    images_ref, frames_ref, interface_ref, m_ref, gram_ref,
):
    def split_gram(m_value, sketch_t):
        high = m_value.astype(BF16)
        low = (m_value - high.astype(F32)).astype(BF16)
        return symmetric_gram(high, sketch_t) + symmetric_gram(low, sketch_t)

    @pl.when(x_ref[0] == 0)
    def _():
        m_ref[...] = m_0_ref[...]
        gram_ref[...] = split_gram(m_0_ref[...], third_ref[:SKETCH, :RANK])

    @pl.when(x_ref[0] == 1)
    def _():
        m_ref[...] = m_1_ref[:SKETCH, :RANK].astype(F32)
        gram_ref[...] = symmetric_gram(m_1_ref[:SKETCH, :RANK], second_ref[:SKETCH, :RANK])

    @pl.when(x_ref[0] == 2)
    def _():
        m_ref[...] = m_2_ref[:SKETCH, :RANK].astype(F32)
        gram_ref[...] = symmetric_gram(m_2_ref[:SKETCH, :RANK], first_ref[:SKETCH, :RANK])

    @pl.when(x_ref[0] == 3)
    def _():
        m_value = m_3_ref[:SKETCH, :RANK]
        m_ref[...] = m_value.astype(F32)
        gram_ref[...] = 0.5 * (dot(m_value, right_ref[...], 1, 0) + dot(right_ref[...], m_value, 0, 1))

    inverse = inverse_factor(gram_ref[...])
    interface_ref[...] = dot(inverse, m_ref[...], 1, 0, lax.Precision.HIGHEST)
    for i in range(images_ref.shape[0]):
        orth = dot(images_ref[i], inverse, 1, 1, lax.Precision.HIGHEST)
        frames_ref[i] = (orth * scale).astype(BF16)


def call(kernel, *operands, out, scalar=False, scratch=()):
    specs = [pl.BlockSpec(memory_space=pltpu.VMEM) for _ in operands]
    if scalar:
        specs[0] = pl.BlockSpec(memory_space=pltpu.SMEM)
    outs = [jax.ShapeDtypeStruct(shape, kind) for shape, kind in out]
    return pl.pallas_call(
        kernel,
        out_shape=outs,
        in_specs=specs,
        out_specs=[pl.BlockSpec(memory_space=pltpu.VMEM) for _ in outs],
        scratch_shapes=[pltpu.VMEM(shape, F32) for shape in scratch],
        compiler_params=PARAMS,
    )(*operands)


PAYLOAD = ((ROWS, LANES), BF16)


def everywhere(shard, axes, count, groups=None):
    copies = jnp.broadcast_to(shard, (count, *shard.shape))
    return lax.all_to_all(copies, axes, 0, 0, axis_index_groups=groups, tiled=True)


def added(pieces):
    return pieces.astype(F32).sum(axis=0).astype(BF16)


def plane_sum(value, near, far):
    tiles = value.reshape(near, ROWS // near, LANES)
    shard = added(lax.all_to_all(tiles, ("y", "c"), 0, 0, tiled=True))
    return added(everywhere(shard, "z", far))


def whole_pair(shard, pairs, near):
    groups = [[x * near + d for x in pair for d in range(near)] for pair in pairs]
    rows = everywhere(shard, ("x", "y", "c"), 2 * near, groups)
    return rows[:near].reshape(ROWS, LANES), rows[near:].reshape(ROWS, LANES)


def body(train_cores, sketch_cores, left_interface, right_sketch):
    near = lax.axis_size("y") * lax.axis_size("c")
    far = lax.axis_size("z")
    plane = lax.axis_index("x")
    plane_ref = plane.astype(jnp.int32).reshape(1)
    core = jnp.swapaxes(train_cores[0], 0, 1)
    sketch_core = jnp.swapaxes(sketch_cores[0], 0, 1)
    modes = core.shape[0]
    frame_scale = math.sqrt(SKETCH * modes * lax.axis_size(MODE))
    left_t = left_interface.T

    def first_of(value, pairs):
        return whole_pair(plane_sum(value, near, far), pairs, near)[0]

    term, rest = call(
        first_kernel, plane_ref, core, sketch_core, right_sketch, left_t, out=[PAYLOAD, PAYLOAD], scalar=True
    )
    first = first_of(term, ((3, 2), (0, 1)))
    (term,) = call(sketch_kernel, core, sketch_core, first, out=[PAYLOAD])
    second = first_of(term, ((2, 1), (3, 0)))
    (term,) = call(last_sketch_kernel, plane_ref, core, sketch_core, second, rest, out=[PAYLOAD], scalar=True)
    third, rest = whole_pair(plane_sum(term, near, far), ((1, 0), (3, 2)), near)

    carry_kind = ((SKETCH, RANK), BF16)
    term, carry_1, m_0 = call(
        first_project_kernel, first, rest, third, core, second, out=[PAYLOAD, carry_kind, ((SKETCH, RANK), F32)]
    )
    m_1 = first_of(term, ((1, 2), (0, 3)))
    term, carry_2 = call(project_kernel, m_1, second, core, first, out=[PAYLOAD, carry_kind])
    m_2 = first_of(term, ((2, 3), (0, 1)))
    term, images = call(
        last_project_kernel, plane_ref, m_2, first, core, right_sketch, left_t, carry_1, carry_2,
        third, second, first, out=[PAYLOAD, ((modes, SKETCH, SKETCH), F32)], scalar=True,
    )
    m_3 = everywhere(plane_sum(term, near, far), ("y", "c"), near).reshape(ROWS, LANES)

    def finish(*refs):
        final_kernel(frame_scale, *refs)

    frames, interface = call(
        finish, plane_ref, m_0, m_1, m_2, m_3, third, second, first, right_sketch, images,
        out=[((modes, SKETCH, SKETCH), BF16), ((SKETCH, RANK), F32)], scalar=True,
        scratch=((SKETCH, RANK), (SKETCH, SKETCH)),
    )
    return (jnp.swapaxes(frames, 0, 1)[None], interface[None])


def solution(mesh):
    split = Mesh(mesh.devices.reshape(4, 16, 2, 4), AXES)
    placed = (P("x", None, MODE, None), P("x", None, MODE, None), P(), P())
    return jax.shard_map(
        body,
        mesh=split,
        in_specs=placed,
        out_specs=(P("x", None, MODE, None), P("x", None, None)),
        check_vma=False,
    )
```

```python
import math

import jax
import jax.numpy as jnp
from jax import lax
from jax.experimental import pallas as pl
from jax.experimental.pallas import tpu as pltpu
from jax.sharding import Mesh
from jax.sharding import PartitionSpec as P

AXES = ("y", "zh", "zl", "c", "x")
MODE = ("y", "zh", "zl", "c")
SIZES = (4, 8, 2, 2, 4)
NEAR = tuple((y, zl, c) for y in range(4) for zl in range(2) for c in range(2))
FAR = 8
RANK = 400
SKETCH = 100
ROWS = 128
LANES = 512
F32 = jnp.float32
BF16 = jnp.bfloat16
PARAMS = pltpu.CompilerParams(vmem_limit_bytes=24 * 1024 * 1024)


def dot(a, b, ca, cb, precision=None):
    return lax.dot_general(
        a, b, (((ca,), (cb,)), ((), ())), precision=precision, preferred_element_type=F32
    )


def inverse_factor(gram):
    size = gram.shape[0]
    count = -(-size // 8)
    padded = jnp.pad(gram, ((0, count * 8 - size), (0, 128 - size)))
    tiles = [padded[8 * t : 8 * t + 8] for t in range(count)]
    lane = lax.broadcasted_iota(jnp.int32, (8, 128), 1)
    sub = lax.broadcasted_iota(jnp.int32, (8, 128), 0)

    def column(tile, j):
        return jnp.broadcast_to(tile[:, j : j + 1], (8, 128))

    def line(tile, s):
        return jnp.broadcast_to(tile[s : s + 1], (8, 128))

    for own in range(count):
        base = 8 * own
        width = min(8, size - base)
        step = lane - base
        columns = {t: [column(tiles[t], base + c) for c in range(width)] for t in range(own, count)}
        head = columns[own]
        scales, leads = [], []
        tile = tiles[own]
        for s in range(width):
            scales.append(1.0 / line(head[s], s))
            leads.append([line(head[c], s) if c > s else None for c in range(width)])
            factor = jnp.where(sub > s, head[s] * scales[s], 0.0)
            pivot = jnp.where(step == s, 1.0, line(tile, s))
            tile = jnp.where((step == s) & (sub > s), 0.0, tile) - factor * pivot
            for c in range(s + 1, width):
                head[c] = head[c] - factor * leads[s][c]
        tiles[own] = tile
        reduced = jnp.where((step > sub) & (step < 8), 0.0, jnp.where(step == sub, 1.0, tile))
        pivots = [line(reduced, s) for s in range(width)]
        for t in range(own + 1, count):
            col = columns[t]
            new = jnp.where((step >= 0) & (step < 8), 0.0, tiles[t])
            for s in range(width):
                factor = col[s] * scales[s]
                new = new - factor * pivots[s]
                for c in range(s + 1, width):
                    col[c] = col[c] - factor * leads[s][c]
            tiles[t] = new
    done = []
    for t in range(count):
        row = sub + 8 * t
        diagonal = jnp.sum(jnp.where(lane == row, tiles[t], 0.0), axis=1, keepdims=True)
        lower = jnp.where(lane < row, tiles[t], jnp.where(lane == row, 1.0, 0.0))
        done.append(lower * lax.rsqrt(diagonal))
    return jnp.concatenate(done, axis=0)[:size, :size]


def symmetric_gram(m_value, sketch_t):
    return 0.5 * (dot(m_value, sketch_t, 1, 1) + dot(sketch_t, m_value, 1, 1))


def sketch_term(core_ref, sketch_core_ref, sketch, dim):
    total = None
    for i in range(core_ref.shape[0]):
        partial = dot(core_ref[i], sketch, 1, dim).astype(BF16)
        term = dot(sketch_core_ref[i], partial, 1, 1)
        total = term if total is None else total + term
    return total


def first_kernel(x_ref, core_ref, sketch_core_ref, right_ref, left_ref, out_ref, rest_ref):
    out_ref[...] = jnp.zeros((ROWS, LANES), BF16)
    rest_ref[...] = jnp.zeros((ROWS, LANES), BF16)

    @pl.when(x_ref[0] != 0)
    def _():
        out_ref[:SKETCH, :RANK] = sketch_term(
            core_ref, sketch_core_ref, right_ref[...], 0
        ).astype(BF16)

    @pl.when(x_ref[0] == 0)
    def _():
        square = None
        left_t = left_ref[...].astype(BF16)
        for i in range(core_ref.shape[0]):
            built = dot(left_t, core_ref[i], 0, 0).astype(BF16)
            term = dot(built, built, 0, 0)
            square = term if square is None else square + term
        square = square.astype(BF16)
        out_ref[:, :RANK] = square[:128]
        rest_ref[:, :256] = square[128:256, 128:384]
        rest_ref[:, 256:384] = square[256:384, 256:384]
        rest_ref[:, 384:400] = square[128:256, 384:400]
        rest_ref[:, 400:416] = square[256:384, 384:400]
        rest_ref[:16, 416:432] = square[384:400, 384:400]


def sketch_kernel(core_ref, sketch_core_ref, sketch_ref, out_ref):
    out_ref[...] = jnp.zeros((ROWS, LANES), BF16)
    out_ref[:SKETCH, :RANK] = sketch_term(
        core_ref, sketch_core_ref, sketch_ref[:SKETCH, :RANK], 1
    ).astype(BF16)


def last_sketch_kernel(x_ref, core_ref, sketch_core_ref, sketch_ref, rest_ref, out_ref):
    @pl.when(x_ref[0] == 0)
    def _():
        out_ref[...] = rest_ref[...]

    @pl.when(x_ref[0] != 0)
    def _():
        sketch_kernel(core_ref, sketch_core_ref, sketch_ref, out_ref)


def gram_term(core_ref, carry_low, sketch_t):
    total = None
    for i in range(core_ref.shape[0]):
        built = dot(carry_low, core_ref[i], 1, 0).astype(BF16)
        images = dot(built, sketch_t, 1, 1).astype(BF16)
        term = dot(images, built, 0, 0)
        total = term if total is None else total + term
    return total


def project_kernel(m_ref, before_ref, core_ref, sketch_ref, out_ref, carry_ref):
    m_value = m_ref[:SKETCH, :RANK]
    inverse = inverse_factor(symmetric_gram(m_value, before_ref[:SKETCH, :RANK]))
    carry = dot(inverse, m_value.astype(F32), 1, 0, lax.Precision.HIGHEST).astype(BF16)
    carry_ref[...] = carry
    out_ref[...] = jnp.zeros((ROWS, LANES), BF16)
    out_ref[:SKETCH, :RANK] = gram_term(core_ref, carry, sketch_ref[:SKETCH, :RANK]).astype(BF16)


def first_project_kernel(upper_ref, rest_ref, before_ref, core_ref, sketch_ref, out_ref, carry_ref, m0_ref):
    s = before_ref[:SKETCH, :RANK]
    sa, sb, sc, sd = s[:, :128], s[:, 128:256], s[:, 256:384], s[:, 384:400]
    a = upper_ref[:, :RANK]
    b = rest_ref[:, :256]
    c = rest_ref[:, 256:384]
    b_end = rest_ref[:, 384:400]
    c_end = rest_ref[:, 400:416]
    d_end = rest_ref[:16, 416:432]
    over_a = dot(sa, a, 1, 0)
    m0_ref[:, :128] = over_a[:, :128] + dot(s[:, 128:], a[:, 128:], 1, 1)
    m0_ref[:, 128:256] = (
        over_a[:, 128:256] + dot(sb, b[:, :128], 1, 0) + dot(sc, b[:, 128:], 1, 1) + dot(sd, b_end, 1, 1)
    )
    m0_ref[:, 256:384] = over_a[:, 256:384] + dot(sb, b[:, 128:], 1, 0) + dot(sc, c, 1, 0) + dot(sd, c_end, 1, 1)
    m0_ref[:, 384:400] = over_a[:, 384:400] + dot(sb, b_end, 1, 0) + dot(sc, c_end, 1, 0) + dot(sd, d_end, 1, 0)
    m_value = m0_ref[...]
    high = m_value.astype(BF16)
    low = (m_value - high.astype(F32)).astype(BF16)
    inverse = inverse_factor(symmetric_gram(high, s) + symmetric_gram(low, s))
    carry = dot(inverse, m_value, 1, 0, lax.Precision.HIGHEST).astype(BF16)
    carry_ref[...] = carry
    out_ref[...] = jnp.zeros((ROWS, LANES), BF16)
    out_ref[:SKETCH, :RANK] = gram_term(core_ref, carry, sketch_ref[:SKETCH, :RANK]).astype(BF16)


def last_project_kernel(
    x_ref, m_ref, before_ref, core_ref, right_ref, left_ref, carry_1_ref, carry_2_ref,
    third_ref, second_ref, first_ref, out_ref, images_ref,
):
    out_ref[...] = jnp.zeros((ROWS, LANES), BF16)

    @pl.when(x_ref[0] == 3)
    def _():
        m_value = m_ref[:SKETCH, :RANK]
        inverse = inverse_factor(symmetric_gram(m_value, before_ref[:SKETCH, :RANK]))
        carry = dot(inverse, m_value.astype(F32), 1, 0, lax.Precision.HIGHEST).astype(BF16)
        total = None
        for i in range(core_ref.shape[0]):
            built = dot(carry, core_ref[i], 1, 0).astype(BF16)
            images = dot(built, right_ref[...], 1, 0)
            images_ref[i] = images
            term = dot(images.astype(BF16), built, 0, 0)
            total = term if total is None else total + term
        out_ref[:SKETCH, :RANK] = total.astype(BF16)

    def images_of(carry, dim, sketch_t):
        for i in range(core_ref.shape[0]):
            built = dot(carry, core_ref[i], dim, 0).astype(BF16)
            images_ref[i] = dot(built, sketch_t, 1, 1)

    @pl.when(x_ref[0] == 2)
    def _():
        images_of(carry_2_ref[...], 1, first_ref[:SKETCH, :RANK])

    @pl.when(x_ref[0] == 1)
    def _():
        images_of(carry_1_ref[...], 1, second_ref[:SKETCH, :RANK])

    @pl.when(x_ref[0] == 0)
    def _():
        images_of(left_ref[...].astype(BF16), 0, third_ref[:SKETCH, :RANK])


def final_kernel(
    scale, x_ref, m_0_ref, m_1_ref, m_2_ref, m_3_ref, third_ref, second_ref, first_ref, right_ref,
    images_ref, frames_ref, interface_ref, m_ref, gram_ref,
):
    def split_gram(m_value, sketch_t):
        high = m_value.astype(BF16)
        low = (m_value - high.astype(F32)).astype(BF16)
        return symmetric_gram(high, sketch_t) + symmetric_gram(low, sketch_t)

    @pl.when(x_ref[0] == 0)
    def _():
        m_ref[...] = m_0_ref[...]
        gram_ref[...] = split_gram(m_0_ref[...], third_ref[:SKETCH, :RANK])

    @pl.when(x_ref[0] == 1)
    def _():
        m_ref[...] = m_1_ref[:SKETCH, :RANK].astype(F32)
        gram_ref[...] = symmetric_gram(m_1_ref[:SKETCH, :RANK], second_ref[:SKETCH, :RANK])

    @pl.when(x_ref[0] == 2)
    def _():
        m_ref[...] = m_2_ref[:SKETCH, :RANK].astype(F32)
        gram_ref[...] = symmetric_gram(m_2_ref[:SKETCH, :RANK], first_ref[:SKETCH, :RANK])

    @pl.when(x_ref[0] == 3)
    def _():
        m_value = m_3_ref[:SKETCH, :RANK]
        m_ref[...] = m_value.astype(F32)
        gram_ref[...] = 0.5 * (dot(m_value, right_ref[...], 1, 0) + dot(right_ref[...], m_value, 0, 1))

    inverse = inverse_factor(gram_ref[...])
    interface_ref[...] = dot(inverse, m_ref[...], 1, 0, lax.Precision.HIGHEST)
    for i in range(images_ref.shape[0]):
        orth = dot(images_ref[i], inverse, 1, 1, lax.Precision.HIGHEST)
        frames_ref[i] = (orth * scale).astype(BF16)


def call(kernel, *operands, out, scalar=False, scratch=()):
    specs = [pl.BlockSpec(memory_space=pltpu.VMEM) for _ in operands]
    if scalar:
        specs[0] = pl.BlockSpec(memory_space=pltpu.SMEM)
    outs = [jax.ShapeDtypeStruct(shape, kind) for shape, kind in out]
    return pl.pallas_call(
        kernel,
        out_shape=outs,
        in_specs=specs,
        out_specs=[pl.BlockSpec(memory_space=pltpu.VMEM) for _ in outs],
        scratch_shapes=[pltpu.VMEM(shape, F32) for shape in scratch],
        compiler_params=PARAMS,
    )(*operands)


PAYLOAD = ((ROWS, LANES), BF16)


def device(place, zh, x):
    y, zl, c = place
    if zh >= FAR // 2:
        zl, c = 1 - zl, 1 - c
    index = 0
    for at, size in zip((y, zh, zl, c, x), SIZES):
        index = index * size + at
    return index


def near_groups(planes):
    return [[device(place, zh, x) for place in NEAR] for x in planes for zh in range(FAR)]


def far_groups(planes):
    return [[device(place, zh, x) for x in planes for zh in range(FAR)] for place in NEAR]


def everywhere(shard, groups):
    copies = jnp.broadcast_to(shard, (len(groups[0]), *shard.shape))
    return lax.all_to_all(copies, AXES, 0, 0, axis_index_groups=groups, tiled=True)


def shard_sum(value):
    tiles = value.reshape(len(NEAR), ROWS // len(NEAR), LANES)
    return added(lax.all_to_all(tiles, AXES, 0, 0, axis_index_groups=near_groups(range(4)), tiled=True))


def added(pieces):
    return pieces.astype(F32).sum(axis=0).astype(BF16)


def paired(value, pairs):
    spare = [x for x in range(4) if not any(x in pair for pair in pairs)]
    groups = [group for pair in pairs for group in far_groups(pair)] + near_groups(spare)
    pieces = everywhere(shard_sum(value), groups)
    return pieces[:FAR], pieces[FAR:]


def whole(shard):
    return everywhere(shard, near_groups(range(4)))


def body(train_cores, sketch_cores, left_interface, right_sketch):
    plane = lax.axis_index("x")
    plane_ref = plane.astype(jnp.int32).reshape(1)
    core = jnp.swapaxes(train_cores[0], 0, 1)
    sketch_core = jnp.swapaxes(sketch_cores[0], 0, 1)
    modes = core.shape[0]
    frame_scale = math.sqrt(SKETCH * modes * lax.axis_size(MODE))
    left_t = left_interface.T

    def full(shard):
        return whole(shard).reshape(ROWS, LANES)

    term, rest = call(
        first_kernel, plane_ref, core, sketch_core, right_sketch, left_t, out=[PAYLOAD, PAYLOAD], scalar=True
    )
    first = full(added(paired(term, ((3, 2), (0, 1)))[0]))
    (term,) = call(sketch_kernel, core, sketch_core, first, out=[PAYLOAD])
    second = full(added(paired(term, ((2, 1),))[0]))
    (term,) = call(last_sketch_kernel, plane_ref, core, sketch_core, second, rest, out=[PAYLOAD], scalar=True)
    both = paired(term, ((1, 0),))
    arrived = whole(jnp.concatenate([added(both[0]), added(both[1])], axis=0))
    third = arrived[:, :8].reshape(ROWS, LANES)
    rest = arrived[:, 8:].reshape(ROWS, LANES)

    carry_kind = ((SKETCH, RANK), BF16)
    term, carry_1, m_0 = call(
        first_project_kernel, first, rest, third, core, second, out=[PAYLOAD, carry_kind, ((SKETCH, RANK), F32)]
    )
    m_1 = full(added(paired(term, ((1, 2),))[0]))
    term, carry_2 = call(project_kernel, m_1, second, core, first, out=[PAYLOAD, carry_kind])
    m_2 = full(added(paired(term, ((2, 3),))[0]))
    term, images = call(
        last_project_kernel, plane_ref, m_2, first, core, right_sketch, left_t, carry_1, carry_2,
        third, second, first, out=[PAYLOAD, ((modes, SKETCH, SKETCH), F32)], scalar=True,
    )
    alone = [group for x in range(4) for group in far_groups((x,))]
    m_3 = full(added(everywhere(shard_sum(term), alone)))

    def finish(*refs):
        final_kernel(frame_scale, *refs)

    frames, interface = call(
        finish, plane_ref, m_0, m_1, m_2, m_3, third, second, first, right_sketch, images,
        out=[((modes, SKETCH, SKETCH), BF16), ((SKETCH, RANK), F32)], scalar=True,
        scratch=((SKETCH, RANK), (SKETCH, SKETCH)),
    )
    return (jnp.swapaxes(frames, 0, 1)[None], interface[None])


def solution(mesh):
    split = Mesh(mesh.devices.reshape(*SIZES), AXES)
    placed = (P("x", None, MODE, None), P("x", None, MODE, None), P(), P())
    return jax.shard_map(
        body,
        mesh=split,
        in_specs=placed,
        out_specs=(P("x", None, MODE, None), P("x", None, None)),
        check_vma=False,
    )
```

```python
import math

import jax
import jax.numpy as jnp
from jax import lax
from jax.experimental import pallas as pl
from jax.experimental.pallas import tpu as pltpu
from jax.sharding import Mesh
from jax.sharding import PartitionSpec as P

AXES = ("y", "zh", "zl", "c", "x")
MODE = ("y", "zh", "zl", "c")
SIZES = (4, 8, 2, 2, 4)
NEAR = tuple((y, zl, c) for y in range(4) for zl in range(2) for c in range(2))
FAR = 8
RANK = 400
SKETCH = 100
ROWS = 128
LANES = 512
F32 = jnp.float32
BF16 = jnp.bfloat16
PARAMS = pltpu.CompilerParams(vmem_limit_bytes=24 * 1024 * 1024)


def dot(a, b, ca, cb):
    return lax.dot_general(a, b, (((ca,), (cb,)), ((), ())), preferred_element_type=F32)


def inverse_factor(gram):
    size = gram.shape[0]
    count = -(-size // 8)
    padded = jnp.pad(gram, ((0, count * 8 - size), (0, 128 - size)))
    tiles = [padded[8 * t : 8 * t + 8] for t in range(count)]
    lane = lax.broadcasted_iota(jnp.int32, (8, 128), 1)
    sub = lax.broadcasted_iota(jnp.int32, (8, 128), 0)

    none = jnp.where(lane >= 128, 1.0, 0.0)

    def column(tile, j):
        return jnp.broadcast_to(tile[:, j : j + 1], (8, 128))

    def line(tile, s):
        return jnp.broadcast_to(tile[s : s + 1], (8, 128))

    for own in range(count):
        base = 8 * own
        width = min(8, size - base)
        step = lane - base
        columns = {t: [column(tiles[t], base + c) for c in range(width)] for t in range(own, count)}
        head = [value + none for value in columns[own]]
        scales, leads = [], []
        tile = tiles[own]
        for s in range(width):
            scales.append(line(1.0 / head[s], s))
            leads.append([line(head[c], s) if c > s else None for c in range(width)])
            factor = jnp.where(sub > s, head[s] * scales[s], 0.0)
            pivot = jnp.where(step == s, 1.0, line(tile, s))
            tile = jnp.where((step == s) & (sub > s), 0.0, tile) - factor * pivot
            for c in range(s + 1, width):
                head[c] = head[c] - factor * leads[s][c]
        tiles[own] = tile
        reduced = jnp.where((step > sub) & (step < 8), 0.0, jnp.where(step == sub, 1.0, tile))
        pivots = [line(reduced, s) for s in range(width)]
        for t in range(own + 1, count):
            col = columns[t]
            new = jnp.where((step >= 0) & (step < 8), 0.0, tiles[t])
            for s in range(width):
                factor = col[s] * scales[s]
                new = new - factor * pivots[s]
                for c in range(s + 1, width):
                    col[c] = col[c] - factor * leads[s][c]
            tiles[t] = new
    done = []
    for t in range(count):
        row = sub + 8 * t
        diagonal = jnp.sum(jnp.where(lane == row, tiles[t], 0.0), axis=1, keepdims=True)
        lower = jnp.where(lane < row, tiles[t], jnp.where(lane == row, 1.0, 0.0))
        done.append(lower * lax.rsqrt(diagonal))
    return jnp.concatenate(done, axis=0)[:size, :size]


def halves(value):
    high = value.astype(BF16)
    return high, (value - high.astype(F32)).astype(BF16)


def wide_dot(a, b, ca, cb):
    a_high, a_low = halves(a)
    b_high, b_low = halves(b)
    return dot(a_high, b_high, ca, cb) + (dot(a_high, b_low, ca, cb) + dot(a_low, b_high, ca, cb))


def left_wide_dot(a, b, ca, cb):
    a_high, a_low = halves(a)
    return dot(a_high, b, ca, cb) + dot(a_low, b, ca, cb)


def symmetric_gram(m_value, sketch_t):
    return 0.5 * (dot(m_value, sketch_t, 1, 1) + dot(sketch_t, m_value, 1, 1))


def sketch_term(core_ref, sketch_core_ref, sketch, dim):
    total = None
    for i in range(core_ref.shape[0]):
        partial = dot(core_ref[i], sketch, 1, dim).astype(BF16)
        term = dot(sketch_core_ref[i], partial, 1, 1)
        total = term if total is None else total + term
    return total


def first_kernel(x_ref, core_ref, sketch_core_ref, right_ref, left_ref, out_ref, rest_ref):
    out_ref[...] = jnp.zeros((ROWS, LANES), BF16)
    rest_ref[...] = jnp.zeros((ROWS, LANES), BF16)

    @pl.when(x_ref[0] != 0)
    def _():
        out_ref[:SKETCH, :RANK] = sketch_term(
            core_ref, sketch_core_ref, right_ref[...], 0
        ).astype(BF16)

    @pl.when(x_ref[0] == 0)
    def _():
        square = None
        left_t = left_ref[...].astype(BF16)
        for i in range(core_ref.shape[0]):
            built = dot(left_t, core_ref[i], 0, 0).astype(BF16)
            term = dot(built, built, 0, 0)
            square = term if square is None else square + term
        square = square.astype(BF16)
        out_ref[:, :RANK] = square[:128]
        rest_ref[:, :256] = square[128:256, 128:384]
        rest_ref[:, 256:384] = square[256:384, 256:384]
        rest_ref[:, 384:400] = square[128:256, 384:400]
        rest_ref[:, 400:416] = square[256:384, 384:400]
        rest_ref[:16, 416:432] = square[384:400, 384:400]


def sketch_kernel(core_ref, sketch_core_ref, sketch_ref, out_ref):
    out_ref[...] = jnp.zeros((ROWS, LANES), BF16)
    out_ref[:SKETCH, :RANK] = sketch_term(
        core_ref, sketch_core_ref, sketch_ref[:SKETCH, :RANK], 1
    ).astype(BF16)


def last_sketch_kernel(x_ref, core_ref, sketch_core_ref, sketch_ref, rest_ref, out_ref):
    @pl.when(x_ref[0] == 0)
    def _():
        out_ref[...] = rest_ref[...]

    @pl.when(x_ref[0] != 0)
    def _():
        sketch_kernel(core_ref, sketch_core_ref, sketch_ref, out_ref)


def gram_term(core_ref, carry_low, sketch_t):
    total = None
    for i in range(core_ref.shape[0]):
        built = dot(carry_low, core_ref[i], 1, 0).astype(BF16)
        images = dot(built, sketch_t, 1, 1).astype(BF16)
        term = dot(images, built, 0, 0)
        total = term if total is None else total + term
    return total


def project_kernel(m_ref, before_ref, core_ref, sketch_ref, out_ref, carry_ref):
    m_value = m_ref[:SKETCH, :RANK]
    inverse = inverse_factor(symmetric_gram(m_value, before_ref[:SKETCH, :RANK]))
    carry = left_wide_dot(inverse, m_value, 1, 0).astype(BF16)
    carry_ref[...] = carry
    out_ref[...] = jnp.zeros((ROWS, LANES), BF16)
    out_ref[:SKETCH, :RANK] = gram_term(core_ref, carry, sketch_ref[:SKETCH, :RANK]).astype(BF16)


def first_project_kernel(upper_ref, rest_ref, before_ref, core_ref, sketch_ref, out_ref, carry_ref, m0_ref):
    s = before_ref[:SKETCH, :RANK]
    sa, sb, sc, sd = s[:, :128], s[:, 128:256], s[:, 256:384], s[:, 384:400]
    a = upper_ref[:, :RANK]
    b = rest_ref[:, :256]
    c = rest_ref[:, 256:384]
    b_end = rest_ref[:, 384:400]
    c_end = rest_ref[:, 400:416]
    d_end = rest_ref[:16, 416:432]
    over_a = dot(sa, a, 1, 0)
    m0_ref[:, :128] = over_a[:, :128] + dot(s[:, 128:], a[:, 128:], 1, 1)
    m0_ref[:, 128:256] = (
        over_a[:, 128:256] + dot(sb, b[:, :128], 1, 0) + dot(sc, b[:, 128:], 1, 1) + dot(sd, b_end, 1, 1)
    )
    m0_ref[:, 256:384] = over_a[:, 256:384] + dot(sb, b[:, 128:], 1, 0) + dot(sc, c, 1, 0) + dot(sd, c_end, 1, 1)
    m0_ref[:, 384:400] = over_a[:, 384:400] + dot(sb, b_end, 1, 0) + dot(sc, c_end, 1, 0) + dot(sd, d_end, 1, 0)
    m_value = m0_ref[...]
    high, low = halves(m_value)
    inverse = inverse_factor(symmetric_gram(high, s) + symmetric_gram(low, s))
    carry = wide_dot(inverse, m_value, 1, 0).astype(BF16)
    carry_ref[...] = carry
    out_ref[...] = jnp.zeros((ROWS, LANES), BF16)
    out_ref[:SKETCH, :RANK] = gram_term(core_ref, carry, sketch_ref[:SKETCH, :RANK]).astype(BF16)


def last_project_kernel(
    x_ref, m_ref, before_ref, core_ref, right_ref, left_ref, carry_1_ref, carry_2_ref,
    third_ref, second_ref, first_ref, out_ref, images_ref,
):
    out_ref[...] = jnp.zeros((ROWS, LANES), BF16)

    @pl.when(x_ref[0] == 3)
    def _():
        m_value = m_ref[:SKETCH, :RANK]
        inverse = inverse_factor(symmetric_gram(m_value, before_ref[:SKETCH, :RANK]))
        carry = left_wide_dot(inverse, m_value, 1, 0).astype(BF16)
        total = None
        for i in range(core_ref.shape[0]):
            built = dot(carry, core_ref[i], 1, 0).astype(BF16)
            images = dot(built, right_ref[...], 1, 0)
            images_ref[i] = images
            term = dot(images.astype(BF16), built, 0, 0)
            total = term if total is None else total + term
        out_ref[:SKETCH, :RANK] = total.astype(BF16)

    def images_of(carry, dim, sketch_t):
        for i in range(core_ref.shape[0]):
            built = dot(carry, core_ref[i], dim, 0).astype(BF16)
            images_ref[i] = dot(built, sketch_t, 1, 1)

    @pl.when(x_ref[0] == 2)
    def _():
        images_of(carry_2_ref[...], 1, first_ref[:SKETCH, :RANK])

    @pl.when(x_ref[0] == 1)
    def _():
        images_of(carry_1_ref[...], 1, second_ref[:SKETCH, :RANK])

    @pl.when(x_ref[0] == 0)
    def _():
        images_of(left_ref[...].astype(BF16), 0, third_ref[:SKETCH, :RANK])


def final_kernel(
    scale, x_ref, m_0_ref, m_1_ref, m_2_ref, m_3_ref, third_ref, second_ref, first_ref, right_ref,
    images_ref, frames_ref, interface_ref, m_ref, gram_ref,
):
    def split_gram(m_value, sketch_t):
        high, low = halves(m_value)
        return symmetric_gram(high, sketch_t) + symmetric_gram(low, sketch_t)

    @pl.when(x_ref[0] == 0)
    def _():
        m_ref[...] = m_0_ref[...]
        gram_ref[...] = split_gram(m_0_ref[...], third_ref[:SKETCH, :RANK])

    @pl.when(x_ref[0] == 1)
    def _():
        m_ref[...] = m_1_ref[:SKETCH, :RANK].astype(F32)
        gram_ref[...] = symmetric_gram(m_1_ref[:SKETCH, :RANK], second_ref[:SKETCH, :RANK])

    @pl.when(x_ref[0] == 2)
    def _():
        m_ref[...] = m_2_ref[:SKETCH, :RANK].astype(F32)
        gram_ref[...] = symmetric_gram(m_2_ref[:SKETCH, :RANK], first_ref[:SKETCH, :RANK])

    @pl.when(x_ref[0] == 3)
    def _():
        m_value = m_3_ref[:SKETCH, :RANK]
        m_ref[...] = m_value.astype(F32)
        gram_ref[...] = 0.5 * (dot(m_value, right_ref[...], 1, 0) + dot(right_ref[...], m_value, 0, 1))

    inverse = inverse_factor(gram_ref[...])
    interface_ref[:, 0, :] = wide_dot(inverse, m_ref[...], 1, 0)
    for i in range(images_ref.shape[0]):
        orth = wide_dot(images_ref[i], inverse, 1, 1)
        frames_ref[:, i, :] = (orth * scale).astype(BF16)


def call(kernel, *operands, out, scalar=False, scratch=()):
    specs = [pl.BlockSpec(memory_space=pltpu.VMEM) for _ in operands]
    if scalar:
        specs[0] = pl.BlockSpec(memory_space=pltpu.SMEM)
    outs = [jax.ShapeDtypeStruct(shape, kind) for shape, kind in out]
    return pl.pallas_call(
        kernel,
        out_shape=outs,
        in_specs=specs,
        out_specs=[pl.BlockSpec(memory_space=pltpu.VMEM) for _ in outs],
        scratch_shapes=[pltpu.VMEM(shape, F32) for shape in scratch],
        compiler_params=PARAMS,
    )(*operands)


PAYLOAD = ((ROWS, LANES), BF16)


def device(place, zh, x):
    y, zl, c = place
    if zh >= FAR // 2:
        zl, c = 1 - zl, 1 - c
    index = 0
    for at, size in zip((y, zh, zl, c, x), SIZES):
        index = index * size + at
    return index


def near_groups(planes):
    return [[device(place, zh, x) for place in NEAR] for x in planes for zh in range(FAR)]


def far_groups(planes):
    return [[device(place, zh, x) for x in planes for zh in range(FAR)] for place in NEAR]


def everywhere(shard, groups):
    copies = jnp.broadcast_to(shard, (len(groups[0]), *shard.shape))
    return lax.all_to_all(copies, AXES, 0, 0, axis_index_groups=groups, tiled=True)


def shard_sum(value):
    tiles = value.reshape(len(NEAR), ROWS // len(NEAR), LANES)
    return added(lax.all_to_all(tiles, AXES, 0, 0, axis_index_groups=near_groups(range(4)), tiled=True))


def added(pieces):
    return pieces.astype(F32).sum(axis=0).astype(BF16)


def paired(value, pairs):
    spare = [x for x in range(4) if not any(x in pair for pair in pairs)]
    groups = [group for pair in pairs for group in far_groups(pair)] + near_groups(spare)
    pieces = everywhere(shard_sum(value), groups)
    return pieces[:FAR], pieces[FAR:]


def whole(shard):
    return everywhere(shard, near_groups(range(4)))


def body(train_cores, sketch_cores, left_interface, right_sketch):
    plane = lax.axis_index("x")
    plane_ref = plane.astype(jnp.int32).reshape(1)
    core = jnp.swapaxes(train_cores[0], 0, 1)
    sketch_core = jnp.swapaxes(sketch_cores[0], 0, 1)
    modes = core.shape[0]
    frame_scale = math.sqrt(SKETCH * modes * lax.axis_size(MODE))
    left_t = left_interface.T

    def full(shard):
        return whole(shard).reshape(ROWS, LANES)

    term, rest = call(
        first_kernel, plane_ref, core, sketch_core, right_sketch, left_t, out=[PAYLOAD, PAYLOAD], scalar=True
    )
    first = full(added(paired(term, ((3, 2), (0, 1)))[0]))
    (term,) = call(sketch_kernel, core, sketch_core, first, out=[PAYLOAD])
    second = full(added(paired(term, ((2, 1),))[0]))
    (term,) = call(last_sketch_kernel, plane_ref, core, sketch_core, second, rest, out=[PAYLOAD], scalar=True)
    both = paired(term, ((1, 0),))
    arrived = whole(jnp.concatenate([added(both[0]), added(both[1])], axis=0))
    third = arrived[:, :8].reshape(ROWS, LANES)
    rest = arrived[:, 8:].reshape(ROWS, LANES)

    carry_kind = ((SKETCH, RANK), BF16)
    term, carry_1, m_0 = call(
        first_project_kernel, first, rest, third, core, second, out=[PAYLOAD, carry_kind, ((SKETCH, RANK), F32)]
    )
    m_1 = full(added(paired(term, ((1, 2),))[0]))
    term, carry_2 = call(project_kernel, m_1, second, core, first, out=[PAYLOAD, carry_kind])
    m_2 = full(added(paired(term, ((2, 3),))[0]))
    term, images = call(
        last_project_kernel, plane_ref, m_2, first, core, right_sketch, left_t, carry_1, carry_2,
        third, second, first, out=[PAYLOAD, ((modes, SKETCH, SKETCH), F32)], scalar=True,
    )
    alone = [group for x in range(4) for group in far_groups((x,))]
    m_3 = full(added(everywhere(shard_sum(term), alone)))

    def finish(*refs):
        final_kernel(frame_scale, *refs)

    frames, interface = call(
        finish, plane_ref, m_0, m_1, m_2, m_3, third, second, first, right_sketch, images,
        out=[((SKETCH, modes, SKETCH), BF16), ((SKETCH, 1, RANK), F32)], scalar=True,
        scratch=((SKETCH, RANK), (SKETCH, SKETCH)),
    )
    return (frames[None], interface.reshape(1, SKETCH, RANK))


def solution(mesh):
    split = Mesh(mesh.devices.reshape(*SIZES), AXES)
    placed = (P("x", None, MODE, None), P("x", None, MODE, None), P(), P())
    return jax.shard_map(
        body,
        mesh=split,
        in_specs=placed,
        out_specs=(P("x", None, MODE, None), P("x", None, None)),
        check_vma=False,
    )
```

```python
import math

import jax
import jax.numpy as jnp
from jax import lax
from jax.experimental import pallas as pl
from jax.experimental.pallas import tpu as pltpu
from jax.sharding import Mesh
from jax.sharding import PartitionSpec as P

AXES = ("y", "zh", "zl", "c", "x")
MODE = ("y", "zh", "zl", "c")
SIZES = (4, 8, 2, 2, 4)
NEAR = tuple((y, zl, c) for y in range(4) for zl in range(2) for c in range(2))
FAR = 8
RANK = 400
SKETCH = 100
ROWS = 128
LANES = 512
MAIN = 384
F32 = jnp.float32
BF16 = jnp.bfloat16
PARAMS = pltpu.CompilerParams(vmem_limit_bytes=24 * 1024 * 1024)


def dot(a, b, ca, cb):
    return lax.dot_general(a, b, (((ca,), (cb,)), ((), ())), preferred_element_type=F32)


def inverse_factor(gram):
    size = gram.shape[0]
    count = -(-size // 8)
    padded = jnp.pad(gram, ((0, count * 8 - size), (0, 128 - size)))
    tiles = [padded[8 * t : 8 * t + 8] for t in range(count)]
    lane = lax.broadcasted_iota(jnp.int32, (8, 128), 1)
    sub = lax.broadcasted_iota(jnp.int32, (8, 128), 0)

    none = jnp.where(lane >= 128, 1.0, 0.0)

    def column(tile, j):
        return jnp.broadcast_to(tile[:, j : j + 1], (8, 128))

    def line(tile, s):
        return jnp.broadcast_to(tile[s : s + 1], (8, 128))

    for own in range(count):
        base = 8 * own
        width = min(8, size - base)
        step = lane - base
        columns = {t: [column(tiles[t], base + c) for c in range(width)] for t in range(own, count)}
        head = [value + none for value in columns[own]]
        scales, leads = [], []
        tile = tiles[own]
        for s in range(width):
            scales.append(line(1.0 / head[s], s))
            leads.append([line(head[c], s) if c > s else None for c in range(width)])
            factor = jnp.where(sub > s, head[s] * scales[s], 0.0)
            pivot = jnp.where(step == s, 1.0, line(tile, s))
            tile = jnp.where((step == s) & (sub > s), 0.0, tile) - factor * pivot
            for c in range(s + 1, width):
                head[c] = head[c] - factor * leads[s][c]
        tiles[own] = tile
        reduced = jnp.where((step > sub) & (step < 8), 0.0, jnp.where(step == sub, 1.0, tile))
        pivots = [line(reduced, s) for s in range(width)]
        for t in range(own + 1, count):
            col = columns[t]
            new = jnp.where((step >= 0) & (step < 8), 0.0, tiles[t])
            for s in range(width):
                factor = col[s] * scales[s]
                new = new - factor * pivots[s]
                for c in range(s + 1, width):
                    col[c] = col[c] - factor * leads[s][c]
            tiles[t] = new
    done = []
    for t in range(count):
        row = sub + 8 * t
        diagonal = jnp.sum(jnp.where(lane == row, tiles[t], 0.0), axis=1, keepdims=True)
        lower = jnp.where(lane < row, tiles[t], jnp.where(lane == row, 1.0, 0.0))
        done.append(lower * lax.rsqrt(diagonal))
    return jnp.concatenate(done, axis=0)[:size, :size]


def halves(value):
    high = value.astype(BF16)
    return high, (value - high.astype(F32)).astype(BF16)


def wide_dot(a, b, ca, cb):
    a_high, a_low = halves(a)
    b_high, b_low = halves(b)
    return dot(a_high, b_high, ca, cb) + (dot(a_high, b_low, ca, cb) + dot(a_low, b_high, ca, cb))


def left_wide_dot(a, b, ca, cb):
    a_high, a_low = halves(a)
    return dot(a_high, b, ca, cb) + dot(a_low, b, ca, cb)


def read(ref):
    return ref[:SKETCH, :MAIN], ref[104:120, :SKETCH]


def write(ref, main, rest):
    ref[...] = jnp.zeros(ref.shape, BF16)
    ref[:SKETCH, :MAIN] = main.astype(BF16)
    ref[104:120, :SKETCH] = rest.astype(BF16)


def symmetric_gram(m_pieces, sketch_pieces):
    main, rest = m_pieces
    sketch, sketch_rest = sketch_pieces
    return 0.5 * (
        dot(main, sketch, 1, 1)
        + dot(rest, sketch_rest, 0, 0)
        + dot(sketch, main, 1, 1)
        + dot(sketch_rest, rest, 0, 0)
    )


def sketch_term(out_ref, core_ref, sketch_core_ref, partial_of):
    total = rest = None
    for i in range(core_ref.shape[0]):
        partial = partial_of(core_ref[i]).astype(BF16)
        term = dot(sketch_core_ref[i], partial[:MAIN], 1, 1)
        end = dot(partial[MAIN:], sketch_core_ref[i], 1, 1)
        total, rest = (term, end) if total is None else (total + term, rest + end)
    write(out_ref, total, rest)


def first_kernel(x_ref, core_ref, sketch_core_ref, right_ref, left_ref, out_ref, rest_ref):
    rest_ref[...] = jnp.zeros((ROWS, MAIN), BF16)

    @pl.when(x_ref[0] != 0)
    def _():
        sketch_term(out_ref, core_ref, sketch_core_ref, lambda core: dot(core, right_ref[...], 1, 0))

    @pl.when(x_ref[0] == 0)
    def _():
        square = None
        left_t = left_ref[...].astype(BF16)
        for i in range(core_ref.shape[0]):
            built = dot(left_t, core_ref[i], 0, 0).astype(BF16)
            term = dot(built, built, 0, 0)
            square = term if square is None else square + term
        square = square.astype(BF16)
        out_ref[:, RANK:] = jnp.zeros((ROWS, LANES - RANK), BF16)
        out_ref[:, :RANK] = square[:128]
        out_ref[:, 400:416] = square[128:256, 384:400]
        out_ref[:, 416:432] = square[256:384, 384:400]
        out_ref[:16, 432:448] = square[384:400, 384:400]
        rest_ref[:, :256] = square[128:256, 128:384]
        rest_ref[:, 256:384] = square[256:384, 256:384]


def sketch_kernel(core_ref, sketch_core_ref, sketch_ref, out_ref):
    sketch, rest = read(sketch_ref)
    sketch_term(
        out_ref,
        core_ref,
        sketch_core_ref,
        lambda core: dot(core[:, :MAIN], sketch, 1, 1) + dot(core[:, MAIN:], rest, 1, 0),
    )


def last_sketch_kernel(x_ref, core_ref, sketch_core_ref, sketch_ref, rest_ref, out_ref):
    @pl.when(x_ref[0] == 0)
    def _():
        out_ref[...] = rest_ref[...]

    @pl.when(x_ref[0] != 0)
    def _():
        sketch_kernel(core_ref, sketch_core_ref, sketch_ref, out_ref)


def gram_term(out_ref, core_ref, carry, images_of, images_ref=None):
    total = rest = None
    for i in range(core_ref.shape[0]):
        built = dot(carry, core_ref[i], 1, 0).astype(BF16)
        images = images_of(built)
        if images_ref is not None:
            images_ref[i] = images
        images = images.astype(BF16)
        term = dot(images, built[:, :MAIN], 0, 0)
        end = dot(built[:, MAIN:], images, 0, 0)
        total, rest = (term, end) if total is None else (total + term, rest + end)
    write(out_ref, total, rest)


def images_with(sketch_ref):
    sketch, rest = read(sketch_ref)
    return lambda built: dot(built[:, :MAIN], sketch, 1, 1) + dot(built[:, MAIN:], rest, 1, 0)


def project(carry_ref, m_ref, before_ref):
    main, rest = read(m_ref)
    inverse = inverse_factor(symmetric_gram((main, rest), read(before_ref)))
    carry_ref[:, :MAIN] = left_wide_dot(inverse, main, 1, 0).astype(BF16)
    carry_ref[:, MAIN:] = left_wide_dot(inverse, rest, 1, 1).astype(BF16)


def project_kernel(m_ref, before_ref, core_ref, sketch_ref, out_ref, carry_ref):
    project(carry_ref, m_ref, before_ref)
    gram_term(out_ref, core_ref, carry_ref[...], images_with(sketch_ref))


def m_0_gram(m_value, sketch, sketch_rest):
    high, low = halves(m_value)
    total = None
    for part in (high, low):
        term = 0.5 * (
            dot(part[:, :MAIN], sketch, 1, 1)
            + dot(part[:, MAIN:], sketch_rest, 1, 0)
            + dot(sketch, part[:, :MAIN], 1, 1)
            + dot(sketch_rest, part[:, MAIN:], 0, 1)
        )
        total = term if total is None else total + term
    return total


def first_project_kernel(upper_ref, rest_ref, before_ref, core_ref, sketch_ref, out_ref, carry_ref, m0_ref):
    s, sd = read(before_ref)
    sa, sb, sc = s[:, :128], s[:, 128:256], s[:, 256:384]
    a = upper_ref[:, :RANK]
    b = rest_ref[:, :256]
    c = rest_ref[:, 256:384]
    b_end = upper_ref[:, 400:416]
    c_end = upper_ref[:, 416:432]
    d_end = upper_ref[:16, 432:448]
    over_a = dot(sa, a, 1, 0)
    m0_ref[:, :128] = over_a[:, :128] + dot(s[:, 128:], a[:, 128:MAIN], 1, 1) + dot(sd, a[:, MAIN:], 0, 1)
    m0_ref[:, 128:256] = (
        over_a[:, 128:256] + dot(sb, b[:, :128], 1, 0) + dot(sc, b[:, 128:], 1, 1) + dot(sd, b_end, 0, 1)
    )
    m0_ref[:, 256:384] = over_a[:, 256:384] + dot(sb, b[:, 128:], 1, 0) + dot(sc, c, 1, 0) + dot(sd, c_end, 0, 1)
    m0_ref[:, 384:400] = over_a[:, 384:400] + dot(sb, b_end, 1, 0) + dot(sc, c_end, 1, 0) + dot(sd, d_end, 0, 0)
    m_value = m0_ref[...]
    inverse = inverse_factor(m_0_gram(m_value, s, sd))
    carry = wide_dot(inverse, m_value, 1, 0).astype(BF16)
    carry_ref[...] = carry
    gram_term(out_ref, core_ref, carry, images_with(sketch_ref))


def last_project_kernel(
    x_ref, m_ref, before_ref, core_ref, right_ref, left_ref, carry_1_ref, carry_2_ref,
    third_ref, second_ref, first_ref, out_ref, images_ref, carry_ref,
):
    @pl.when(x_ref[0] == 3)
    def _():
        project(carry_ref, m_ref, before_ref)
        gram_term(out_ref, core_ref, carry_ref[...], lambda built: dot(built, right_ref[...], 1, 0), images_ref)

    def only_images(carry, dim, sketch_ref):
        out_ref[...] = jnp.zeros(out_ref.shape, BF16)
        images_of = images_with(sketch_ref)
        for i in range(core_ref.shape[0]):
            images_ref[i] = images_of(dot(carry, core_ref[i], dim, 0).astype(BF16))

    @pl.when(x_ref[0] == 2)
    def _():
        only_images(carry_2_ref[...], 1, first_ref)

    @pl.when(x_ref[0] == 1)
    def _():
        only_images(carry_1_ref[...], 1, second_ref)

    @pl.when(x_ref[0] == 0)
    def _():
        only_images(left_ref[...].astype(BF16), 0, third_ref)


def final_kernel(
    scale, x_ref, m_0_ref, m_1_ref, m_2_ref, m_3_ref, third_ref, second_ref, first_ref, right_ref,
    images_ref, frames_ref, interface_ref, main_ref, rest_ref, gram_ref,
):
    def take(m_ref):
        main, rest = read(m_ref)
        main_ref[...] = main.astype(F32)
        rest_ref[...] = rest.astype(F32)
        return main, rest

    @pl.when(x_ref[0] == 0)
    def _():
        m_value = m_0_ref[...]
        main_ref[...] = m_value[:, :MAIN]
        rest_ref[...] = m_value[:, MAIN:].T
        gram_ref[...] = m_0_gram(m_value, *read(third_ref))

    @pl.when(x_ref[0] == 1)
    def _():
        gram_ref[...] = symmetric_gram(take(m_1_ref), read(second_ref))

    @pl.when(x_ref[0] == 2)
    def _():
        gram_ref[...] = symmetric_gram(take(m_2_ref), read(first_ref))

    @pl.when(x_ref[0] == 3)
    def _():
        main, rest = take(m_3_ref)
        right, right_rest = right_ref[:MAIN], right_ref[MAIN:]
        gram_ref[...] = 0.5 * (
            dot(main, right, 1, 0) + dot(rest, right_rest, 0, 0) + dot(right, main, 0, 1) + dot(right_rest, rest, 0, 0)
        )

    inverse = inverse_factor(gram_ref[...])
    interface_ref[:, 0, :MAIN] = wide_dot(inverse, main_ref[...], 1, 0)
    interface_ref[:, 0, MAIN:] = wide_dot(inverse, rest_ref[...], 1, 1)
    for i in range(images_ref.shape[0]):
        orth = wide_dot(images_ref[i], inverse, 1, 1)
        frames_ref[:, i, :] = (orth * scale).astype(BF16)


def call(kernel, *operands, out, scalar=False, scratch=()):
    specs = [pl.BlockSpec(memory_space=pltpu.VMEM) for _ in operands]
    if scalar:
        specs[0] = pl.BlockSpec(memory_space=pltpu.SMEM)
    outs = [jax.ShapeDtypeStruct(shape, kind) for shape, kind in out]
    return pl.pallas_call(
        kernel,
        out_shape=outs,
        in_specs=specs,
        out_specs=[pl.BlockSpec(memory_space=pltpu.VMEM) for _ in outs],
        scratch_shapes=[pltpu.VMEM(*piece) for piece in scratch],
        compiler_params=PARAMS,
    )(*operands)


WIDE = ((ROWS, LANES), BF16)
PAYLOAD = ((ROWS, MAIN), BF16)


def device(place, zh, x):
    y, zl, c = place
    if zh >= FAR // 2:
        zl, c = 1 - zl, 1 - c
    index = 0
    for at, size in zip((y, zh, zl, c, x), SIZES):
        index = index * size + at
    return index


def near_groups(planes):
    return [[device(place, zh, x) for place in NEAR] for x in planes for zh in range(FAR)]


def far_groups(planes):
    return [[device(place, zh, x) for x in planes for zh in range(FAR)] for place in NEAR]


def everywhere(shard, groups):
    copies = jnp.broadcast_to(shard, (len(groups[0]), *shard.shape))
    return lax.all_to_all(copies, AXES, 0, 0, axis_index_groups=groups, tiled=True)


def shard_sum(value):
    tiles = value.reshape(len(NEAR), ROWS // len(NEAR), -1)
    return added(lax.all_to_all(tiles, AXES, 0, 0, axis_index_groups=near_groups(range(4)), tiled=True))


def added(pieces):
    return pieces.astype(F32).sum(axis=0).astype(BF16)


def paired(value, pairs):
    spare = [x for x in range(4) if not any(x in pair for pair in pairs)]
    groups = [group for pair in pairs for group in far_groups(pair)] + near_groups(spare)
    pieces = everywhere(shard_sum(value), groups)
    return pieces[:FAR], pieces[FAR:]


def whole(shard):
    return everywhere(shard, near_groups(range(4)))


def body(train_cores, sketch_cores, left_interface, right_sketch):
    plane = lax.axis_index("x")
    plane_ref = plane.astype(jnp.int32).reshape(1)
    core = jnp.swapaxes(train_cores[0], 0, 1)
    sketch_core = jnp.swapaxes(sketch_cores[0], 0, 1)
    modes = core.shape[0]
    frame_scale = math.sqrt(SKETCH * modes * lax.axis_size(MODE))
    left_t = left_interface.T

    def full(shard):
        return whole(shard).reshape(ROWS, -1)

    term, rest = call(
        first_kernel, plane_ref, core, sketch_core, right_sketch, left_t, out=[WIDE, PAYLOAD], scalar=True
    )
    first = full(added(paired(term, ((3, 2), (0, 1)))[0]))
    (term,) = call(sketch_kernel, core, sketch_core, first, out=[PAYLOAD])
    second = full(added(paired(term, ((2, 1),))[0]))
    (term,) = call(last_sketch_kernel, plane_ref, core, sketch_core, second, rest, out=[PAYLOAD], scalar=True)
    both = paired(term, ((1, 0),))
    arrived = whole(jnp.concatenate([added(both[0]), added(both[1])], axis=0))
    third = arrived[:, :8].reshape(ROWS, MAIN)
    rest = arrived[:, 8:].reshape(ROWS, MAIN)

    carry_kind = ((SKETCH, RANK), BF16)
    term, carry_1, m_0 = call(
        first_project_kernel, first, rest, third, core, second, out=[PAYLOAD, carry_kind, ((SKETCH, RANK), F32)]
    )
    m_1 = full(added(paired(term, ((1, 2),))[0]))
    term, carry_2 = call(project_kernel, m_1, second, core, first, out=[PAYLOAD, carry_kind])
    m_2 = full(added(paired(term, ((2, 3),))[0]))
    term, images = call(
        last_project_kernel, plane_ref, m_2, first, core, right_sketch, left_t, carry_1, carry_2,
        third, second, first, out=[PAYLOAD, ((modes, SKETCH, SKETCH), F32)], scalar=True,
        scratch=[((SKETCH, RANK), BF16)],
    )
    alone = [group for x in range(4) for group in far_groups((x,))]
    m_3 = full(added(everywhere(shard_sum(term), alone)))

    def finish(*refs):
        final_kernel(frame_scale, *refs)

    frames, interface = call(
        finish, plane_ref, m_0, m_1, m_2, m_3, third, second, first, right_sketch, images,
        out=[((SKETCH, modes, SKETCH), BF16), ((SKETCH, 1, RANK), F32)], scalar=True,
        scratch=[((SKETCH, MAIN), F32), ((RANK - MAIN, SKETCH), F32), ((SKETCH, SKETCH), F32)],
    )
    return (frames[None], interface.reshape(1, SKETCH, RANK))


def solution(mesh):
    split = Mesh(mesh.devices.reshape(*SIZES), AXES)
    placed = (P("x", None, MODE, None), P("x", None, MODE, None), P(), P())
    return jax.shard_map(
        body,
        mesh=split,
        in_specs=placed,
        out_specs=(P("x", None, MODE, None), P("x", None, None)),
        check_vma=False,
    )
```

```python
import math

import jax
import jax.numpy as jnp
from jax import lax
from jax.experimental import pallas as pl
from jax.experimental.pallas import tpu as pltpu
from jax.sharding import Mesh
from jax.sharding import PartitionSpec as P

AXES = ("y", "zh", "zl", "c", "x")
MODE = ("y", "zh", "zl", "c")
SIZES = (4, 8, 2, 2, 4)
NEAR = tuple((y, zl, c) for y in range(4) for zl in range(2) for c in range(2))
FAR = 8
RANK = 400
SKETCH = 100
ROWS = 128
LANES = 512
MAIN = 384
F32 = jnp.float32
BF16 = jnp.bfloat16
PARAMS = pltpu.CompilerParams(vmem_limit_bytes=24 * 1024 * 1024)


def dot(a, b, ca, cb):
    return lax.dot_general(a, b, (((ca,), (cb,)), ((), ())), preferred_element_type=F32)


def inverse_factor(gram):
    size = gram.shape[0]
    count = -(-size // 8)
    padded = jnp.pad(gram, ((0, count * 8 - size), (0, 128 - size)))
    tiles = [padded[8 * t : 8 * t + 8] for t in range(count)]
    lane = lax.broadcasted_iota(jnp.int32, (8, 128), 1)
    sub = lax.broadcasted_iota(jnp.int32, (8, 128), 0)

    none = jnp.where(lane >= 128, 1.0, 0.0)

    def column(tile, j):
        return jnp.broadcast_to(tile[:, j : j + 1], (8, 128))

    def line(tile, s):
        return jnp.broadcast_to(tile[s : s + 1], (8, 128))

    for own in range(count):
        base = 8 * own
        width = min(8, size - base)
        step = lane - base
        columns = {t: [column(tiles[t], base + c) for c in range(width)] for t in range(own, count)}
        head = [value + none for value in columns[own]]
        scales, leads = [], []
        tile = tiles[own]
        for s in range(width):
            scales.append(line(1.0 / head[s], s))
            leads.append([line(head[c], s) if c > s else None for c in range(width)])
            factor = jnp.where(sub > s, head[s] * scales[s], 0.0)
            pivot = jnp.where(step == s, 1.0, line(tile, s))
            tile = jnp.where((step == s) & (sub > s), 0.0, tile) - factor * pivot
            for c in range(s + 1, width):
                head[c] = head[c] - factor * leads[s][c]
        tiles[own] = tile
        reduced = jnp.where((step > sub) & (step < 8), 0.0, jnp.where(step == sub, 1.0, tile))
        pivots = [line(reduced, s) for s in range(width)]
        for t in range(own + 1, count):
            col = columns[t]
            new = jnp.where((step >= 0) & (step < 8), 0.0, tiles[t])
            for s in range(width):
                factor = col[s] * scales[s]
                new = new - factor * pivots[s]
                for c in range(s + 1, width):
                    col[c] = col[c] - factor * leads[s][c]
            tiles[t] = new
    done = []
    for t in range(count):
        row = sub + 8 * t
        diagonal = jnp.sum(jnp.where(lane == row, tiles[t], 0.0), axis=1, keepdims=True)
        lower = jnp.where(lane < row, tiles[t], jnp.where(lane == row, 1.0, 0.0))
        done.append(lower * lax.rsqrt(diagonal))
    return jnp.concatenate(done, axis=0)[:size, :size]


def halves(value):
    high = value.astype(BF16)
    return high, (value - high.astype(F32)).astype(BF16)


def wide_dot(a, b, ca, cb):
    a_high, a_low = halves(a)
    b_high, b_low = halves(b)
    return dot(a_high, b_high, ca, cb) + (dot(a_high, b_low, ca, cb) + dot(a_low, b_high, ca, cb))


def left_wide_dot(a, b, ca, cb):
    a_high, a_low = halves(a)
    return dot(a_high, b, ca, cb) + dot(a_low, b, ca, cb)


def read(ref):
    return ref[:SKETCH, :MAIN], ref[104:120, :SKETCH]


def write(ref, main, rest):
    ref[...] = jnp.zeros(ref.shape, BF16)
    ref[:SKETCH, :MAIN] = main.astype(BF16)
    ref[104:120, :SKETCH] = rest.astype(BF16)


def symmetric_gram(m_pieces, sketch_pieces):
    main, rest = m_pieces
    sketch, sketch_rest = sketch_pieces
    return 0.5 * (
        dot(main, sketch, 1, 1)
        + dot(rest, sketch_rest, 0, 0)
        + dot(sketch, main, 1, 1)
        + dot(sketch_rest, rest, 0, 0)
    )


def sketch_term(out_ref, core_ref, sketch_core_ref, partial_of):
    total = rest = None
    for i in range(core_ref.shape[0]):
        partial = partial_of(core_ref[i]).astype(BF16)
        term = dot(sketch_core_ref[i], partial[:MAIN], 1, 1)
        end = dot(partial[MAIN:], sketch_core_ref[i], 1, 1)
        total, rest = (term, end) if total is None else (total + term, rest + end)
    write(out_ref, total, rest)


def first_kernel(x_ref, core_ref, sketch_core_ref, right_ref, left_ref, out_ref, rest_ref):
    rest_ref[...] = jnp.zeros((ROWS, MAIN), BF16)

    @pl.when(x_ref[0] != 0)
    def _():
        sketch_term(out_ref, core_ref, sketch_core_ref, lambda core: dot(core, right_ref[...], 1, 0))

    @pl.when(x_ref[0] == 0)
    def _():
        square = None
        left_t = left_ref[...].astype(BF16)
        for i in range(core_ref.shape[0]):
            built = dot(left_t, core_ref[i], 0, 0).astype(BF16)
            term = dot(built, built, 0, 0)
            square = term if square is None else square + term
        square = square.astype(BF16)
        out_ref[:, RANK:] = jnp.zeros((ROWS, LANES - RANK), BF16)
        out_ref[:, :RANK] = square[:128]
        out_ref[:, 400:416] = square[128:256, 384:400]
        out_ref[:, 416:432] = square[256:384, 384:400]
        out_ref[:16, 432:448] = square[384:400, 384:400]
        rest_ref[:, :256] = square[128:256, 128:384]
        rest_ref[:, 256:384] = square[256:384, 256:384]


def sketch_kernel(core_ref, sketch_core_ref, sketch_ref, out_ref):
    sketch, rest = read(sketch_ref)
    sketch_term(
        out_ref,
        core_ref,
        sketch_core_ref,
        lambda core: dot(core[:, :MAIN], sketch, 1, 1) + dot(core[:, MAIN:], rest, 1, 0),
    )


def last_sketch_kernel(x_ref, core_ref, sketch_core_ref, sketch_ref, rest_ref, out_ref):
    @pl.when(x_ref[0] == 0)
    def _():
        out_ref[...] = rest_ref[...]

    @pl.when(x_ref[0] != 0)
    def _():
        sketch_kernel(core_ref, sketch_core_ref, sketch_ref, out_ref)


def gram_term(out_ref, core_ref, carry, images_of, images_ref=None):
    total = rest = None
    for i in range(core_ref.shape[0]):
        built = dot(carry, core_ref[i], 1, 0).astype(BF16)
        images = images_of(built)
        if images_ref is not None:
            images_ref[i] = images
        images = images.astype(BF16)
        term = dot(images, built[:, :MAIN], 0, 0)
        end = dot(built[:, MAIN:], images, 0, 0)
        total, rest = (term, end) if total is None else (total + term, rest + end)
    write(out_ref, total, rest)


def images_with(sketch_ref):
    sketch, rest = read(sketch_ref)
    return lambda built: dot(built[:, :MAIN], sketch, 1, 1) + dot(built[:, MAIN:], rest, 1, 0)


def project(carry_ref, m_ref, before_ref):
    main, rest = read(m_ref)
    inverse = inverse_factor(symmetric_gram((main, rest), read(before_ref)))
    carry_ref[:, :MAIN] = left_wide_dot(inverse, main, 1, 0).astype(BF16)
    carry_ref[:, MAIN:] = left_wide_dot(inverse, rest, 1, 1).astype(BF16)


def project_kernel(m_ref, before_ref, core_ref, sketch_ref, out_ref, carry_ref):
    project(carry_ref, m_ref, before_ref)
    gram_term(out_ref, core_ref, carry_ref[...], images_with(sketch_ref))


def m_0_gram(m_value, sketch, sketch_rest):
    high, low = halves(m_value)
    total = None
    for part in (high, low):
        term = 0.5 * (
            dot(part[:, :MAIN], sketch, 1, 1)
            + dot(part[:, MAIN:], sketch_rest, 1, 0)
            + dot(sketch, part[:, :MAIN], 1, 1)
            + dot(sketch_rest, part[:, MAIN:], 0, 1)
        )
        total = term if total is None else total + term
    return total


def first_project_kernel(upper_ref, rest_ref, before_ref, core_ref, sketch_ref, out_ref, carry_ref, m0_ref):
    s, sd = read(before_ref)
    sa, sb, sc = s[:, :128], s[:, 128:256], s[:, 256:384]
    a = upper_ref[:, :RANK]
    b = rest_ref[:, :256]
    c = rest_ref[:, 256:384]
    b_end = upper_ref[:, 400:416]
    c_end = upper_ref[:, 416:432]
    d_end = upper_ref[:16, 432:448]
    over_a = dot(sa, a, 1, 0)
    m0_ref[:, :128] = over_a[:, :128] + dot(s[:, 128:], a[:, 128:MAIN], 1, 1) + dot(sd, a[:, MAIN:], 0, 1)
    m0_ref[:, 128:256] = (
        over_a[:, 128:256] + dot(sb, b[:, :128], 1, 0) + dot(sc, b[:, 128:], 1, 1) + dot(sd, b_end, 0, 1)
    )
    m0_ref[:, 256:384] = over_a[:, 256:384] + dot(sb, b[:, 128:], 1, 0) + dot(sc, c, 1, 0) + dot(sd, c_end, 0, 1)
    m0_ref[:, 384:400] = over_a[:, 384:400] + dot(sb, b_end, 1, 0) + dot(sc, c_end, 1, 0) + dot(sd, d_end, 0, 0)
    m_value = m0_ref[...]
    inverse = inverse_factor(m_0_gram(m_value, s, sd))
    carry = wide_dot(inverse, m_value, 1, 0).astype(BF16)
    carry_ref[...] = carry
    gram_term(out_ref, core_ref, carry, images_with(sketch_ref))


def last_project_kernel(
    x_ref, m_ref, before_ref, core_ref, right_ref, left_ref, carry_1_ref, carry_2_ref,
    third_ref, second_ref, first_ref, out_ref, images_ref, carry_ref,
):
    @pl.when(x_ref[0] == 3)
    def _():
        project(carry_ref, m_ref, before_ref)
        gram_term(out_ref, core_ref, carry_ref[...], lambda built: dot(built, right_ref[...], 1, 0), images_ref)

    def only_images(carry, dim, sketch_ref):
        out_ref[...] = jnp.zeros(out_ref.shape, BF16)
        images_of = images_with(sketch_ref)
        for i in range(core_ref.shape[0]):
            images_ref[i] = images_of(dot(carry, core_ref[i], dim, 0).astype(BF16))

    @pl.when(x_ref[0] == 2)
    def _():
        only_images(carry_2_ref[...], 1, first_ref)

    @pl.when(x_ref[0] == 1)
    def _():
        only_images(carry_1_ref[...], 1, second_ref)

    @pl.when(x_ref[0] == 0)
    def _():
        only_images(left_ref[...].astype(BF16), 0, third_ref)


def final_kernel(
    scale, x_ref, m_0_ref, m_1_ref, m_2_ref, m_3_ref, third_ref, second_ref, first_ref, right_ref,
    images_ref, frames_ref, interface_ref, main_ref, rest_ref, gram_ref,
):
    def take(m_ref):
        main, rest = read(m_ref)
        main_ref[...] = main.astype(F32)
        rest_ref[...] = rest.astype(F32)
        return main, rest

    @pl.when(x_ref[0] == 0)
    def _():
        m_value = m_0_ref[...]
        main_ref[...] = m_value[:, :MAIN]
        rest_ref[...] = m_value[:, MAIN:].T
        gram_ref[...] = m_0_gram(m_value, *read(third_ref))

    @pl.when(x_ref[0] == 1)
    def _():
        gram_ref[...] = symmetric_gram(take(m_1_ref), read(second_ref))

    @pl.when(x_ref[0] == 2)
    def _():
        gram_ref[...] = symmetric_gram(take(m_2_ref), read(first_ref))

    @pl.when(x_ref[0] == 3)
    def _():
        main, rest = take(m_3_ref)
        right, right_rest = right_ref[:MAIN], right_ref[MAIN:]
        gram_ref[...] = 0.5 * (
            dot(main, right, 1, 0) + dot(rest, right_rest, 0, 0) + dot(right, main, 0, 1) + dot(right_rest, rest, 0, 0)
        )

    inverse = inverse_factor(gram_ref[...])
    interface_ref[:, 0, :MAIN] = wide_dot(inverse, main_ref[...], 1, 0)
    interface_ref[:, 0, MAIN:] = wide_dot(inverse, rest_ref[...], 1, 1)
    for i in range(images_ref.shape[0]):
        orth = wide_dot(images_ref[i], inverse, 1, 1)
        frames_ref[:, i, :] = (orth * scale).astype(BF16)


def call(kernel, *operands, out, scalar=False, scratch=()):
    specs = [pl.BlockSpec(memory_space=pltpu.VMEM) for _ in operands]
    if scalar:
        specs[0] = pl.BlockSpec(memory_space=pltpu.SMEM)
    outs = [jax.ShapeDtypeStruct(shape, kind) for shape, kind in out]
    return pl.pallas_call(
        kernel,
        out_shape=outs,
        in_specs=specs,
        out_specs=[pl.BlockSpec(memory_space=pltpu.VMEM) for _ in outs],
        scratch_shapes=[pltpu.VMEM(*piece) for piece in scratch],
        compiler_params=PARAMS,
    )(*operands)


WIDE = ((ROWS, LANES), BF16)
PAYLOAD = ((ROWS, MAIN), BF16)


def device(place, zh, x):
    y, zl, c = place
    if zh >= FAR // 2:
        zl, c = 1 - zl, 1 - c
    index = 0
    for at, size in zip((y, zh, zl, c, x), SIZES):
        index = index * size + at
    return index


def near_group(zh, x):
    return [device(place, zh, x) for place in NEAR]


def far_groups(planes):
    groups = [[device(place, zh, x) for zh in range(FAR)] for x in planes for place in NEAR]
    for x in range(4):
        if x not in planes:
            for zh in range(FAR):
                for chip in range(2):
                    groups.append([device(place, zh, x) for place in NEAR if place[1] == chip])
    return groups


def pair_groups(pairs):
    groups = [near_group(zh, x) + near_group(zh, other) for x, other in pairs for zh in range(FAR)]
    for x in range(4):
        if not any(x in pair for pair in pairs):
            groups += [near_group(zh, x) + near_group(zh + 1, x) for zh in range(0, FAR, 2)]
    return groups


NEAR_GROUPS = [near_group(zh, x) for x in range(4) for zh in range(FAR)]


def exchanged(tiles, groups):
    return lax.all_to_all(tiles, AXES, 0, 0, axis_index_groups=groups, tiled=True)


def everywhere(shard, groups):
    return exchanged(jnp.broadcast_to(shard, (len(groups[0]), *shard.shape)), groups)


def added(pieces):
    return pieces.astype(F32).sum(axis=0).astype(BF16)


def plane_sum(value, planes):
    tiles = value.reshape(len(NEAR), ROWS // len(NEAR), -1)
    return added(everywhere(added(exchanged(tiles, NEAR_GROUPS)), far_groups(planes)))


def whole_pair(shard, pairs):
    rows = everywhere(shard, pair_groups(pairs))
    return rows[: len(NEAR)].reshape(ROWS, -1), rows[len(NEAR) :].reshape(ROWS, -1)


def body(train_cores, sketch_cores, left_interface, right_sketch):
    plane = lax.axis_index("x")
    plane_ref = plane.astype(jnp.int32).reshape(1)
    core = jnp.swapaxes(train_cores[0], 0, 1)
    sketch_core = jnp.swapaxes(sketch_cores[0], 0, 1)
    modes = core.shape[0]
    frame_scale = math.sqrt(SKETCH * modes * lax.axis_size(MODE))
    left_t = left_interface.T

    term, rest = call(
        first_kernel, plane_ref, core, sketch_core, right_sketch, left_t, out=[WIDE, PAYLOAD], scalar=True
    )
    first = whole_pair(plane_sum(term, (3, 0)), ((3, 2), (0, 1)))[0]
    (term,) = call(sketch_kernel, core, sketch_core, first, out=[PAYLOAD])
    second = whole_pair(plane_sum(term, (2,)), ((2, 1),))[0]
    (term,) = call(last_sketch_kernel, plane_ref, core, sketch_core, second, rest, out=[PAYLOAD], scalar=True)
    third, rest = whole_pair(plane_sum(term, (1, 0)), ((1, 0),))

    carry_kind = ((SKETCH, RANK), BF16)
    term, carry_1, m_0 = call(
        first_project_kernel, first, rest, third, core, second, out=[PAYLOAD, carry_kind, ((SKETCH, RANK), F32)]
    )
    m_1 = whole_pair(plane_sum(term, (1,)), ((1, 2),))[0]
    term, carry_2 = call(project_kernel, m_1, second, core, first, out=[PAYLOAD, carry_kind])
    m_2 = whole_pair(plane_sum(term, (2,)), ((2, 3),))[0]
    term, images = call(
        last_project_kernel, plane_ref, m_2, first, core, right_sketch, left_t, carry_1, carry_2,
        third, second, first, out=[PAYLOAD, ((modes, SKETCH, SKETCH), F32)], scalar=True,
        scratch=[((SKETCH, RANK), BF16)],
    )
    m_3 = everywhere(plane_sum(term, (3,)), NEAR_GROUPS).reshape(ROWS, -1)

    def finish(*refs):
        final_kernel(frame_scale, *refs)

    frames, interface = call(
        finish, plane_ref, m_0, m_1, m_2, m_3, third, second, first, right_sketch, images,
        out=[((SKETCH, modes, SKETCH), BF16), ((SKETCH, 1, RANK), F32)], scalar=True,
        scratch=[((SKETCH, MAIN), F32), ((RANK - MAIN, SKETCH), F32), ((SKETCH, SKETCH), F32)],
    )
    return (frames[None], interface.reshape(1, SKETCH, RANK))


def solution(mesh):
    split = Mesh(mesh.devices.reshape(*SIZES), AXES)
    placed = (P("x", None, MODE, None), P("x", None, MODE, None), P(), P())
    return jax.shard_map(
        body,
        mesh=split,
        in_specs=placed,
        out_specs=(P("x", None, MODE, None), P("x", None, None)),
        check_vma=False,
    )
```

```python
import math

import jax
import jax.numpy as jnp
from jax import lax
from jax.experimental import pallas as pl
from jax.experimental.pallas import tpu as pltpu
from jax.sharding import Mesh
from jax.sharding import PartitionSpec as P

AXES = ("y", "zh", "zl", "c", "x")
MODE = ("y", "zh", "zl", "c")
SIZES = (4, 8, 2, 2, 4)
NEAR = tuple(((0, 2, 1, 3)[k % 4], (k + k // 4) % 2, k // 8) for k in range(16))
FAR = 8
FAR_ORDER = (0, 4, 1, 5, 2, 6, 3, 7)
RANK = 400
SKETCH = 100
ROWS = 128
LANES = 512
MAIN = 384
F32 = jnp.float32
BF16 = jnp.bfloat16
PARAMS = pltpu.CompilerParams(vmem_limit_bytes=24 * 1024 * 1024)


def dot(a, b, ca, cb):
    return lax.dot_general(a, b, (((ca,), (cb,)), ((), ())), preferred_element_type=F32)


def inverse_factor(gram):
    size = gram.shape[0]
    count = -(-size // 8)
    padded = jnp.pad(gram, ((0, count * 8 - size), (0, 128 - size)))
    tiles = [padded[8 * t : 8 * t + 8] for t in range(count)]
    lane = lax.broadcasted_iota(jnp.int32, (8, 128), 1)
    sub = lax.broadcasted_iota(jnp.int32, (8, 128), 0)

    none = jnp.where(lane >= 128, 1.0, 0.0)

    def column(tile, j):
        return jnp.broadcast_to(tile[:, j : j + 1], (8, 128))

    def line(tile, s):
        return jnp.broadcast_to(tile[s : s + 1], (8, 128))

    for own in range(count):
        base = 8 * own
        width = min(8, size - base)
        step = lane - base
        columns = {t: [column(tiles[t], base + c) for c in range(width)] for t in range(own, count)}
        head = [value + none for value in columns[own]]
        scales, leads = [], []
        tile = tiles[own]
        for s in range(width):
            scales.append(line(1.0 / head[s], s))
            leads.append([line(head[c], s) if c > s else None for c in range(width)])
            factor = jnp.where(sub > s, head[s] * scales[s], 0.0)
            pivot = jnp.where(step == s, 1.0, line(tile, s))
            tile = jnp.where((step == s) & (sub > s), 0.0, tile) - factor * pivot
            for c in range(s + 1, width):
                head[c] = head[c] - factor * leads[s][c]
        tiles[own] = tile
        reduced = jnp.where((step > sub) & (step < 8), 0.0, jnp.where(step == sub, 1.0, tile))
        pivots = [line(reduced, s) for s in range(width)]
        for t in range(own + 1, count):
            col = columns[t]
            new = jnp.where((step >= 0) & (step < 8), 0.0, tiles[t])
            for s in range(width):
                factor = col[s] * scales[s]
                new = new - factor * pivots[s]
                for c in range(s + 1, width):
                    col[c] = col[c] - factor * leads[s][c]
            tiles[t] = new
    done = []
    for t in range(count):
        row = sub + 8 * t
        diagonal = jnp.sum(jnp.where(lane == row, tiles[t], 0.0), axis=1, keepdims=True)
        lower = jnp.where(lane < row, tiles[t], jnp.where(lane == row, 1.0, 0.0))
        done.append(lower * lax.rsqrt(diagonal))
    return jnp.concatenate(done, axis=0)[:size, :size]


def halves(value):
    high = value.astype(BF16)
    return high, (value - high.astype(F32)).astype(BF16)


def wide_dot(a, b, ca, cb):
    a_high, a_low = halves(a)
    b_high, b_low = halves(b)
    return dot(a_high, b_high, ca, cb) + (dot(a_high, b_low, ca, cb) + dot(a_low, b_high, ca, cb))


def left_wide_dot(a, b, ca, cb):
    a_high, a_low = halves(a)
    return dot(a_high, b, ca, cb) + dot(a_low, b, ca, cb)


def read(ref):
    return ref[:SKETCH, :MAIN], ref[104:120, :SKETCH]


def write(ref, main, rest):
    ref[...] = jnp.zeros(ref.shape, BF16)
    ref[:SKETCH, :MAIN] = main.astype(BF16)
    ref[104:120, :SKETCH] = rest.astype(BF16)


def symmetric_gram(m_pieces, sketch_pieces):
    main, rest = m_pieces
    sketch, sketch_rest = sketch_pieces
    return 0.5 * (
        dot(main, sketch, 1, 1)
        + dot(rest, sketch_rest, 0, 0)
        + dot(sketch, main, 1, 1)
        + dot(sketch_rest, rest, 0, 0)
    )


def sketch_term(out_ref, core_ref, sketch_core_ref, partial_of):
    total = rest = None
    for i in range(core_ref.shape[0]):
        partial = partial_of(core_ref[i]).astype(BF16)
        term = dot(sketch_core_ref[i], partial[:MAIN], 1, 1)
        end = dot(partial[MAIN:], sketch_core_ref[i], 1, 1)
        total, rest = (term, end) if total is None else (total + term, rest + end)
    write(out_ref, total, rest)


def first_kernel(x_ref, core_ref, sketch_core_ref, right_ref, left_ref, out_ref, rest_ref):
    rest_ref[...] = jnp.zeros((ROWS, MAIN), BF16)

    @pl.when(x_ref[0] != 0)
    def _():
        sketch_term(out_ref, core_ref, sketch_core_ref, lambda core: dot(core, right_ref[...], 1, 0))

    @pl.when(x_ref[0] == 0)
    def _():
        square = None
        left_t = left_ref[...].astype(BF16)
        for i in range(core_ref.shape[0]):
            built = dot(left_t, core_ref[i], 0, 0).astype(BF16)
            term = dot(built, built, 0, 0)
            square = term if square is None else square + term
        square = square.astype(BF16)
        out_ref[:, RANK:] = jnp.zeros((ROWS, LANES - RANK), BF16)
        out_ref[:, :RANK] = square[:128]
        out_ref[:, 400:416] = square[128:256, 384:400]
        out_ref[:, 416:432] = square[256:384, 384:400]
        out_ref[:16, 432:448] = square[384:400, 384:400]
        rest_ref[:, :256] = square[128:256, 128:384]
        rest_ref[:, 256:384] = square[256:384, 256:384]


def sketch_kernel(core_ref, sketch_core_ref, sketch_ref, out_ref):
    sketch, rest = read(sketch_ref)
    sketch_term(
        out_ref,
        core_ref,
        sketch_core_ref,
        lambda core: dot(core[:, :MAIN], sketch, 1, 1) + dot(core[:, MAIN:], rest, 1, 0),
    )


def last_sketch_kernel(x_ref, core_ref, sketch_core_ref, sketch_ref, rest_ref, out_ref):
    @pl.when(x_ref[0] == 0)
    def _():
        out_ref[...] = rest_ref[...]

    @pl.when(x_ref[0] != 0)
    def _():
        sketch_kernel(core_ref, sketch_core_ref, sketch_ref, out_ref)


def gram_term(out_ref, core_ref, carry, images_of, images_ref=None):
    total = rest = None
    for i in range(core_ref.shape[0]):
        built = dot(carry, core_ref[i], 1, 0).astype(BF16)
        images = images_of(built)
        if images_ref is not None:
            images_ref[i] = images
        images = images.astype(BF16)
        term = dot(images, built[:, :MAIN], 0, 0)
        end = dot(built[:, MAIN:], images, 0, 0)
        total, rest = (term, end) if total is None else (total + term, rest + end)
    write(out_ref, total, rest)


def images_with(sketch_ref):
    sketch, rest = read(sketch_ref)
    return lambda built: dot(built[:, :MAIN], sketch, 1, 1) + dot(built[:, MAIN:], rest, 1, 0)


def project(carry_ref, m_ref, before_ref):
    main, rest = read(m_ref)
    inverse = inverse_factor(symmetric_gram((main, rest), read(before_ref)))
    carry_ref[:, :MAIN] = left_wide_dot(inverse, main, 1, 0).astype(BF16)
    carry_ref[:, MAIN:] = left_wide_dot(inverse, rest, 1, 1).astype(BF16)


def project_kernel(m_ref, before_ref, core_ref, sketch_ref, out_ref, carry_ref):
    project(carry_ref, m_ref, before_ref)
    gram_term(out_ref, core_ref, carry_ref[...], images_with(sketch_ref))


def m_0_gram(m_value, sketch, sketch_rest):
    high, low = halves(m_value)
    total = None
    for part in (high, low):
        term = 0.5 * (
            dot(part[:, :MAIN], sketch, 1, 1)
            + dot(part[:, MAIN:], sketch_rest, 1, 0)
            + dot(sketch, part[:, :MAIN], 1, 1)
            + dot(sketch_rest, part[:, MAIN:], 0, 1)
        )
        total = term if total is None else total + term
    return total


def first_project_kernel(upper_ref, rest_ref, before_ref, core_ref, sketch_ref, out_ref, carry_ref, m0_ref):
    s, sd = read(before_ref)
    sa, sb, sc = s[:, :128], s[:, 128:256], s[:, 256:384]
    a = upper_ref[:, :RANK]
    b = rest_ref[:, :256]
    c = rest_ref[:, 256:384]
    b_end = upper_ref[:, 400:416]
    c_end = upper_ref[:, 416:432]
    d_end = upper_ref[:16, 432:448]
    over_a = dot(sa, a, 1, 0)
    m0_ref[:, :128] = over_a[:, :128] + dot(s[:, 128:], a[:, 128:MAIN], 1, 1) + dot(sd, a[:, MAIN:], 0, 1)
    m0_ref[:, 128:256] = (
        over_a[:, 128:256] + dot(sb, b[:, :128], 1, 0) + dot(sc, b[:, 128:], 1, 1) + dot(sd, b_end, 0, 1)
    )
    m0_ref[:, 256:384] = over_a[:, 256:384] + dot(sb, b[:, 128:], 1, 0) + dot(sc, c, 1, 0) + dot(sd, c_end, 0, 1)
    m0_ref[:, 384:400] = over_a[:, 384:400] + dot(sb, b_end, 1, 0) + dot(sc, c_end, 1, 0) + dot(sd, d_end, 0, 0)
    m_value = m0_ref[...]
    inverse = inverse_factor(m_0_gram(m_value, s, sd))
    carry = wide_dot(inverse, m_value, 1, 0).astype(BF16)
    carry_ref[...] = carry
    gram_term(out_ref, core_ref, carry, images_with(sketch_ref))


def last_project_kernel(
    x_ref, m_ref, before_ref, core_ref, right_ref, left_ref, carry_1_ref, carry_2_ref,
    third_ref, second_ref, first_ref, out_ref, images_ref, carry_ref,
):
    @pl.when(x_ref[0] == 3)
    def _():
        project(carry_ref, m_ref, before_ref)
        gram_term(out_ref, core_ref, carry_ref[...], lambda built: dot(built, right_ref[...], 1, 0), images_ref)

    def only_images(carry, dim, sketch_ref):
        out_ref[...] = jnp.zeros(out_ref.shape, BF16)
        images_of = images_with(sketch_ref)
        for i in range(core_ref.shape[0]):
            images_ref[i] = images_of(dot(carry, core_ref[i], dim, 0).astype(BF16))

    @pl.when(x_ref[0] == 2)
    def _():
        only_images(carry_2_ref[...], 1, first_ref)

    @pl.when(x_ref[0] == 1)
    def _():
        only_images(carry_1_ref[...], 1, second_ref)

    @pl.when(x_ref[0] == 0)
    def _():
        only_images(left_ref[...].astype(BF16), 0, third_ref)


def final_kernel(
    scale, x_ref, m_0_ref, m_1_ref, m_2_ref, m_3_ref, third_ref, second_ref, first_ref, right_ref,
    images_ref, frames_ref, interface_ref, main_ref, rest_ref, gram_ref,
):
    def take(m_ref):
        main, rest = read(m_ref)
        main_ref[...] = main.astype(F32)
        rest_ref[...] = rest.astype(F32)
        return main, rest

    @pl.when(x_ref[0] == 0)
    def _():
        m_value = m_0_ref[...]
        main_ref[...] = m_value[:, :MAIN]
        rest_ref[...] = m_value[:, MAIN:].T
        gram_ref[...] = m_0_gram(m_value, *read(third_ref))

    @pl.when(x_ref[0] == 1)
    def _():
        gram_ref[...] = symmetric_gram(take(m_1_ref), read(second_ref))

    @pl.when(x_ref[0] == 2)
    def _():
        gram_ref[...] = symmetric_gram(take(m_2_ref), read(first_ref))

    @pl.when(x_ref[0] == 3)
    def _():
        main, rest = take(m_3_ref)
        right, right_rest = right_ref[:MAIN], right_ref[MAIN:]
        gram_ref[...] = 0.5 * (
            dot(main, right, 1, 0) + dot(rest, right_rest, 0, 0) + dot(right, main, 0, 1) + dot(right_rest, rest, 0, 0)
        )

    inverse = inverse_factor(gram_ref[...])
    interface_ref[:, 0, :MAIN] = wide_dot(inverse, main_ref[...], 1, 0)
    interface_ref[:, 0, MAIN:] = wide_dot(inverse, rest_ref[...], 1, 1)
    for i in range(images_ref.shape[0]):
        orth = wide_dot(images_ref[i], inverse, 1, 1)
        frames_ref[:, i, :] = (orth * scale).astype(BF16)


def call(kernel, *operands, out, scalar=False, scratch=()):
    specs = [pl.BlockSpec(memory_space=pltpu.VMEM) for _ in operands]
    if scalar:
        specs[0] = pl.BlockSpec(memory_space=pltpu.SMEM)
    outs = [jax.ShapeDtypeStruct(shape, kind) for shape, kind in out]
    return pl.pallas_call(
        kernel,
        out_shape=outs,
        in_specs=specs,
        out_specs=[pl.BlockSpec(memory_space=pltpu.VMEM) for _ in outs],
        scratch_shapes=[pltpu.VMEM(*piece) for piece in scratch],
        compiler_params=PARAMS,
    )(*operands)


WIDE = ((ROWS, LANES), BF16)
PAYLOAD = ((ROWS, MAIN), BF16)


def device(place, zh, x):
    y, zl, c = place
    if zh >= FAR // 2:
        zl, c = 1 - zl, 1 - c
    index = 0
    for at, size in zip((y, zh, zl, c, x), SIZES):
        index = index * size + at
    return index


def near_group(zh, x):
    return [device(place, zh, x) for place in NEAR]


def far_groups(planes):
    groups = [[device(place, zh, x) for zh in FAR_ORDER] for x in planes for place in NEAR]
    for x in range(4):
        if x not in planes:
            for zh in range(FAR):
                for chip in range(2):
                    groups.append([device(place, zh, x) for place in NEAR if place[1] == chip])
    return groups


def pair_groups(pairs):
    groups = [near_group(zh, x) + near_group(zh, other) for x, other in pairs for zh in range(FAR)]
    for x in range(4):
        if not any(x in pair for pair in pairs):
            groups += [near_group(zh, x) + near_group(zh + 1, x) for zh in range(0, FAR, 2)]
    return groups


NEAR_GROUPS = [near_group(zh, x) for x in range(4) for zh in range(FAR)]


def exchanged(tiles, groups):
    return lax.all_to_all(tiles, AXES, 0, 0, axis_index_groups=groups, tiled=True)


def everywhere(shard, groups):
    return exchanged(jnp.broadcast_to(shard, (len(groups[0]), *shard.shape)), groups)


def added(pieces):
    return pieces.astype(F32).sum(axis=0).astype(BF16)


def plane_sum(value, planes):
    tiles = value.reshape(len(NEAR), ROWS // len(NEAR), -1)
    return added(everywhere(added(exchanged(tiles, NEAR_GROUPS)), far_groups(planes)))


def whole_pair(shard, pairs):
    rows = everywhere(shard, pair_groups(pairs))
    return rows[: len(NEAR)].reshape(ROWS, -1), rows[len(NEAR) :].reshape(ROWS, -1)


def body(train_cores, sketch_cores, left_interface, right_sketch):
    plane = lax.axis_index("x")
    plane_ref = plane.astype(jnp.int32).reshape(1)
    core = jnp.swapaxes(train_cores[0], 0, 1)
    sketch_core = jnp.swapaxes(sketch_cores[0], 0, 1)
    modes = core.shape[0]
    frame_scale = math.sqrt(SKETCH * modes * lax.axis_size(MODE))
    left_t = left_interface.T

    term, rest = call(
        first_kernel, plane_ref, core, sketch_core, right_sketch, left_t, out=[WIDE, PAYLOAD], scalar=True
    )
    first = whole_pair(plane_sum(term, (3, 0)), ((3, 2), (0, 1)))[0]
    (term,) = call(sketch_kernel, core, sketch_core, first, out=[PAYLOAD])
    second = whole_pair(plane_sum(term, (2,)), ((2, 1),))[0]
    (term,) = call(last_sketch_kernel, plane_ref, core, sketch_core, second, rest, out=[PAYLOAD], scalar=True)
    third, rest = whole_pair(plane_sum(term, (1, 0)), ((1, 0),))

    carry_kind = ((SKETCH, RANK), BF16)
    term, carry_1, m_0 = call(
        first_project_kernel, first, rest, third, core, second, out=[PAYLOAD, carry_kind, ((SKETCH, RANK), F32)]
    )
    m_1 = whole_pair(plane_sum(term, (1,)), ((1, 2),))[0]
    term, carry_2 = call(project_kernel, m_1, second, core, first, out=[PAYLOAD, carry_kind])
    m_2 = whole_pair(plane_sum(term, (2,)), ((2, 3),))[0]
    term, images = call(
        last_project_kernel, plane_ref, m_2, first, core, right_sketch, left_t, carry_1, carry_2,
        third, second, first, out=[PAYLOAD, ((modes, SKETCH, SKETCH), F32)], scalar=True,
        scratch=[((SKETCH, RANK), BF16)],
    )
    m_3 = everywhere(plane_sum(term, (3,)), NEAR_GROUPS).reshape(ROWS, -1)

    def finish(*refs):
        final_kernel(frame_scale, *refs)

    frames, interface = call(
        finish, plane_ref, m_0, m_1, m_2, m_3, third, second, first, right_sketch, images,
        out=[((SKETCH, modes, SKETCH), BF16), ((SKETCH, 1, RANK), F32)], scalar=True,
        scratch=[((SKETCH, MAIN), F32), ((RANK - MAIN, SKETCH), F32), ((SKETCH, SKETCH), F32)],
    )
    return (frames[None], interface.reshape(1, SKETCH, RANK))


def solution(mesh):
    split = Mesh(mesh.devices.reshape(*SIZES), AXES)
    placed = (P("x", None, MODE, None), P("x", None, MODE, None), P(), P())
    return jax.shard_map(
        body,
        mesh=split,
        in_specs=placed,
        out_specs=(P("x", None, MODE, None), P("x", None, None)),
        check_vma=False,
    )
```

```python
import math

import jax
import jax.numpy as jnp
from jax import lax
from jax.experimental import pallas as pl
from jax.experimental.pallas import tpu as pltpu
from jax.sharding import Mesh
from jax.sharding import PartitionSpec as P

AXES = ("y", "zh", "zl", "c", "x")
MODE = ("y", "zh", "zl", "c")
SIZES = (4, 8, 2, 2, 4)
NEAR = tuple((y, zl, c) for y in range(4) for zl in range(2) for c in range(2))
FAR = 8
RANK = 400
SKETCH = 100
ROWS = 128
MAIN = 384
F32 = jnp.float32
BF16 = jnp.bfloat16
PARAMS = pltpu.CompilerParams(vmem_limit_bytes=24 * 1024 * 1024)


def dot(a, b, ca, cb):
    return lax.dot_general(a, b, (((ca,), (cb,)), ((), ())), preferred_element_type=F32)


def inverse_factor(gram):
    size = gram.shape[0]
    count = -(-size // 8)
    padded = jnp.pad(gram, ((0, count * 8 - size), (0, 128 - size)))
    tiles = [padded[8 * t : 8 * t + 8] for t in range(count)]
    lane = lax.broadcasted_iota(jnp.int32, (8, 128), 1)
    sub = lax.broadcasted_iota(jnp.int32, (8, 128), 0)

    none = jnp.where(lane >= 128, 1.0, 0.0)

    def column(tile, j):
        return jnp.broadcast_to(tile[:, j : j + 1], (8, 128))

    def line(tile, s):
        return jnp.broadcast_to(tile[s : s + 1], (8, 128))

    for own in range(count):
        base = 8 * own
        width = min(8, size - base)
        step = lane - base
        columns = {t: [column(tiles[t], base + c) for c in range(width)] for t in range(own, count)}
        head = [value + none for value in columns[own]]
        scales, leads = [], []
        tile = tiles[own]
        for s in range(width):
            scales.append(line(1.0 / head[s], s))
            leads.append([line(head[c], s) if c > s else None for c in range(width)])
            factor = jnp.where(sub > s, head[s] * scales[s], 0.0)
            pivot = jnp.where(step == s, 1.0, line(tile, s))
            tile = jnp.where((step == s) & (sub > s), 0.0, tile) - factor * pivot
            for c in range(s + 1, width):
                head[c] = head[c] - factor * leads[s][c]
        tiles[own] = tile
        reduced = jnp.where((step > sub) & (step < 8), 0.0, jnp.where(step == sub, 1.0, tile))
        pivots = [line(reduced, s) for s in range(width)]
        for t in range(own + 1, count):
            col = columns[t]
            new = jnp.where((step >= 0) & (step < 8), 0.0, tiles[t])
            for s in range(width):
                factor = col[s] * scales[s]
                new = new - factor * pivots[s]
                for c in range(s + 1, width):
                    col[c] = col[c] - factor * leads[s][c]
            tiles[t] = new
    done = []
    for t in range(count):
        row = sub + 8 * t
        diagonal = jnp.sum(jnp.where(lane == row, tiles[t], 0.0), axis=1, keepdims=True)
        lower = jnp.where(lane < row, tiles[t], jnp.where(lane == row, 1.0, 0.0))
        done.append(lower * lax.rsqrt(diagonal))
    return jnp.concatenate(done, axis=0)[:size, :size]


def halves(value):
    high = value.astype(BF16)
    return high, (value - high.astype(F32)).astype(BF16)


def wide_dot(a, b, ca, cb):
    a_high, a_low = halves(a)
    b_high, b_low = halves(b)
    return dot(a_high, b_high, ca, cb) + (dot(a_high, b_low, ca, cb) + dot(a_low, b_high, ca, cb))


def left_wide_dot(a, b, ca, cb):
    a_high, a_low = halves(a)
    return dot(a_high, b, ca, cb) + dot(a_low, b, ca, cb)


def read(ref):
    return ref[:SKETCH, :MAIN], ref[104:120, :SKETCH]


def write(ref, main, rest):
    ref[...] = jnp.zeros(ref.shape, BF16)
    ref[:SKETCH, :MAIN] = main.astype(BF16)
    ref[104:120, :SKETCH] = rest.astype(BF16)


def symmetric_gram(m_pieces, sketch_pieces):
    main, rest = m_pieces
    sketch, sketch_rest = sketch_pieces
    return 0.5 * (
        dot(main, sketch, 1, 1)
        + dot(rest, sketch_rest, 0, 0)
        + dot(sketch, main, 1, 1)
        + dot(sketch_rest, rest, 0, 0)
    )


def sketch_term(out_ref, core_ref, sketch_core_ref, partial_of):
    total = rest = None
    for i in range(core_ref.shape[0]):
        partial = partial_of(core_ref[i]).astype(BF16)
        term = dot(sketch_core_ref[i], partial[:MAIN], 1, 1)
        end = dot(partial[MAIN:], sketch_core_ref[i], 1, 1)
        total, rest = (term, end) if total is None else (total + term, rest + end)
    write(out_ref, total, rest)


def first_kernel(x_ref, core_ref, sketch_core_ref, right_ref, left_ref, out_ref, rest_ref):
    rest_ref[...] = jnp.zeros((ROWS, MAIN), BF16)

    @pl.when(x_ref[0] != 0)
    def _():
        sketch_term(out_ref, core_ref, sketch_core_ref, lambda core: dot(core, right_ref[...], 1, 0))

    @pl.when(x_ref[0] == 0)
    def _():
        square = None
        left_t = left_ref[...].astype(BF16)
        for i in range(core_ref.shape[0]):
            built = dot(left_t, core_ref[i], 0, 0).astype(BF16)
            term = dot(built, built, 0, 0)
            square = term if square is None else square + term
        square = square.astype(BF16)
        out_ref[...] = square[:128, :MAIN]
        for k in range(4):
            out_ref[64:128, 16 * k : 16 * k + 16] = square[64 * k : 64 * k + 64, MAIN:]
        rest_ref[:, :256] = square[128:256, 128:384]
        rest_ref[:, 256:384] = square[256:384, 256:384]
        rest_ref[64:128, 256:272] = square[256:320, MAIN:]
        rest_ref[64:128, 272:288] = square[320:384, MAIN:]
        rest_ref[64:80, 288:304] = square[384:400, MAIN:]


def sketch_kernel(core_ref, sketch_core_ref, sketch_ref, out_ref):
    sketch, rest = read(sketch_ref)
    sketch_term(
        out_ref,
        core_ref,
        sketch_core_ref,
        lambda core: dot(core[:, :MAIN], sketch, 1, 1) + dot(core[:, MAIN:], rest, 1, 0),
    )


def last_sketch_kernel(x_ref, core_ref, sketch_core_ref, sketch_ref, rest_ref, out_ref):
    @pl.when(x_ref[0] == 0)
    def _():
        out_ref[...] = rest_ref[...]

    @pl.when(x_ref[0] != 0)
    def _():
        sketch_kernel(core_ref, sketch_core_ref, sketch_ref, out_ref)


def images_with(sketch_ref):
    sketch, rest = read(sketch_ref)
    return lambda built: dot(built[:, :MAIN], sketch, 1, 1) + dot(built[:, MAIN:], rest, 1, 0)


def prepare(core_ref, product, images_of, y_ref, z_ref):
    for i in range(core_ref.shape[0]):
        high, low = halves(product(core_ref[i]))
        y_ref[0, i], y_ref[1, i] = high, low
        z_ref[0, i], z_ref[1, i] = halves(images_of(high) + images_of(low))


def gram_term(out_ref, images_ref, inverse, y_ref, z_ref):
    inverse_high, inverse_low = halves(inverse)

    def scaled(ref, i):
        return dot(inverse_high, ref[0, i], 1, 0) + (
            dot(inverse_high, ref[1, i], 1, 0) + dot(inverse_low, ref[0, i], 1, 0)
        )

    total = rest = None
    for i in range(images_ref.shape[0]):
        built = scaled(y_ref, i).astype(BF16)
        images = scaled(z_ref, i)
        images_ref[i] = images
        images = images.astype(BF16)
        term = dot(images, built[:, :MAIN], 0, 0)
        end = dot(built[:, MAIN:], images, 0, 0)
        total, rest = (term, end) if total is None else (total + term, rest + end)
    write(out_ref, total, rest)


def project(m_ref, before_ref, core_ref, images_of, out_ref, images_ref, y_ref, z_ref):
    main, rest = read(m_ref)
    gram = symmetric_gram((main, rest), read(before_ref))
    prepare(
        core_ref, lambda core: dot(main, core[:MAIN], 1, 0) + dot(rest, core[MAIN:], 0, 0), images_of, y_ref, z_ref
    )
    gram_term(out_ref, images_ref, inverse_factor(gram), y_ref, z_ref)


def project_kernel(m_ref, before_ref, core_ref, sketch_ref, out_ref, images_ref, y_ref, z_ref):
    project(m_ref, before_ref, core_ref, images_with(sketch_ref), out_ref, images_ref, y_ref, z_ref)


def m_0_gram(m_value, sketch, sketch_rest):
    high, low = halves(m_value)
    total = None
    for part in (high, low):
        term = 0.5 * (
            dot(part[:, :MAIN], sketch, 1, 1)
            + dot(part[:, MAIN:], sketch_rest, 1, 0)
            + dot(sketch, part[:, :MAIN], 1, 1)
            + dot(sketch_rest, part[:, MAIN:], 0, 1)
        )
        total = term if total is None else total + term
    return total


def first_project_kernel(
    upper_ref, rest_ref, before_ref, core_ref, sketch_ref, out_ref, images_ref, m0_ref, y_ref, z_ref
):
    s, sd = read(before_ref)
    sa, sb, sc = s[:, :128], s[:, 128:256], s[:, 256:384]

    def mended(block):
        wide = block.astype(F32)
        row = lax.broadcasted_iota(jnp.int32, (128, 128), 0)
        lane = lax.broadcasted_iota(jnp.int32, (128, 128), 1)
        return jnp.where((row >= 64) & (lane < 64), wide.T, wide).astype(BF16)

    def ends(ref, lane):
        return jnp.concatenate([ref[64:128, lane : lane + 16], ref[64:128, lane + 16 : lane + 32]], axis=0)

    a_end, b_end, c_end = ends(upper_ref, 0), ends(upper_ref, 32), ends(rest_ref, 256)
    d_end = rest_ref[64:80, 288:304]
    a_own = mended(upper_ref[:, :128])
    a_far = upper_ref[:, 128:]
    b = rest_ref[:, :256]
    c = mended(rest_ref[:, 256:384])
    m0_ref[:, :128] = dot(sa, a_own, 1, 0) + dot(s[:, 128:], a_far, 1, 1) + dot(sd, a_end, 0, 1)
    m0_ref[:, 128:256] = (
        dot(sa, a_far[:, :128], 1, 0) + dot(sb, b[:, :128], 1, 0) + dot(sc, b[:, 128:], 1, 1) + dot(sd, b_end, 0, 1)
    )
    m0_ref[:, 256:384] = (
        dot(sa, a_far[:, 128:], 1, 0) + dot(sb, b[:, 128:], 1, 0) + dot(sc, c, 1, 0) + dot(sd, c_end, 0, 1)
    )
    m0_ref[:, 384:] = dot(sa, a_end, 1, 0) + dot(sb, b_end, 1, 0) + dot(sc, c_end, 1, 0) + dot(sd, d_end, 0, 0)
    m_value = m0_ref[...]
    gram = m_0_gram(m_value, s, sd)
    high, low = halves(m_value)
    prepare(
        core_ref, lambda core: dot(high, core, 1, 0) + dot(low, core, 1, 0), images_with(sketch_ref), y_ref, z_ref
    )
    gram_term(out_ref, images_ref, inverse_factor(gram), y_ref, z_ref)


def last_project_kernel(
    x_ref, m_ref, before_ref, core_ref, right_ref, left_ref, third_ref, out_ref, images_ref, y_ref, z_ref
):
    @pl.when(x_ref[0] == 3)
    def _():
        project(
            m_ref, before_ref, core_ref, lambda built: dot(built, right_ref[...], 1, 0), out_ref, images_ref,
            y_ref, z_ref,
        )

    @pl.when(x_ref[0] != 3)
    def _():
        out_ref[...] = jnp.zeros(out_ref.shape, BF16)
        images_of = images_with(third_ref)
        left_t = left_ref[...].astype(BF16)
        for i in range(core_ref.shape[0]):
            images_ref[i] = images_of(dot(left_t, core_ref[i], 0, 0).astype(BF16))


def final_kernel(
    scale, x_ref, m_0_ref, m_1_ref, m_2_ref, m_3_ref, third_ref, second_ref, first_ref, right_ref,
    images_1_ref, images_2_ref, images_0_ref, frames_ref, interface_ref, main_ref, rest_ref, gram_ref, images_ref,
):
    def take(m_ref):
        main, rest = read(m_ref)
        main_ref[...] = main.astype(F32)
        rest_ref[...] = rest.astype(F32)
        return main, rest

    @pl.when(x_ref[0] == 0)
    def _():
        m_value = m_0_ref[...]
        main_ref[...] = m_value[:, :MAIN]
        rest_ref[...] = m_value[:, MAIN:].T
        images_ref[...] = images_0_ref[...]
        gram_ref[...] = m_0_gram(m_value, *read(third_ref))

    @pl.when(x_ref[0] == 1)
    def _():
        images_ref[...] = images_1_ref[...]
        gram_ref[...] = symmetric_gram(take(m_1_ref), read(second_ref))

    @pl.when(x_ref[0] == 2)
    def _():
        images_ref[...] = images_2_ref[...]
        gram_ref[...] = symmetric_gram(take(m_2_ref), read(first_ref))

    @pl.when(x_ref[0] == 3)
    def _():
        images_ref[...] = images_0_ref[...]
        main, rest = take(m_3_ref)
        right, right_rest = right_ref[:MAIN], right_ref[MAIN:]
        gram_ref[...] = 0.5 * (
            dot(main, right, 1, 0) + dot(rest, right_rest, 0, 0) + dot(right, main, 0, 1) + dot(right_rest, rest, 0, 0)
        )

    inverse = inverse_factor(gram_ref[...])
    interface_ref[:, 0, :MAIN] = wide_dot(inverse, main_ref[...], 1, 0)
    interface_ref[:, 0, MAIN:] = wide_dot(inverse, rest_ref[...], 1, 1)
    for i in range(images_ref.shape[0]):
        frames_ref[:, i, :] = (wide_dot(images_ref[i], inverse, 1, 1) * scale).astype(BF16)


def call(kernel, *operands, out, scalar=False, scratch=()):
    specs = [pl.BlockSpec(memory_space=pltpu.VMEM) for _ in operands]
    if scalar:
        specs[0] = pl.BlockSpec(memory_space=pltpu.SMEM)
    outs = [jax.ShapeDtypeStruct(shape, kind) for shape, kind in out]
    return pl.pallas_call(
        kernel,
        out_shape=outs,
        in_specs=specs,
        out_specs=[pl.BlockSpec(memory_space=pltpu.VMEM) for _ in outs],
        scratch_shapes=[pltpu.VMEM(*piece) for piece in scratch],
        compiler_params=PARAMS,
    )(*operands)


PAYLOAD = ((ROWS, MAIN), BF16)


def device(place, zh, x):
    y, zl, c = place
    if zh >= FAR // 2:
        zl, c = 1 - zl, 1 - c
    index = 0
    for at, size in zip((y, zh, zl, c, x), SIZES):
        index = index * size + at
    return index


def near_group(zh, x):
    return [device(place, zh, x) for place in NEAR]


def far_groups(planes):
    groups = [[device(place, zh, x) for zh in range(FAR)] for x in planes for place in NEAR]
    for x in range(4):
        if x not in planes:
            for zh in range(FAR):
                for chip in range(2):
                    groups.append([device(place, zh, x) for place in NEAR if place[1] == chip])
    return groups


def pair_groups(pairs):
    groups = [near_group(zh, x) + near_group(zh, other) for x, other in pairs for zh in range(FAR)]
    for x in range(4):
        if not any(x in pair for pair in pairs):
            groups += [near_group(zh, x) + near_group(zh + 1, x) for zh in range(0, FAR, 2)]
    return groups


NEAR_GROUPS = [near_group(zh, x) for x in range(4) for zh in range(FAR)]


def exchanged(tiles, groups):
    return lax.all_to_all(tiles, AXES, 0, 0, axis_index_groups=groups, tiled=True)


def everywhere(shard, groups):
    return exchanged(jnp.broadcast_to(shard, (len(groups[0]), *shard.shape)), groups)


def added(pieces):
    return pieces.astype(F32).sum(axis=0).astype(BF16)


def plane_sum(value, planes):
    tiles = value.reshape(len(NEAR), ROWS // len(NEAR), -1)
    return added(everywhere(added(exchanged(tiles, NEAR_GROUPS)), far_groups(planes)))


def whole_pair(shard, pairs):
    rows = everywhere(shard, pair_groups(pairs))
    return rows[: len(NEAR)].reshape(ROWS, -1), rows[len(NEAR) :].reshape(ROWS, -1)


def body(train_cores, sketch_cores, left_interface, right_sketch):
    plane = lax.axis_index("x")
    plane_ref = plane.astype(jnp.int32).reshape(1)
    core = jnp.swapaxes(train_cores[0], 0, 1)
    sketch_core = jnp.swapaxes(sketch_cores[0], 0, 1)
    modes = core.shape[0]
    frame_scale = math.sqrt(SKETCH * modes * lax.axis_size(MODE))
    left_t = left_interface.T

    term, rest = call(
        first_kernel, plane_ref, core, sketch_core, right_sketch, left_t, out=[PAYLOAD, PAYLOAD], scalar=True
    )
    first = whole_pair(plane_sum(term, (3, 0)), ((3, 2), (0, 1)))[0]
    (term,) = call(sketch_kernel, core, sketch_core, first, out=[PAYLOAD])
    second = whole_pair(plane_sum(term, (2,)), ((2, 1),))[0]
    (term,) = call(last_sketch_kernel, plane_ref, core, sketch_core, second, rest, out=[PAYLOAD], scalar=True)
    third, rest = whole_pair(plane_sum(term, (1, 0)), ((1, 0),))

    images_kind = ((modes, SKETCH, SKETCH), F32)
    kept = [((2, modes, SKETCH, RANK), BF16), ((2, modes, SKETCH, SKETCH), BF16)]
    term, images_1, m_0 = call(
        first_project_kernel, first, rest, third, core, second,
        out=[PAYLOAD, images_kind, ((SKETCH, RANK), F32)], scratch=kept,
    )
    m_1 = whole_pair(plane_sum(term, (1,)), ((1, 2),))[0]
    term, images_2 = call(project_kernel, m_1, second, core, first, out=[PAYLOAD, images_kind], scratch=kept)
    m_2 = whole_pair(plane_sum(term, (2,)), ((2, 3),))[0]
    term, images = call(
        last_project_kernel, plane_ref, m_2, first, core, right_sketch, left_t, third,
        out=[PAYLOAD, images_kind], scalar=True, scratch=kept,
    )
    m_3 = everywhere(plane_sum(term, (3,)), NEAR_GROUPS).reshape(ROWS, -1)

    def finish(*refs):
        final_kernel(frame_scale, *refs)

    frames, interface = call(
        finish, plane_ref, m_0, m_1, m_2, m_3, third, second, first, right_sketch,
        images_1, images_2, images,
        out=[((SKETCH, modes, SKETCH), BF16), ((SKETCH, 1, RANK), F32)], scalar=True,
        scratch=[((SKETCH, MAIN), F32), ((RANK - MAIN, SKETCH), F32), ((SKETCH, SKETCH), F32), images_kind],
    )
    return (frames[None], interface.reshape(1, SKETCH, RANK))


def solution(mesh):
    split = Mesh(mesh.devices.reshape(*SIZES), AXES)
    placed = (P("x", None, MODE, None), P("x", None, MODE, None), P(), P())
    return jax.shard_map(
        body,
        mesh=split,
        in_specs=placed,
        out_specs=(P("x", None, MODE, None), P("x", None, None)),
        check_vma=False,
    )
```

```python
import math

import jax
import jax.numpy as jnp
from jax import lax
from jax.experimental import pallas as pl
from jax.experimental.pallas import tpu as pltpu
from jax.sharding import Mesh
from jax.sharding import PartitionSpec as P

AXES = ("y", "zh", "zl", "c", "x")
MODE = ("y", "zh", "zl", "c")
SIZES = (4, 8, 2, 2, 4)
NEAR = tuple((y, zl, c) for y in range(4) for zl in range(2) for c in range(2))
FAR = 8
RANK = 400
SKETCH = 100
ROWS = 128
MAIN = 384
F32 = jnp.float32
BF16 = jnp.bfloat16
PARAMS = pltpu.CompilerParams(vmem_limit_bytes=24 * 1024 * 1024)


def dot(a, b, ca, cb):
    return lax.dot_general(a, b, (((ca,), (cb,)), ((), ())), preferred_element_type=F32)


def inverse_factor(gram):
    size = gram.shape[0]
    count = -(-size // 8)
    padded = jnp.pad(gram, ((0, count * 8 - size), (0, 128 - size)))
    tiles = [padded[8 * t : 8 * t + 8] for t in range(count)]
    lane = lax.broadcasted_iota(jnp.int32, (8, 128), 1)
    sub = lax.broadcasted_iota(jnp.int32, (8, 128), 0)
    none = jnp.where(lane >= 128, 1.0, 0.0)
    even = sub % 2 == 0
    start = sub - sub % 2

    def column(tile, j):
        return jnp.broadcast_to(tile[:, j : j + 1], (8, 128))

    def line(tile, s):
        return jnp.broadcast_to(tile[s : s + 1], (8, 128))

    for own in range(count):
        base = 8 * own
        width = min(8, size - base)
        step = lane - base
        columns = {t: [column(tiles[t], base + c) for c in range(width)] for t in range(own, count)}
        head = [value + none for value in columns[own]]
        solves, leads = [], []
        tile = tiles[own]
        for s in range(0, width, 2):
            a, b, c = line(head[s], s), line(head[s + 1], s), line(head[s + 1], s + 1)
            scale = 1.0 / (a * c - b * b)
            solve = (a * scale, b * scale, c * scale)
            solves.append(solve)
            leads.append([(line(head[k], s), line(head[k], s + 1)) if k > s + 1 else None for k in range(width)])
            if s + 2 < width:
                below = sub > s + 1
                first = jnp.where(below, head[s] * solve[2] - head[s + 1] * solve[1], 0.0)
                second = jnp.where(below, head[s + 1] * solve[0] - head[s] * solve[1], 0.0)
                pair = (step == s) | (step == s + 1)
                top = jnp.where(pair, jnp.where(step == s, 1.0, 0.0), line(tile, s))
                low = jnp.where(pair, jnp.where(step == s + 1, 1.0, 0.0), line(tile, s + 1))
                tile = jnp.where(pair & below, 0.0, tile) - first * top - second * low
                for k in range(s + 2, width):
                    head[k] = head[k] - first * leads[-1][k][0] - second * leads[-1][k][1]
        tiles[own] = tile
        reduced = jnp.where((step >= start) & (step < 8), jnp.where(step == sub, 1.0, 0.0), tile)
        pivots = [line(reduced, s) for s in range(width)]
        for t in range(own + 1, count):
            col = columns[t]
            new = jnp.where((step >= 0) & (step < 8), 0.0, tiles[t])
            for s in range(0, width, 2):
                a, b, c = solves[s // 2]
                first = col[s] * c - col[s + 1] * b
                second = col[s + 1] * a - col[s] * b
                new = new - first * pivots[s] - second * pivots[s + 1]
                for k in range(s + 2, width):
                    col[k] = col[k] - first * leads[s // 2][k][0] - second * leads[s // 2][k][1]
            tiles[t] = new
    done = []
    for t in range(count):
        row = sub + 8 * t
        tile = tiles[t]
        diagonal = jnp.sum(jnp.where(lane == row, tile, 0.0), axis=1, keepdims=True)
        side = jnp.sum(jnp.where((lane == row - 1) & ~even, tile, 0.0), axis=1, keepdims=True)
        lower = jnp.where(lane < start + 8 * t, tile, jnp.where(lane == row, 1.0, 0.0))
        ratio = jnp.where(even[:, :1], 0.0, side / jnp.concatenate([diagonal[-1:], diagonal[:-1]], axis=0))
        above = jnp.concatenate([lower[-1:], lower[:-1]], axis=0)
        done.append((lower - ratio * above) * lax.rsqrt(diagonal - ratio * side))
    return jnp.concatenate(done, axis=0)[:size, :size]


def halves(value):
    high = value.astype(BF16)
    return high, (value - high.astype(F32)).astype(BF16)


def wide_dot(a, b, ca, cb):
    a_high, a_low = halves(a)
    b_high, b_low = halves(b)
    return dot(a_high, b_high, ca, cb) + (dot(a_high, b_low, ca, cb) + dot(a_low, b_high, ca, cb))


def left_wide_dot(a, b, ca, cb):
    a_high, a_low = halves(a)
    return dot(a_high, b, ca, cb) + dot(a_low, b, ca, cb)


def read(ref):
    return ref[:SKETCH, :MAIN], ref[104:120, :SKETCH]


def write(ref, main, rest):
    ref[...] = jnp.zeros(ref.shape, BF16)
    ref[:SKETCH, :MAIN] = main.astype(BF16)
    ref[104:120, :SKETCH] = rest.astype(BF16)


def symmetric_gram(m_pieces, sketch_pieces):
    main, rest = m_pieces
    sketch, sketch_rest = sketch_pieces
    return 0.5 * (
        dot(main, sketch, 1, 1)
        + dot(rest, sketch_rest, 0, 0)
        + dot(sketch, main, 1, 1)
        + dot(sketch_rest, rest, 0, 0)
    )


def sketch_term(out_ref, core_ref, sketch_core_ref, partial_of):
    total = rest = None
    for i in range(core_ref.shape[0]):
        partial = partial_of(core_ref[i]).astype(BF16)
        term = dot(sketch_core_ref[i], partial[:MAIN], 1, 1)
        end = dot(partial[MAIN:], sketch_core_ref[i], 1, 1)
        total, rest = (term, end) if total is None else (total + term, rest + end)
    write(out_ref, total, rest)


def first_kernel(x_ref, core_ref, sketch_core_ref, right_ref, left_ref, out_ref, rest_ref):
    rest_ref[...] = jnp.zeros((ROWS, MAIN), BF16)

    @pl.when(x_ref[0] != 0)
    def _():
        sketch_term(out_ref, core_ref, sketch_core_ref, lambda core: dot(core, right_ref[...], 1, 0))

    @pl.when(x_ref[0] == 0)
    def _():
        square = None
        left_t = left_ref[...].astype(BF16)
        for i in range(core_ref.shape[0]):
            built = dot(left_t, core_ref[i], 0, 0).astype(BF16)
            term = dot(built, built, 0, 0)
            square = term if square is None else square + term
        square = square.astype(BF16)
        out_ref[...] = square[:128, :MAIN]
        for k in range(4):
            out_ref[64:128, 16 * k : 16 * k + 16] = square[64 * k : 64 * k + 64, MAIN:]
        rest_ref[:, :256] = square[128:256, 128:384]
        rest_ref[:, 256:384] = square[256:384, 256:384]
        rest_ref[64:128, 256:272] = square[256:320, MAIN:]
        rest_ref[64:128, 272:288] = square[320:384, MAIN:]
        rest_ref[64:80, 288:304] = square[384:400, MAIN:]


def sketch_kernel(core_ref, sketch_core_ref, sketch_ref, out_ref):
    sketch, rest = read(sketch_ref)
    sketch_term(
        out_ref,
        core_ref,
        sketch_core_ref,
        lambda core: dot(core[:, :MAIN], sketch, 1, 1) + dot(core[:, MAIN:], rest, 1, 0),
    )


def last_sketch_kernel(x_ref, core_ref, sketch_core_ref, sketch_ref, rest_ref, out_ref):
    @pl.when(x_ref[0] == 0)
    def _():
        out_ref[...] = rest_ref[...]

    @pl.when(x_ref[0] != 0)
    def _():
        sketch_kernel(core_ref, sketch_core_ref, sketch_ref, out_ref)


def images_with(sketch_ref):
    sketch, rest = read(sketch_ref)
    return lambda built: dot(built[:, :MAIN], sketch, 1, 1) + dot(built[:, MAIN:], rest, 1, 0)


def prepare(core_ref, product, images_of, y_ref, z_ref):
    for i in range(core_ref.shape[0]):
        high, low = halves(product(core_ref[i]))
        y_ref[0, i], y_ref[1, i] = high, low
        z_ref[0, i], z_ref[1, i] = halves(images_of(high) + images_of(low))


def gram_term(out_ref, images_ref, inverse, y_ref, z_ref):
    inverse_high, inverse_low = halves(inverse)

    def scaled(ref, i):
        return dot(inverse_high, ref[0, i], 1, 0) + (
            dot(inverse_high, ref[1, i], 1, 0) + dot(inverse_low, ref[0, i], 1, 0)
        )

    total = rest = None
    for i in range(images_ref.shape[0]):
        built = scaled(y_ref, i).astype(BF16)
        images = scaled(z_ref, i)
        images_ref[i] = images
        images = images.astype(BF16)
        term = dot(images, built[:, :MAIN], 0, 0)
        end = dot(built[:, MAIN:], images, 0, 0)
        total, rest = (term, end) if total is None else (total + term, rest + end)
    write(out_ref, total, rest)


def project(m_ref, before_ref, core_ref, images_of, out_ref, images_ref, y_ref, z_ref):
    main, rest = read(m_ref)
    gram = symmetric_gram((main, rest), read(before_ref))
    prepare(
        core_ref, lambda core: dot(main, core[:MAIN], 1, 0) + dot(rest, core[MAIN:], 0, 0), images_of, y_ref, z_ref
    )
    gram_term(out_ref, images_ref, inverse_factor(gram), y_ref, z_ref)


def project_kernel(m_ref, before_ref, core_ref, sketch_ref, out_ref, images_ref, y_ref, z_ref):
    project(m_ref, before_ref, core_ref, images_with(sketch_ref), out_ref, images_ref, y_ref, z_ref)


def m_0_gram(m_value, sketch, sketch_rest):
    high, low = halves(m_value)
    total = None
    for part in (high, low):
        term = 0.5 * (
            dot(part[:, :MAIN], sketch, 1, 1)
            + dot(part[:, MAIN:], sketch_rest, 1, 0)
            + dot(sketch, part[:, :MAIN], 1, 1)
            + dot(sketch_rest, part[:, MAIN:], 0, 1)
        )
        total = term if total is None else total + term
    return total


def first_project_kernel(
    upper_ref, rest_ref, before_ref, core_ref, sketch_ref, out_ref, images_ref, m0_ref, y_ref, z_ref
):
    s, sd = read(before_ref)
    sa, sb, sc = s[:, :128], s[:, 128:256], s[:, 256:384]

    def mended(block):
        wide = block.astype(F32)
        row = lax.broadcasted_iota(jnp.int32, (128, 128), 0)
        lane = lax.broadcasted_iota(jnp.int32, (128, 128), 1)
        return jnp.where((row >= 64) & (lane < 64), wide.T, wide).astype(BF16)

    def ends(ref, lane):
        return jnp.concatenate([ref[64:128, lane : lane + 16], ref[64:128, lane + 16 : lane + 32]], axis=0)

    a_end, b_end, c_end = ends(upper_ref, 0), ends(upper_ref, 32), ends(rest_ref, 256)
    d_end = rest_ref[64:80, 288:304]
    a_own = mended(upper_ref[:, :128])
    a_far = upper_ref[:, 128:]
    b = rest_ref[:, :256]
    c = mended(rest_ref[:, 256:384])
    m0_ref[:, :128] = dot(sa, a_own, 1, 0) + dot(s[:, 128:], a_far, 1, 1) + dot(sd, a_end, 0, 1)
    m0_ref[:, 128:256] = (
        dot(sa, a_far[:, :128], 1, 0) + dot(sb, b[:, :128], 1, 0) + dot(sc, b[:, 128:], 1, 1) + dot(sd, b_end, 0, 1)
    )
    m0_ref[:, 256:384] = (
        dot(sa, a_far[:, 128:], 1, 0) + dot(sb, b[:, 128:], 1, 0) + dot(sc, c, 1, 0) + dot(sd, c_end, 0, 1)
    )
    m0_ref[:, 384:] = dot(sa, a_end, 1, 0) + dot(sb, b_end, 1, 0) + dot(sc, c_end, 1, 0) + dot(sd, d_end, 0, 0)
    m_value = m0_ref[...]
    gram = m_0_gram(m_value, s, sd)
    high, low = halves(m_value)
    prepare(
        core_ref, lambda core: dot(high, core, 1, 0) + dot(low, core, 1, 0), images_with(sketch_ref), y_ref, z_ref
    )
    gram_term(out_ref, images_ref, inverse_factor(gram), y_ref, z_ref)


def last_project_kernel(
    x_ref, m_ref, before_ref, core_ref, right_ref, left_ref, third_ref, out_ref, images_ref, y_ref, z_ref
):
    @pl.when(x_ref[0] == 3)
    def _():
        project(
            m_ref, before_ref, core_ref, lambda built: dot(built, right_ref[...], 1, 0), out_ref, images_ref,
            y_ref, z_ref,
        )

    @pl.when(x_ref[0] != 3)
    def _():
        out_ref[...] = jnp.zeros(out_ref.shape, BF16)
        images_of = images_with(third_ref)
        left_t = left_ref[...].astype(BF16)
        for i in range(core_ref.shape[0]):
            images_ref[i] = images_of(dot(left_t, core_ref[i], 0, 0).astype(BF16))


def final_kernel(
    scale, x_ref, m_0_ref, m_1_ref, m_2_ref, m_3_ref, third_ref, second_ref, first_ref, right_ref,
    images_1_ref, images_2_ref, images_0_ref, frames_ref, interface_ref, main_ref, rest_ref, gram_ref, images_ref,
):
    def take(m_ref):
        main, rest = read(m_ref)
        main_ref[...] = main.astype(F32)
        rest_ref[...] = rest.astype(F32)
        return main, rest

    @pl.when(x_ref[0] == 0)
    def _():
        m_value = m_0_ref[...]
        main_ref[...] = m_value[:, :MAIN]
        rest_ref[...] = m_value[:, MAIN:].T
        images_ref[...] = images_0_ref[...]
        gram_ref[...] = m_0_gram(m_value, *read(third_ref))

    @pl.when(x_ref[0] == 1)
    def _():
        images_ref[...] = images_1_ref[...]
        gram_ref[...] = symmetric_gram(take(m_1_ref), read(second_ref))

    @pl.when(x_ref[0] == 2)
    def _():
        images_ref[...] = images_2_ref[...]
        gram_ref[...] = symmetric_gram(take(m_2_ref), read(first_ref))

    @pl.when(x_ref[0] == 3)
    def _():
        images_ref[...] = images_0_ref[...]
        main, rest = take(m_3_ref)
        right, right_rest = right_ref[:MAIN], right_ref[MAIN:]
        gram_ref[...] = 0.5 * (
            dot(main, right, 1, 0) + dot(rest, right_rest, 0, 0) + dot(right, main, 0, 1) + dot(right_rest, rest, 0, 0)
        )

    inverse = inverse_factor(gram_ref[...])
    interface_ref[:, 0, :MAIN] = wide_dot(inverse, main_ref[...], 1, 0)
    interface_ref[:, 0, MAIN:] = wide_dot(inverse, rest_ref[...], 1, 1)
    for i in range(images_ref.shape[0]):
        frames_ref[:, i, :] = (wide_dot(images_ref[i], inverse, 1, 1) * scale).astype(BF16)


def call(kernel, *operands, out, scalar=False, scratch=()):
    specs = [pl.BlockSpec(memory_space=pltpu.VMEM) for _ in operands]
    if scalar:
        specs[0] = pl.BlockSpec(memory_space=pltpu.SMEM)
    outs = [jax.ShapeDtypeStruct(shape, kind) for shape, kind in out]
    return pl.pallas_call(
        kernel,
        out_shape=outs,
        in_specs=specs,
        out_specs=[pl.BlockSpec(memory_space=pltpu.VMEM) for _ in outs],
        scratch_shapes=[pltpu.VMEM(*piece) for piece in scratch],
        compiler_params=PARAMS,
    )(*operands)


PAYLOAD = ((ROWS, MAIN), BF16)


def device(place, zh, x):
    y, zl, c = place
    if zh >= FAR // 2:
        zl, c = 1 - zl, 1 - c
    index = 0
    for at, size in zip((y, zh, zl, c, x), SIZES):
        index = index * size + at
    return index


def near_group(zh, x):
    return [device(place, zh, x) for place in NEAR]


def far_groups(planes):
    groups = [[device(place, zh, x) for zh in range(FAR)] for x in planes for place in NEAR]
    for x in range(4):
        if x not in planes:
            for zh in range(FAR):
                for chip in range(2):
                    groups.append([device(place, zh, x) for place in NEAR if place[1] == chip])
    return groups


def pair_groups(pairs):
    groups = [near_group(zh, x) + near_group(zh, other) for x, other in pairs for zh in range(FAR)]
    for x in range(4):
        if not any(x in pair for pair in pairs):
            groups += [near_group(zh, x) + near_group(zh + 1, x) for zh in range(0, FAR, 2)]
    return groups


NEAR_GROUPS = [near_group(zh, x) for x in range(4) for zh in range(FAR)]


def exchanged(tiles, groups):
    return lax.all_to_all(tiles, AXES, 0, 0, axis_index_groups=groups, tiled=True)


def everywhere(shard, groups):
    return exchanged(jnp.broadcast_to(shard, (len(groups[0]), *shard.shape)), groups)


def added(pieces):
    return pieces.astype(F32).sum(axis=0).astype(BF16)


def plane_sum(value, planes):
    tiles = value.reshape(len(NEAR), ROWS // len(NEAR), -1)
    return added(everywhere(added(exchanged(tiles, NEAR_GROUPS)), far_groups(planes)))


def whole_pair(shard, pairs):
    rows = everywhere(shard, pair_groups(pairs))
    return rows[: len(NEAR)].reshape(ROWS, -1), rows[len(NEAR) :].reshape(ROWS, -1)


def body(train_cores, sketch_cores, left_interface, right_sketch):
    plane = lax.axis_index("x")
    plane_ref = plane.astype(jnp.int32).reshape(1)
    core = jnp.swapaxes(train_cores[0], 0, 1)
    sketch_core = jnp.swapaxes(sketch_cores[0], 0, 1)
    modes = core.shape[0]
    frame_scale = math.sqrt(SKETCH * modes * lax.axis_size(MODE))
    left_t = left_interface.T

    term, rest = call(
        first_kernel, plane_ref, core, sketch_core, right_sketch, left_t, out=[PAYLOAD, PAYLOAD], scalar=True
    )
    first = whole_pair(plane_sum(term, (3, 0)), ((3, 2), (0, 1)))[0]
    (term,) = call(sketch_kernel, core, sketch_core, first, out=[PAYLOAD])
    second = whole_pair(plane_sum(term, (2,)), ((2, 1),))[0]
    (term,) = call(last_sketch_kernel, plane_ref, core, sketch_core, second, rest, out=[PAYLOAD], scalar=True)
    third, rest = whole_pair(plane_sum(term, (1, 0)), ((1, 0),))

    images_kind = ((modes, SKETCH, SKETCH), F32)
    kept = [((2, modes, SKETCH, RANK), BF16), ((2, modes, SKETCH, SKETCH), BF16)]
    term, images_1, m_0 = call(
        first_project_kernel, first, rest, third, core, second,
        out=[PAYLOAD, images_kind, ((SKETCH, RANK), F32)], scratch=kept,
    )
    m_1 = whole_pair(plane_sum(term, (1,)), ((1, 2),))[0]
    term, images_2 = call(project_kernel, m_1, second, core, first, out=[PAYLOAD, images_kind], scratch=kept)
    m_2 = whole_pair(plane_sum(term, (2,)), ((2, 3),))[0]
    term, images = call(
        last_project_kernel, plane_ref, m_2, first, core, right_sketch, left_t, third,
        out=[PAYLOAD, images_kind], scalar=True, scratch=kept,
    )
    m_3 = everywhere(plane_sum(term, (3,)), NEAR_GROUPS).reshape(ROWS, -1)

    def finish(*refs):
        final_kernel(frame_scale, *refs)

    frames, interface = call(
        finish, plane_ref, m_0, m_1, m_2, m_3, third, second, first, right_sketch,
        images_1, images_2, images,
        out=[((SKETCH, modes, SKETCH), BF16), ((SKETCH, 1, RANK), F32)], scalar=True,
        scratch=[((SKETCH, MAIN), F32), ((RANK - MAIN, SKETCH), F32), ((SKETCH, SKETCH), F32), images_kind],
    )
    return (frames[None], interface.reshape(1, SKETCH, RANK))


def solution(mesh):
    split = Mesh(mesh.devices.reshape(*SIZES), AXES)
    placed = (P("x", None, MODE, None), P("x", None, MODE, None), P(), P())
    return jax.shard_map(
        body,
        mesh=split,
        in_specs=placed,
        out_specs=(P("x", None, MODE, None), P("x", None, None)),
        check_vma=False,
    )
```

```python
import math

import jax
import jax.numpy as jnp
from jax import lax
from jax.experimental import pallas as pl
from jax.experimental.pallas import tpu as pltpu
from jax.sharding import Mesh
from jax.sharding import PartitionSpec as P

AXES = ("y", "zh", "zl", "c", "x")
MODE = ("y", "zh", "zl", "c")
SIZES = (4, 8, 2, 2, 4)
NEAR = tuple((y, zl, c) for y in range(4) for zl in range(2) for c in range(2))
FAR = 8
RANK = 400
SKETCH = 100
ROWS = 128
MAIN = 384
F32 = jnp.float32
BF16 = jnp.bfloat16
PARAMS = pltpu.CompilerParams(vmem_limit_bytes=24 * 1024 * 1024)


def dot(a, b, ca, cb):
    return lax.dot_general(a, b, (((ca,), (cb,)), ((), ())), preferred_element_type=F32)


def inverse_factor(gram):
    size = gram.shape[0]
    count = -(-size // 8)
    padded = jnp.pad(gram, ((0, count * 8 - size), (0, 128 - size)))
    tiles = [padded[8 * t : 8 * t + 8] for t in range(count)]
    lane = lax.broadcasted_iota(jnp.int32, (8, 128), 1)
    sub = lax.broadcasted_iota(jnp.int32, (8, 128), 0)
    none = jnp.where(lane >= 128, 1.0, 0.0)
    even = sub % 2 == 0
    start = sub - sub % 2

    def column(tile, j):
        return jnp.broadcast_to(tile[:, j : j + 1], (8, 128))

    def line(tile, s):
        return jnp.broadcast_to(tile[s : s + 1], (8, 128))

    for own in range(count):
        base = 8 * own
        width = min(8, size - base)
        step = lane - base
        columns = {t: [column(tiles[t], base + c) for c in range(width)] for t in range(own, count)}
        head = [value + none for value in columns[own]]
        solves, leads = [], []
        tile = tiles[own]
        for s in range(0, width, 2):
            a, b, c = line(head[s], s), line(head[s + 1], s), line(head[s + 1], s + 1)
            scale = 1.0 / (a * c - b * b)
            solve = (a * scale, b * scale, c * scale)
            solves.append(solve)
            leads.append([(line(head[k], s), line(head[k], s + 1)) if k > s + 1 else None for k in range(width)])
            if s + 2 < width:
                below = sub > s + 1
                first = jnp.where(below, head[s] * solve[2] - head[s + 1] * solve[1], 0.0)
                second = jnp.where(below, head[s + 1] * solve[0] - head[s] * solve[1], 0.0)
                pair = (step == s) | (step == s + 1)
                top = jnp.where(pair, jnp.where(step == s, 1.0, 0.0), line(tile, s))
                low = jnp.where(pair, jnp.where(step == s + 1, 1.0, 0.0), line(tile, s + 1))
                tile = jnp.where(pair & below, 0.0, tile) - first * top - second * low
                for k in range(s + 2, width):
                    head[k] = head[k] - first * leads[-1][k][0] - second * leads[-1][k][1]
        tiles[own] = tile
        reduced = jnp.where((step >= start) & (step < 8), jnp.where(step == sub, 1.0, 0.0), tile)
        pivots = [line(reduced, s) for s in range(width)]
        for t in range(own + 1, count):
            col = columns[t]
            new = jnp.where((step >= 0) & (step < 8), 0.0, tiles[t])
            for s in range(0, width, 2):
                a, b, c = solves[s // 2]
                first = col[s] * c - col[s + 1] * b
                second = col[s + 1] * a - col[s] * b
                new = new - first * pivots[s] - second * pivots[s + 1]
                for k in range(s + 2, width):
                    col[k] = col[k] - first * leads[s // 2][k][0] - second * leads[s // 2][k][1]
            tiles[t] = new
    done = []
    for t in range(count):
        row = sub + 8 * t
        tile = tiles[t]
        diagonal = jnp.sum(jnp.where(lane == row, tile, 0.0), axis=1, keepdims=True)
        side = jnp.sum(jnp.where((lane == row - 1) & ~even, tile, 0.0), axis=1, keepdims=True)
        lower = jnp.where(lane < start + 8 * t, tile, jnp.where(lane == row, 1.0, 0.0))
        ratio = jnp.where(even[:, :1], 0.0, side / jnp.concatenate([diagonal[-1:], diagonal[:-1]], axis=0))
        above = jnp.concatenate([lower[-1:], lower[:-1]], axis=0)
        done.append((lower - ratio * above) * lax.rsqrt(diagonal - ratio * side))
    return jnp.concatenate(done, axis=0)[:size, :size]


def halves(value):
    high = value.astype(BF16)
    return high, (value - high.astype(F32)).astype(BF16)


def wide_dot(a, b, ca, cb):
    a_high, a_low = halves(a)
    b_high, b_low = halves(b)
    return dot(a_high, b_high, ca, cb) + (dot(a_high, b_low, ca, cb) + dot(a_low, b_high, ca, cb))


def left_wide_dot(a, b, ca, cb):
    a_high, a_low = halves(a)
    return dot(a_high, b, ca, cb) + dot(a_low, b, ca, cb)


def read(ref):
    return ref[:SKETCH, :MAIN], ref[104:120, :SKETCH]


def write(ref, main, rest):
    ref[...] = jnp.zeros(ref.shape, BF16)
    ref[:SKETCH, :MAIN] = main.astype(BF16)
    ref[104:120, :SKETCH] = rest.astype(BF16)


def symmetric_gram(m_pieces, sketch_pieces):
    main, rest = m_pieces
    sketch, sketch_rest = sketch_pieces
    return 0.5 * (
        dot(main, sketch, 1, 1)
        + dot(rest, sketch_rest, 0, 0)
        + dot(sketch, main, 1, 1)
        + dot(sketch_rest, rest, 0, 0)
    )


def sketch_term(out_ref, core_ref, sketch_core_ref, partial_of):
    total = None
    for i in range(core_ref.shape[0]):
        partial = partial_of(core_ref[i]).astype(BF16)
        term = dot(sketch_core_ref[i], partial, 1, 1)
        total = term if total is None else total + term
    write(out_ref, total[:, :MAIN], total[:, MAIN:].T)


def first_kernel(x_ref, core_ref, sketch_core_ref, right_ref, left_ref, out_ref, rest_ref):
    rest_ref[...] = jnp.zeros((ROWS, MAIN), BF16)

    @pl.when(x_ref[0] != 0)
    def _():
        sketch_term(out_ref, core_ref, sketch_core_ref, lambda core: dot(core, right_ref[...], 1, 0))

    @pl.when(x_ref[0] == 0)
    def _():
        square = None
        left_t = left_ref[...].astype(BF16)
        for i in range(core_ref.shape[0]):
            built = dot(left_t, core_ref[i], 0, 0).astype(BF16)
            term = dot(built, built, 0, 0)
            square = term if square is None else square + term
        square = square.astype(BF16)
        out_ref[...] = square[:128, :MAIN]
        for k in range(4):
            out_ref[64:128, 16 * k : 16 * k + 16] = square[64 * k : 64 * k + 64, MAIN:]
        rest_ref[:, :256] = square[128:256, 128:384]
        rest_ref[:, 256:384] = square[256:384, 256:384]
        rest_ref[64:128, 256:272] = square[256:320, MAIN:]
        rest_ref[64:128, 272:288] = square[320:384, MAIN:]
        rest_ref[64:80, 288:304] = square[384:400, MAIN:]


def sketch_kernel(core_ref, sketch_core_ref, sketch_ref, out_ref):
    sketch, rest = read(sketch_ref)
    sketch_term(
        out_ref,
        core_ref,
        sketch_core_ref,
        lambda core: dot(core[:, :MAIN], sketch, 1, 1) + dot(core[:, MAIN:], rest, 1, 0),
    )


def last_sketch_kernel(x_ref, core_ref, sketch_core_ref, sketch_ref, rest_ref, out_ref):
    @pl.when(x_ref[0] == 0)
    def _():
        out_ref[...] = rest_ref[...]

    @pl.when(x_ref[0] != 0)
    def _():
        sketch_kernel(core_ref, sketch_core_ref, sketch_ref, out_ref)


def images_with(sketch_ref):
    sketch, rest = read(sketch_ref)
    return lambda built: dot(built[:, :MAIN], sketch, 1, 1) + dot(built[:, MAIN:], rest, 1, 0)


def prepare(core_ref, product, images_of, y_ref, z_ref):
    for i in range(core_ref.shape[0]):
        high, low = halves(product(core_ref[i]))
        y_ref[0, i], y_ref[1, i] = high, low
        z_ref[0, i], z_ref[1, i] = halves(images_of(high) + images_of(low))


def gram_term(out_ref, images_ref, inverse, y_ref, z_ref):
    inverse_high, inverse_low = halves(inverse)

    def scaled(ref, i):
        return dot(inverse_high, ref[0, i], 1, 0) + (
            dot(inverse_high, ref[1, i], 1, 0) + dot(inverse_low, ref[0, i], 1, 0)
        )

    total = rest = None
    for i in range(images_ref.shape[0]):
        built = scaled(y_ref, i).astype(BF16)
        images = scaled(z_ref, i)
        images_ref[i] = images
        images = images.astype(BF16)
        term = dot(images, built[:, :MAIN], 0, 0)
        end = dot(built[:, MAIN:], images, 0, 0)
        total, rest = (term, end) if total is None else (total + term, rest + end)
    write(out_ref, total, rest)


def project(m_ref, before_ref, core_ref, images_of, out_ref, images_ref, y_ref, z_ref):
    main, rest = read(m_ref)
    gram = symmetric_gram((main, rest), read(before_ref))
    prepare(
        core_ref, lambda core: dot(main, core[:MAIN], 1, 0) + dot(rest, core[MAIN:], 0, 0), images_of, y_ref, z_ref
    )
    gram_term(out_ref, images_ref, inverse_factor(gram), y_ref, z_ref)


def project_kernel(m_ref, before_ref, core_ref, sketch_ref, out_ref, images_ref, y_ref, z_ref):
    project(m_ref, before_ref, core_ref, images_with(sketch_ref), out_ref, images_ref, y_ref, z_ref)


def m_0_gram(m_value, sketch, sketch_rest):
    high, low = halves(m_value)
    total = None
    for part in (high, low):
        term = 0.5 * (
            dot(part[:, :MAIN], sketch, 1, 1)
            + dot(part[:, MAIN:], sketch_rest, 1, 0)
            + dot(sketch, part[:, :MAIN], 1, 1)
            + dot(sketch_rest, part[:, MAIN:], 0, 1)
        )
        total = term if total is None else total + term
    return total


def first_project_kernel(
    upper_ref, rest_ref, before_ref, core_ref, sketch_ref, out_ref, images_ref, m0_ref, y_ref, z_ref
):
    s, sd = read(before_ref)
    sa, sb, sc = s[:, :128], s[:, 128:256], s[:, 256:384]

    def mended(block):
        wide = block.astype(F32)
        row = lax.broadcasted_iota(jnp.int32, (128, 128), 0)
        lane = lax.broadcasted_iota(jnp.int32, (128, 128), 1)
        return jnp.where((row >= 64) & (lane < 64), wide.T, wide).astype(BF16)

    def ends(ref, lane):
        return jnp.concatenate([ref[64:128, lane : lane + 16], ref[64:128, lane + 16 : lane + 32]], axis=0)

    a_end, b_end, c_end = ends(upper_ref, 0), ends(upper_ref, 32), ends(rest_ref, 256)
    d_end = rest_ref[64:80, 288:304]
    a_own = mended(upper_ref[:, :128])
    a_far = upper_ref[:, 128:]
    b = rest_ref[:, :256]
    c = mended(rest_ref[:, 256:384])
    m0_ref[:, :128] = dot(sa, a_own, 1, 0) + dot(s[:, 128:], a_far, 1, 1) + dot(sd, a_end, 0, 1)
    m0_ref[:, 128:256] = (
        dot(sa, a_far[:, :128], 1, 0) + dot(sb, b[:, :128], 1, 0) + dot(sc, b[:, 128:], 1, 1) + dot(sd, b_end, 0, 1)
    )
    m0_ref[:, 256:384] = (
        dot(sa, a_far[:, 128:], 1, 0) + dot(sb, b[:, 128:], 1, 0) + dot(sc, c, 1, 0) + dot(sd, c_end, 0, 1)
    )
    m0_ref[:, 384:] = dot(sa, a_end, 1, 0) + dot(sb, b_end, 1, 0) + dot(sc, c_end, 1, 0) + dot(sd, d_end, 0, 0)
    m_value = m0_ref[...]
    gram = m_0_gram(m_value, s, sd)
    high, low = halves(m_value)
    prepare(
        core_ref, lambda core: dot(high, core, 1, 0) + dot(low, core, 1, 0), images_with(sketch_ref), y_ref, z_ref
    )
    gram_term(out_ref, images_ref, inverse_factor(gram), y_ref, z_ref)


def last_project_kernel(
    x_ref, m_ref, before_ref, core_ref, right_ref, left_ref, third_ref, out_ref, images_ref, y_ref, z_ref
):
    @pl.when(x_ref[0] == 3)
    def _():
        project(
            m_ref, before_ref, core_ref, lambda built: dot(built, right_ref[...], 1, 0), out_ref, images_ref,
            y_ref, z_ref,
        )

    @pl.when(x_ref[0] != 3)
    def _():
        out_ref[...] = jnp.zeros(out_ref.shape, BF16)
        images_of = images_with(third_ref)
        left_t = left_ref[...].astype(BF16)
        for i in range(core_ref.shape[0]):
            images_ref[i] = images_of(dot(left_t, core_ref[i], 0, 0).astype(BF16))


def final_kernel(
    scale, x_ref, m_0_ref, m_1_ref, m_2_ref, m_3_ref, third_ref, second_ref, first_ref, right_ref,
    images_1_ref, images_2_ref, images_0_ref, frames_ref, interface_ref, main_ref, rest_ref, gram_ref, images_ref,
):
    def take(m_ref):
        main, rest = read(m_ref)
        main_ref[...] = main.astype(F32)
        rest_ref[...] = rest.astype(F32)
        return main, rest

    @pl.when(x_ref[0] == 0)
    def _():
        m_value = m_0_ref[...]
        main_ref[...] = m_value[:, :MAIN]
        rest_ref[...] = m_value[:, MAIN:].T
        images_ref[...] = images_0_ref[...]
        gram_ref[...] = m_0_gram(m_value, *read(third_ref))

    @pl.when(x_ref[0] == 1)
    def _():
        images_ref[...] = images_1_ref[...]
        gram_ref[...] = symmetric_gram(take(m_1_ref), read(second_ref))

    @pl.when(x_ref[0] == 2)
    def _():
        images_ref[...] = images_2_ref[...]
        gram_ref[...] = symmetric_gram(take(m_2_ref), read(first_ref))

    @pl.when(x_ref[0] == 3)
    def _():
        images_ref[...] = images_0_ref[...]
        main, rest = take(m_3_ref)
        right, right_rest = right_ref[:MAIN], right_ref[MAIN:]
        gram_ref[...] = 0.5 * (
            dot(main, right, 1, 0) + dot(rest, right_rest, 0, 0) + dot(right, main, 0, 1) + dot(right_rest, rest, 0, 0)
        )

    inverse = inverse_factor(gram_ref[...])
    interface_ref[:, 0, :MAIN] = wide_dot(inverse, main_ref[...], 1, 0)
    interface_ref[:, 0, MAIN:] = wide_dot(inverse, rest_ref[...], 1, 1)
    for i in range(images_ref.shape[0]):
        frames_ref[:, i, :] = (wide_dot(images_ref[i], inverse, 1, 1) * scale).astype(BF16)


def call(kernel, *operands, out, scalar=False, scratch=()):
    specs = [pl.BlockSpec(memory_space=pltpu.VMEM) for _ in operands]
    if scalar:
        specs[0] = pl.BlockSpec(memory_space=pltpu.SMEM)
    outs = [jax.ShapeDtypeStruct(shape, kind) for shape, kind in out]
    return pl.pallas_call(
        kernel,
        out_shape=outs,
        in_specs=specs,
        out_specs=[pl.BlockSpec(memory_space=pltpu.VMEM) for _ in outs],
        scratch_shapes=[pltpu.VMEM(*piece) for piece in scratch],
        compiler_params=PARAMS,
    )(*operands)


PAYLOAD = ((ROWS, MAIN), BF16)


def device(place, zh, x):
    y, zl, c = place
    if zh >= FAR // 2:
        zl, c = 1 - zl, 1 - c
    index = 0
    for at, size in zip((y, zh, zl, c, x), SIZES):
        index = index * size + at
    return index


def near_group(zh, x):
    return [device(place, zh, x) for place in NEAR]


def far_groups(planes):
    groups = [[device(place, zh, x) for zh in range(FAR)] for x in planes for place in NEAR]
    for x in range(4):
        if x not in planes:
            for zh in range(FAR):
                for chip in range(2):
                    groups.append([device(place, zh, x) for place in NEAR if place[1] == chip])
    return groups


def pair_groups(pairs):
    groups = [near_group(zh, x) + near_group(zh, other) for x, other in pairs for zh in range(FAR)]
    for x in range(4):
        if not any(x in pair for pair in pairs):
            groups += [near_group(zh, x) + near_group(zh + 1, x) for zh in range(0, FAR, 2)]
    return groups


NEAR_GROUPS = [near_group(zh, x) for x in range(4) for zh in range(FAR)]


def exchanged(tiles, groups):
    return lax.all_to_all(tiles, AXES, 0, 0, axis_index_groups=groups, tiled=True)


def everywhere(shard, groups):
    return exchanged(jnp.broadcast_to(shard, (len(groups[0]), *shard.shape)), groups)


def added(pieces):
    return pieces.astype(F32).sum(axis=0).astype(BF16)


def plane_sum(value, planes):
    tiles = value.reshape(len(NEAR), ROWS // len(NEAR), -1)
    return added(everywhere(added(exchanged(tiles, NEAR_GROUPS)), far_groups(planes)))


def whole_pair(shard, pairs):
    rows = everywhere(shard, pair_groups(pairs))
    return rows[: len(NEAR)].reshape(ROWS, -1), rows[len(NEAR) :].reshape(ROWS, -1)


def body(train_cores, sketch_cores, left_interface, right_sketch):
    plane = lax.axis_index("x")
    plane_ref = plane.astype(jnp.int32).reshape(1)
    core = jnp.swapaxes(train_cores[0], 0, 1)
    sketch_core = jnp.swapaxes(sketch_cores[0], 0, 1)
    modes = core.shape[0]
    frame_scale = math.sqrt(SKETCH * modes * lax.axis_size(MODE))
    left_t = left_interface.T

    term, rest = call(
        first_kernel, plane_ref, core, sketch_core, right_sketch, left_t, out=[PAYLOAD, PAYLOAD], scalar=True
    )
    first = whole_pair(plane_sum(term, (3, 0)), ((3, 2), (0, 1)))[0]
    (term,) = call(sketch_kernel, core, sketch_core, first, out=[PAYLOAD])
    second = whole_pair(plane_sum(term, (2,)), ((2, 1),))[0]
    (term,) = call(last_sketch_kernel, plane_ref, core, sketch_core, second, rest, out=[PAYLOAD], scalar=True)
    third, rest = whole_pair(plane_sum(term, (1, 0)), ((1, 0),))

    images_kind = ((modes, SKETCH, SKETCH), F32)
    kept = [((2, modes, SKETCH, RANK), BF16), ((2, modes, SKETCH, SKETCH), BF16)]
    term, images_1, m_0 = call(
        first_project_kernel, first, rest, third, core, second,
        out=[PAYLOAD, images_kind, ((SKETCH, RANK), F32)], scratch=kept,
    )
    m_1 = whole_pair(plane_sum(term, (1,)), ((1, 2),))[0]
    term, images_2 = call(project_kernel, m_1, second, core, first, out=[PAYLOAD, images_kind], scratch=kept)
    m_2 = whole_pair(plane_sum(term, (2,)), ((2, 3),))[0]
    term, images = call(
        last_project_kernel, plane_ref, m_2, first, core, right_sketch, left_t, third,
        out=[PAYLOAD, images_kind], scalar=True, scratch=kept,
    )
    m_3 = everywhere(plane_sum(term, (3,)), NEAR_GROUPS).reshape(ROWS, -1)

    def finish(*refs):
        final_kernel(frame_scale, *refs)

    frames, interface = call(
        finish, plane_ref, m_0, m_1, m_2, m_3, third, second, first, right_sketch,
        images_1, images_2, images,
        out=[((SKETCH, modes, SKETCH), BF16), ((SKETCH, 1, RANK), F32)], scalar=True,
        scratch=[((SKETCH, MAIN), F32), ((RANK - MAIN, SKETCH), F32), ((SKETCH, SKETCH), F32), images_kind],
    )
    return (frames[None], interface.reshape(1, SKETCH, RANK))


def solution(mesh):
    split = Mesh(mesh.devices.reshape(*SIZES), AXES)
    placed = (P("x", None, MODE, None), P("x", None, MODE, None), P(), P())
    return jax.shard_map(
        body,
        mesh=split,
        in_specs=placed,
        out_specs=(P("x", None, MODE, None), P("x", None, None)),
        check_vma=False,
    )
```
